32 devices in a mesh: inst: 4 (over x, core), shard: 8 (over z, y).
Axes of the slice: x: 2, y: 2, z: 4, core: 2. Of those that a mesh axis runs over, the one named last changes fastest.
Arguments:
- tokens: bfloat16 [2048, 5120], P(('inst', 'shard')), may hold values from -600 to 600
- norm_gain: float32 [5120], P(('inst', 'shard')), may hold values from 0.1 to 1.9
- master_qkv: float32 [5120, 7168], P(('inst', 'shard')), may hold values from -0.078125 to 0.078125
- qkv_bias: float32 [7168], P(('inst', 'shard')), may hold values from -3 to 3
Outputs:
- qkv_out: bfloat16 [32, 512, 896], P(('inst', 'shard'))
The draws below stay inside these ranges and needn't reach their ends.
All inputs are finite; a program needn't handle non-finite values.
Results may differ from the reference program's by a relative error of at most 0.0062.
Values may be sent and summed in bfloat16 or wider, within the bound.
A program may use at most 64 MiB of HBM per device.

```python
import jax
import jax.numpy as jnp
from jax import lax

D = 5120
QHEADS = 40
KVHEADS = 8
HEAD_DIM = 128
TP = 8
TOK_DEV = 64
QKVW = 7168
TOKENS = 2048
N_INST = 4
N_SHARD = 8


def draw_tokens(key, part):
    row_key, col_key, base_key = jax.random.split(key, 3)
    base = jax.random.truncated_normal(base_key, -4.0, 4.0, (TOKENS, D), jnp.float32)
    row_scale = jnp.power(10.0, jax.random.uniform(row_key, (TOKENS, 1), jnp.float32, 0.0, 1.0))
    col_scale = jnp.power(10.0, jax.random.uniform(col_key, (1, D), jnp.float32, 0.0, 1.0))
    return (base * row_scale * col_scale).astype(jnp.bfloat16)


def block_scale(stream_key, shape, cuts, smallest, largest):
    level = 1.0
    for position, shards_of in cuts:
        heights = jax.random.uniform(jax.random.fold_in(jax.random.fold_in(stream_key, 6), position), (shards_of,), jnp.float32, smallest / len(cuts), largest / len(cuts))
        level = level * jnp.repeat(jnp.exp(heights), shape[position] // shards_of).reshape((-1,) + (1,) * (len(shape) - 1 - position))
    return level


def scatter_about(stream_key, extent, scale, bound, cuts=(), dtype=jnp.bfloat16):
    entries = jax.random.normal(stream_key, extent, jnp.float32) * scale
    if len(cuts) > 0:
        entries = block_scale(stream_key, extent, cuts, -0.22, 0.18) * entries
    return jnp.clip(entries, min=-bound, max=bound).astype(dtype)


def setup_inputs(seed: int = 0) -> dict:
    key_of = jax.random.split(jax.random.key(seed), 5)
    tokens = draw_tokens(jax.random.fold_in(key_of[4], 71), 0)
    norm_gain = jnp.clip(1.0 + 0.18 * jax.random.normal(key_of[1], (D,), jnp.float32), 0.1, 1.9)
    master_qkv = scatter_about(key_of[2], (D, QKVW), D ** -0.5, 0.078125, ((0, 32),), jnp.float32)
    qkv_bias = scatter_about(key_of[3], (QKVW,), 0.5, 3.0, ((0, 32),), jnp.float32)
    return {"tokens": tokens, "norm_gain": norm_gain, "master_qkv": master_qkv, "qkv_bias": qkv_bias}


EPSILON = 1e-06

def rank_columns(matrix):
    query_cols = QHEADS * HEAD_DIM
    pair_cols = KVHEADS * HEAD_DIM
    leading = matrix.shape[:-1]
    query = matrix[..., :query_cols].reshape(leading + (TP, query_cols // TP))
    keys = matrix[..., query_cols:query_cols + pair_cols].reshape(leading + (TP, pair_cols // TP))
    values = matrix[..., query_cols + pair_cols:].reshape(leading + (TP, pair_cols // TP))
    return jnp.concatenate([query, keys, values], axis=-1)

def normalize(tokens, gain):
    floats = tokens.astype(jnp.float32)
    scale = lax.rsqrt(lax.optimization_barrier(jnp.mean(floats * floats, axis=-1, keepdims=True)) + EPSILON)
    return (floats * scale * gain.astype(jnp.float32)).astype(jnp.bfloat16)

def reference(tokens, norm_gain, master_qkv, qkv_bias):
    weights = master_qkv.astype(jnp.bfloat16)
    gain_low = norm_gain.astype(jnp.bfloat16)
    bias_low = qkv_bias.astype(jnp.bfloat16)
    normed = normalize(tokens, gain_low)
    rank_width = QKVW // TP
    flat_weights = rank_columns(weights).reshape(D, TP * rank_width)
    flat_bias = rank_columns(bias_low).reshape(TP * rank_width).astype(jnp.float32)
    group_tokens = TP * TOK_DEV
    groups = normed.reshape(TOKENS // group_tokens, group_tokens, D)

    def project(group_rows):
        product = jnp.dot(group_rows, flat_weights, preferred_element_type=jnp.float32) + flat_bias
        shaped = product.astype(jnp.bfloat16).reshape(group_tokens, TP, rank_width)
        return jnp.transpose(shaped, (1, 0, 2))
    outputs = lax.map(project, groups)
    return outputs.reshape(N_INST * N_SHARD, group_tokens, rank_width)
```

```python
import functools

import jax
import jax.numpy as jnp
from jax import lax
from jax.experimental import pallas as pl
from jax.experimental.pallas import tpu as pltpu
from jax.sharding import PartitionSpec as P

QHEADS = 40
KVHEADS = 8
HEAD_DIM = 128
TP = 8


EPSILON = 1e-06
MESH = pl.DeviceIdType.MESH
LANES = 128
TOKEN_PIECES = 2
CHUNKS = ((0, 2), (2, 4), (4, 7))


def partner_2(value, axis, distance):
    mask = 2**distance
    pairs = [(source, source ^ mask) for source in range(lax.axis_size(axis))]
    return lax.ppermute(value, axis, pairs)


def rank_columns(matrix):
    query_cols = QHEADS * HEAD_DIM
    pair_cols = KVHEADS * HEAD_DIM
    leading = matrix.shape[:-1]
    query = matrix[..., :query_cols].reshape(leading + (TP, query_cols // TP))
    keys = matrix[..., query_cols : query_cols + pair_cols].reshape(leading + (TP, pair_cols // TP))
    values = matrix[..., query_cols + pair_cols :].reshape(leading + (TP, pair_cols // TP))
    return jnp.concatenate([query, keys, values], axis=-1)


def normalize(tokens, gain):
    floats = tokens.astype(jnp.float32)
    scale = lax.rsqrt(jnp.mean(floats * floats, axis=-1, keepdims=True) + EPSILON)
    return (floats * scale * gain.astype(jnp.float32)).astype(jnp.bfloat16)


def general_device(tokens, norm_gain, master_qkv, qkv_bias):
    shard_count = lax.axis_size("shard")
    local_rows = master_qkv.shape[0]
    rank_width = master_qkv.shape[1] // TP
    gain_full, bias_full = (
        lax.all_gather(norm_gain.astype(jnp.bfloat16), ("inst", "shard"), axis=0, tiled=True),
        lax.all_gather(qkv_bias.astype(jnp.bfloat16), ("inst", "shard"), axis=0, tiled=True),
    )
    normed = normalize(tokens, gain_full)
    shard_pos = lax.axis_index("shard")
    rank_index = shard_pos % TP
    bit_count = TP.bit_length() - 1
    bit_order = list(range(bit_count))
    group_rows = normed
    for bit_pos in bit_order:
        partner = partner_2(group_rows, "shard", bit_pos)
        lower = jnp.bitwise_and(jnp.right_shift(shard_pos, bit_pos), 1) == 0
        group_rows = jnp.where(
            lower,
            jnp.concatenate([group_rows, partner], 0),
            jnp.concatenate([partner, group_rows], 0),
        )
    copies = shard_count // TP
    inst_block = shard_count * local_rows
    rows_low = master_qkv.astype(jnp.bfloat16)
    ranked = jnp.transpose(rank_columns(rows_low), (1, 0, 2))
    spread = jnp.broadcast_to(ranked[None], (copies,) + ranked.shape)
    outgoing = spread.reshape(shard_count, rows_low.shape[0], rank_width)
    arrived = lax.all_to_all(outgoing, "shard", split_axis=0, concat_axis=0, tiled=True).reshape(
        inst_block, rank_width
    )
    product = jnp.dot(
        group_rows,
        lax.all_gather(arrived, "inst", axis=0, tiled=True),
        preferred_element_type=jnp.float32,
    )
    bias_ranks = rank_columns(bias_full)
    bias_mine = lax.dynamic_index_in_dim(bias_ranks, rank_index, 0, keepdims=False)
    result = (product + bias_mine.astype(jnp.float32)).astype(jnp.bfloat16)
    return result[None]


def kernel(
    dims,
    tok_hbm,
    gain_ref,
    w_hbm,
    bias_ref,
    out_ref,
    tok_ref,
    w_ref,
    xsend,
    xbuf,
    wsend,
    wbuf,
    psend,
    pbuf,
    acc,
    bias_own,
    bbuf,
    load_sem,
    x_recv,
    x_send,
    x_relay,
    w_recv,
    w_send,
    wx_send,
    wc_send,
    p_recv,
    p_send,
    b_recv,
    b_send,
):
    inst_count, shard_count, group = dims
    devices = inst_count * shard_count
    inst = lax.axis_index("inst")
    me = lax.axis_index("shard")
    z = me // 2
    y = lax.rem(me, 2)
    half = z // 2
    flat = inst * shard_count + me
    core_peer = inst + 1 - 2 * lax.rem(inst, 2)
    x_peer = lax.rem(inst + 2, inst_count)
    far_core = lax.rem(core_peer + 2, inst_count)
    z_mate = z + 1 - 2 * lax.rem(z, 2)
    z_pair = lax.rem(z + 2, 4)
    z_near = 2 - half
    z_end = 3 - 3 * half
    inner = z_near + z == 3
    rows = w_ref.shape[0]
    tokens, depth = tok_ref.shape
    tiles = wsend.shape[1]
    half_block = 4 * rows
    pieces = TOKEN_PIECES
    piece_rows = tokens // pieces
    parts = len(CHUNKS)

    token_load = pltpu.make_async_copy(tok_hbm, tok_ref, load_sem.at[0])
    weight_load = pltpu.make_async_copy(w_hbm, w_ref, load_sem.at[1])
    token_load.start()
    weight_load.start()

    barrier = pltpu.get_barrier_semaphore()

    @pl.loop(1, devices)
    def _(step):
        there = lax.rem(flat + step, devices)
        pl.semaphore_signal(
            barrier,
            inc=1,
            device_id=(there // shard_count, lax.rem(there, shard_count)),
            device_id_type=MESH,
        )

    def remote(source, target, send_sem, recv_sem, device):
        return pltpu.make_async_remote_copy(
            src_ref=source,
            dst_ref=target,
            send_sem=send_sem,
            recv_sem=recv_sem,
            device_id=device,
            device_id_type=MESH,
        )

    def each(condition, action):
        pl.when(condition)(action)

    def piece_of(ref, piece):
        return ref.at[pl.ds(piece * piece_rows, piece_rows)]

    def own_x(way, piece):
        which, device, side = (
            (half, z_mate * 2 + y, 0),
            (1 - half, z_near * 2 + y, 0),
            (1 - half, z_pair * 2 + y, 0),
            (half, z * 2 + 1 - y, 1),
        )[way]
        return remote(
            piece_of(xsend.at[which], piece),
            piece_of(xbuf.at[side, z], piece),
            x_send.at[way, piece],
            x_recv.at[side, z, piece],
            (inst, device),
        )

    def relay_x(way, block, piece):
        device, side = ((z_mate * 2 + y, 0), (z * 2 + 1 - y, 1))[way]
        return remote(
            piece_of(xbuf.at[0, block], piece),
            piece_of(xbuf.at[side, block], piece),
            x_relay.at[way, block, piece],
            x_recv.at[side, block, piece],
            (inst, device),
        )

    def place(k):
        dz, dy = k // 2, k % 2
        return (z_mate if dz else z), (1 - y if dy else y)

    def slot_of(owner, k):
        pz, py = place(k)
        return owner * 4 + lax.rem(pz, 2) * 2 + py

    def tiles_of(j):
        first, last = CHUNKS[j % parts]
        return first, last - first, (j // parts) * tiles + first

    def rank_of(k, j):
        pz, py = place(k)
        return (pz if j >= parts else lax.rem(pz + 2, 4)) * 2 + py

    def fresh(k, j):
        first, count, _ = tiles_of(j)
        return wsend.at[rank_of(k, j), pl.ds(first, count)]

    def held(slot, j):
        _, count, first = tiles_of(j)
        return wbuf.at[slot, pl.ds(first, count)]

    def w_copy(k, j):
        pz, py = place(k)
        slot = slot_of(inst, 0)
        return remote(fresh(k, j), held(slot, j), w_send.at[k - 1, j], w_recv.at[slot, j], (inst, pz * 2 + py))

    def wx_copy(k, j):
        slot = slot_of(inst, k)
        source = held(slot, j) if k else fresh(0, j)
        return remote(source, held(slot, j), wx_send.at[k, j], w_recv.at[slot, j], (x_peer, me))

    def wc_copy(side, k, j):
        slot = slot_of((inst, x_peer)[side], k)
        source = held(slot, j) if k or side else fresh(0, j)
        return remote(source, held(slot, j), wc_send.at[side, k, j], w_recv.at[slot, j], (core_peer, me))

    def p_copy(m, j):
        first, count, _ = tiles_of(j)
        return remote(
            psend.at[m, pl.ds(first, count)],
            pbuf.at[m, pl.ds(first, count)],
            p_send.at[m, j],
            p_recv.at[m, j],
            (inst, z_pair * 2 + y),
        )

    def arrived(ref, sem):
        pltpu.make_async_copy(ref, ref, sem).wait()

    def wait_x(side, block, piece):
        arrived(piece_of(xbuf.at[side, block], piece), x_recv.at[side, block, piece])

    def wait_w(slot, j):
        arrived(held(slot, j), w_recv.at[slot, j])

    query = QHEADS * HEAD_DIM // TP
    pair = KVHEADS * HEAD_DIM // TP
    held_bias = bias_ref.shape[1]
    per_row = LANES // group
    groups = held_bias // group

    def needs(owner, rank):
        low, high = owner * held_bias, owner * held_bias + held_bias
        result = None
        for start, extent in (
            (rank * query, query),
            (TP * query + rank * pair, pair),
            (TP * (query + pair) + rank * pair, pair),
        ):
            overlap = jnp.logical_and(start < high, low < start + extent)
            result = overlap if result is None else jnp.logical_or(result, overlap)
        return result

    def bias_copy(step):
        there = lax.rem(flat + step, devices)
        return remote(
            bias_own,
            bbuf.at[flat],
            b_send.at[step],
            b_recv.at[flat],
            (there // shard_count, lax.rem(there, shard_count)),
        )

    def send_bias(finish):
        @pl.loop(1, devices)
        def _(step):
            there = lax.rem(flat + step, devices)

            @pl.when(needs(flat, lax.rem(there, shard_count)))
            def _():
                if finish:
                    bias_copy(step).wait_send()
                else:
                    bias_copy(step).start()

    def bias_row(number_first):
        lane = lax.broadcasted_iota(jnp.int32, (1, LANES), 1) // group
        row = jnp.zeros((1, LANES), jnp.float32)
        for q in range(per_row):
            number = number_first + q
            row = jnp.where(lane == q, bbuf[number // groups, pl.ds(lax.rem(number, groups), 1), :], row)
        return row

    def column_of(t):
        at = t * LANES
        if at < query:
            return me * query + at
        if at < query + pair:
            return TP * query + me * pair + (at - query)
        return TP * (query + pair) + me * pair + (at - query - pair)

    ids = lax.broadcasted_iota(jnp.int32, (rows, rows), 0), lax.broadcasted_iota(jnp.int32, (rows, rows), 1)
    gain_row = gain_ref[...].astype(jnp.bfloat16).astype(jnp.float32)
    gain = jnp.sum(jnp.where(ids[0] == ids[1], jnp.broadcast_to(gain_row, (rows, rows)), 0.0), axis=1, keepdims=True)
    group_id = lax.broadcasted_iota(jnp.int32, (8, held_bias), 0)
    lane_id = lax.broadcasted_iota(jnp.int32, (8, held_bias), 1)
    spread = jnp.where(lane_id // group == group_id, jnp.broadcast_to(bias_ref[...], (8, held_bias)), 0.0)
    from_id = lax.broadcasted_iota(jnp.int32, (held_bias, LANES), 0)
    to_id = lax.broadcasted_iota(jnp.int32, (held_bias, LANES), 1)
    pick = jnp.where(lax.rem(from_id, group) == lax.rem(to_id, group), 1.0, 0.0).astype(jnp.bfloat16)
    bias_own[...] = jnp.dot(spread.astype(jnp.bfloat16), pick, preferred_element_type=jnp.float32)

    token_load.wait()
    step_rows = 16
    for first in range(0, tokens, step_rows):
        values = tok_ref[first : first + step_rows, :].astype(jnp.float32)
        mean = jnp.sum(values * values, axis=-1, keepdims=True) * (1.0 / depth)
        scaled = (values * lax.rsqrt(mean + EPSILON)).astype(jnp.bfloat16)
        for which in range(2):
            for owner in range(inst_count):
                at = (owner * 2 + which) * half_block
                xsend[which, first : first + step_rows, owner * half_block : (owner + 1) * half_block] = scaled[
                    :, at : at + half_block
                ]
    pl.semaphore_wait(barrier, devices - 1)

    for piece in range(pieces):
        own_x(1, piece).start()
        own_x(0, piece).start()
        own_x(3, piece).start()
    xbuf[0, z] = xsend[half]

    weight_load.wait()
    for rank in range(TP):
        starts = (
            (rank * query, 0, query),
            (TP * query + rank * pair, query, pair),
            (TP * (query + pair) + rank * pair, query + pair, pair),
        )
        for source, target, extent in starts:
            for inside in range(0, extent, LANES):
                part = w_ref[:, source + inside : source + inside + LANES].astype(jnp.bfloat16).astype(jnp.float32)
                wsend[rank, (target + inside) // LANES] = (part * gain).astype(jnp.bfloat16)

    def product(m, j):
        first, count, at = tiles_of(j)
        lhs = xbuf[m].reshape(4 * tokens, 4 * half_block)
        result = []
        for t in range(0, count, 2):
            width = min(2, count - t)
            rhs = [wbuf[:, at + t + u].reshape(4 * half_block, LANES) for u in range(width)]
            rhs = jnp.concatenate(rhs, axis=1) if width > 1 else rhs[0]
            value = jnp.dot(lhs, rhs, preferred_element_type=jnp.float32)
            for u in range(width):
                result.append((first + t + u, value[:, u * LANES : (u + 1) * LANES]))
        return result

    def step_wp(j):
        for k in (2, 1, 3):
            w_copy(k, j).start()

    def step_ox(j):
        wx_copy(0, j).start()
        wc_copy(0, 0, j).start()

    def step_rx(block, to_mate):
        for piece in range(pieces):
            wait_x(0, block, piece)
            if to_mate:
                relay_x(0, block, piece).start()
            relay_x(1, block, piece).start()

    def step_rw(j, ks=(2, 1, 3)):
        for k in ks:
            wait_w(slot_of(inst, k), j)
            wx_copy(k, j).start()
            wc_copy(0, k, j).start()

    def step_rc(j, ks=(0, 2, 1, 3)):
        for k in ks:
            wait_w(slot_of(x_peer, k), j)
            wc_copy(1, k, j).start()

    def step_wc(j):
        for k in range(4):
            wait_w(slot_of(core_peer, k), j)
            wait_w(slot_of(far_core, k), j)

    def step_x1():
        for k in range(4):
            for piece in range(pieces):
                wait_x(1, k, piece)

    def step_pm(m, j):
        for t, value in product(m, j):
            psend[m, t] = value.astype(jnp.bfloat16)
        p_copy(m, j).start()

    def step_om(m, j):
        for t, value in product(m, j):
            acc[m, t] = value

    def step_fin(m, j):
        first, count, _ = tiles_of(j)
        arrived(pbuf.at[m, pl.ds(first, count)], p_recv.at[m, j])
        where = 1 - y if m else y
        for t in range(first, first + count):
            value = acc[m, t] + pbuf[m, t].astype(jnp.float32) + bias_row(column_of(t) // group)
            value = value.astype(jnp.bfloat16)
            for k in range(4):
                out_ref[k, where, :, t * LANES : (t + 1) * LANES] = value[k * tokens : (k + 1) * tokens]

    def step_bias():
        send_bias(False)

    def step_bias_wait():
        @pl.loop(1, devices)
        def _(step):
            slot = lax.rem(flat + step, devices)

            @pl.when(needs(slot, me))
            def _():
                arrived(bbuf.at[slot], b_recv.at[slot])

        bbuf[flat] = bias_own[...]

    def run(steps):
        for name, *args in steps:
            names[name](*args)

    names = dict(
        wp=step_wp,
        ox=step_ox,
        rx=step_rx,
        rw=step_rw,
        rc=step_rc,
        wc=step_wc,
        x1=step_x1,
        pm=step_pm,
        om=step_om,
        fin=step_fin,
        bias=step_bias,
        biasw=step_bias_wait,
    )
    first = [("wp", 0), ("ox", 0), ("ox", 1), ("ox", 2)]
    for_inner = [
        ("rx", z_near, True),
        ("rx", z_mate, False),
        ("rx", z_end, True),
        ("wp", 1),
        ("wp", 2),
        ("ox", 3),
        ("ox", 4),
        ("ox", 5),
        ("rw", 0),
        ("wp", 3),
        ("rc", 0),
        ("wc", 0),
        ("pm", 0, 0),
        ("wp", 4),
    ]
    for_outer = [
        ("rx", z_mate, False),
        ("wp", 1),
        ("wp", 2),
        ("ox", 3),
        ("ox", 4),
        ("ox", 5),
        ("rw", 0),
        ("rx", z_near, False),
        ("wp", 3),
        ("rc", 0),
        ("rx", z_end, False),
        ("wp", 4),
        ("wc", 0),
        ("pm", 0, 0),
    ]
    last = [
        ("rw", 1),
        ("rc", 1),
        ("wc", 1),
        ("pm", 0, 1),
        ("wp", 5),
        ("rw", 2),
        ("rc", 2),
        ("wc", 2),
        ("pm", 0, 2),
        ("bias",),
        ("x1",),
        ("pm", 1, 0),
        ("pm", 1, 1),
        ("pm", 1, 2),
        ("biasw",),
        ("rw", 3),
        ("rc", 3),
        ("rw", 4),
        ("rc", 4),
        ("wc", 3),
        ("om", 0, 0 + parts),
        ("om", 1, 0 + parts),
        ("rw", 5),
        ("rc", 5),
        ("wc", 4),
        ("om", 0, 1 + parts),
        ("om", 1, 1 + parts),
        ("wc", 5),
        ("om", 0, 2 + parts),
        ("om", 1, 2 + parts),
        ("fin", 0, 0),
        ("fin", 0, 1),
        ("fin", 0, 2),
        ("fin", 1, 0),
        ("fin", 1, 1),
        ("fin", 1, 2),
    ]
    mine = slot_of(inst, 0)
    run(first)
    wbuf[mine, :tiles] = wsend[rank_of(0, 0)]
    wbuf[mine, tiles:] = wsend[rank_of(0, parts)]
    each(inner, lambda: run(for_inner))
    each(jnp.logical_not(inner), lambda: run(for_outer))
    run(last)

    for piece in range(pieces):
        own_x(0, piece).wait_send()
        own_x(1, piece).wait_send()
        own_x(3, piece).wait_send()
        for block in (z_near, z_mate, z_end):
            relay_x(1, block, piece).wait_send()

        def mate_sends(piece=piece):
            relay_x(0, z_near, piece).wait_send()
            relay_x(0, z_end, piece).wait_send()

        each(inner, mate_sends)
    for j in range(2 * parts):
        for k in range(4):
            if k:
                w_copy(k, j).wait_send()
            wx_copy(k, j).wait_send()
            wc_copy(0, k, j).wait_send()
            wc_copy(1, k, j).wait_send()
    for m in range(2):
        for j in range(parts):
            p_copy(m, j).wait_send()
    send_bias(True)


def kernel_device(dims, tokens, norm_gain, master_qkv, qkv_bias):
    inst_count, shard_count, group = dims
    devices = inst_count * shard_count
    rows = master_qkv.shape[0]
    count, depth = tokens.shape
    tiles = master_qkv.shape[1] // TP // LANES
    pieces = TOKEN_PIECES
    parts = len(CHUNKS)
    dma = pltpu.SemaphoreType.DMA
    vmem = pl.BlockSpec(memory_space=pltpu.VMEM)
    anywhere = pl.BlockSpec(memory_space=pl.ANY)
    low, wide = jnp.bfloat16, jnp.float32
    result = pl.pallas_call(
        functools.partial(kernel, dims),
        out_shape=jax.ShapeDtypeStruct((4, 2, count, tiles * LANES), low),
        in_specs=[anywhere, vmem, anywhere, vmem],
        out_specs=vmem,
        scratch_shapes=[
            pltpu.VMEM((count, depth), low),
            pltpu.VMEM((rows, master_qkv.shape[1]), wide),
            pltpu.VMEM((2, count, depth // 2), low),
            pltpu.VMEM((2, 4, count, depth // 2), low),
            pltpu.VMEM((TP, tiles, rows, LANES), low),
            pltpu.VMEM((4 * inst_count, 2 * tiles, rows, LANES), low),
            pltpu.VMEM((2, tiles, 4 * count, LANES), low),
            pltpu.VMEM((2, tiles, 4 * count, LANES), low),
            pltpu.VMEM((2, tiles, 4 * count, LANES), wide),
            pltpu.VMEM((8, LANES), wide),
            pltpu.VMEM((devices, 8, LANES), wide),
            dma((2,)),
            dma((2, 4, pieces)),
            dma((4, pieces)),
            dma((2, 4, pieces)),
            dma((4 * inst_count, 2 * parts)),
            dma((3, 2 * parts)),
            dma((4, 2 * parts)),
            dma((2, 4, 2 * parts)),
            dma((2, parts)),
            dma((2, parts)),
            dma((devices,)),
            dma((devices,)),
        ],
        compiler_params=pltpu.CompilerParams(
            collective_id=0, has_side_effects=True, vmem_limit_bytes=60 * 1024 * 1024
        ),
    )(tokens, norm_gain.reshape(1, rows), master_qkv, qkv_bias.reshape(1, -1))
    return result.reshape(1, shard_count * count, tiles * LANES)


def per_device(tokens, norm_gain, master_qkv, qkv_bias):
    inst_count, shard_count = lax.axis_size("inst"), lax.axis_size("shard")
    group = 32
    fits = (
        shard_count == TP
        and inst_count == 4
        and master_qkv.shape[0] % 16 == 0
        and tokens.shape[0] % (16 * TOKEN_PIECES) == 0
        and QHEADS * HEAD_DIM // TP % LANES == 0
        and KVHEADS * HEAD_DIM // TP == LANES
        and 4 * master_qkv.shape[0] % LANES == 0
        and qkv_bias.shape[0] % group == 0
    )
    if fits:
        return kernel_device((inst_count, shard_count, group), tokens, norm_gain, master_qkv, qkv_bias)
    return general_device(tokens, norm_gain, master_qkv, qkv_bias)


def solution(mesh):
    in_specs = (
        P(("inst", "shard"), None),
        P(("inst", "shard")),
        P(("inst", "shard"), None),
        P(("inst", "shard")),
    )
    out_specs = P(("inst", "shard"), None, None)
    return jax.shard_map(
        per_device, mesh=mesh, in_specs=in_specs, out_specs=out_specs, check_vma=False
    )
```

```python
import functools

import jax
import jax.numpy as jnp
from jax import lax
from jax.experimental import pallas as pl
from jax.experimental.pallas import tpu as pltpu
from jax.sharding import PartitionSpec as P

QHEADS = 40
KVHEADS = 8
HEAD_DIM = 128
TP = 8


EPSILON = 1e-06
MESH = pl.DeviceIdType.MESH
LANES = 128
TOKEN_PIECES = 2
CHUNKS = ((0, 2), (2, 4), (4, 7))


def partner_2(value, axis, distance):
    mask = 2**distance
    pairs = [(source, source ^ mask) for source in range(lax.axis_size(axis))]
    return lax.ppermute(value, axis, pairs)


def rank_columns(matrix):
    query_cols = QHEADS * HEAD_DIM
    pair_cols = KVHEADS * HEAD_DIM
    leading = matrix.shape[:-1]
    query = matrix[..., :query_cols].reshape(leading + (TP, query_cols // TP))
    keys = matrix[..., query_cols : query_cols + pair_cols].reshape(leading + (TP, pair_cols // TP))
    values = matrix[..., query_cols + pair_cols :].reshape(leading + (TP, pair_cols // TP))
    return jnp.concatenate([query, keys, values], axis=-1)


def normalize(tokens, gain):
    floats = tokens.astype(jnp.float32)
    scale = lax.rsqrt(jnp.mean(floats * floats, axis=-1, keepdims=True) + EPSILON)
    return (floats * scale * gain.astype(jnp.float32)).astype(jnp.bfloat16)


def general_device(tokens, norm_gain, master_qkv, qkv_bias):
    shard_count = lax.axis_size("shard")
    local_rows = master_qkv.shape[0]
    rank_width = master_qkv.shape[1] // TP
    gain_full, bias_full = (
        lax.all_gather(norm_gain.astype(jnp.bfloat16), ("inst", "shard"), axis=0, tiled=True),
        lax.all_gather(qkv_bias.astype(jnp.bfloat16), ("inst", "shard"), axis=0, tiled=True),
    )
    normed = normalize(tokens, gain_full)
    shard_pos = lax.axis_index("shard")
    rank_index = shard_pos % TP
    bit_count = TP.bit_length() - 1
    bit_order = list(range(bit_count))
    group_rows = normed
    for bit_pos in bit_order:
        partner = partner_2(group_rows, "shard", bit_pos)
        lower = jnp.bitwise_and(jnp.right_shift(shard_pos, bit_pos), 1) == 0
        group_rows = jnp.where(
            lower,
            jnp.concatenate([group_rows, partner], 0),
            jnp.concatenate([partner, group_rows], 0),
        )
    copies = shard_count // TP
    inst_block = shard_count * local_rows
    rows_low = master_qkv.astype(jnp.bfloat16)
    ranked = jnp.transpose(rank_columns(rows_low), (1, 0, 2))
    spread = jnp.broadcast_to(ranked[None], (copies,) + ranked.shape)
    outgoing = spread.reshape(shard_count, rows_low.shape[0], rank_width)
    arrived = lax.all_to_all(outgoing, "shard", split_axis=0, concat_axis=0, tiled=True).reshape(
        inst_block, rank_width
    )
    product = jnp.dot(
        group_rows,
        lax.all_gather(arrived, "inst", axis=0, tiled=True),
        preferred_element_type=jnp.float32,
    )
    bias_ranks = rank_columns(bias_full)
    bias_mine = lax.dynamic_index_in_dim(bias_ranks, rank_index, 0, keepdims=False)
    result = (product + bias_mine.astype(jnp.float32)).astype(jnp.bfloat16)
    return result[None]


def kernel(
    dims,
    tok_hbm,
    gain_ref,
    w_hbm,
    bias_ref,
    out_ref,
    tok_ref,
    w_ref,
    xsend,
    xbuf,
    wsend,
    wbuf,
    psend,
    pbuf,
    acc,
    bias_own,
    bbuf,
    load_sem,
    x_recv,
    x_send,
    x_relay,
    w_recv,
    w_send,
    wx_send,
    wc_send,
    p_recv,
    p_send,
    b_recv,
    b_send,
):
    inst_count, shard_count, group = dims
    devices = inst_count * shard_count
    inst = lax.axis_index("inst")
    me = lax.axis_index("shard")
    z = me // 2
    y = lax.rem(me, 2)
    half = z // 2
    flat = inst * shard_count + me
    core_peer = inst + 1 - 2 * lax.rem(inst, 2)
    x_peer = lax.rem(inst + 2, inst_count)
    far_core = lax.rem(core_peer + 2, inst_count)
    z_mate = z + 1 - 2 * lax.rem(z, 2)
    z_pair = lax.rem(z + 2, 4)
    z_near = 2 - half
    z_end = 3 - 3 * half
    inner = z_near + z == 3
    rows = w_ref.shape[0]
    tokens, depth = tok_ref.shape
    tiles = wsend.shape[1]
    half_block = 4 * rows
    pieces = TOKEN_PIECES
    piece_rows = tokens // pieces
    parts = len(CHUNKS)

    token_load = pltpu.make_async_copy(tok_hbm, tok_ref, load_sem.at[0])
    weight_load = pltpu.make_async_copy(w_hbm, w_ref, load_sem.at[1])
    token_load.start()
    weight_load.start()

    barrier = pltpu.get_barrier_semaphore()

    @pl.loop(1, devices)
    def _(step):
        there = lax.rem(flat + step, devices)
        pl.semaphore_signal(
            barrier,
            inc=1,
            device_id=(there // shard_count, lax.rem(there, shard_count)),
            device_id_type=MESH,
        )

    def remote(source, target, send_sem, recv_sem, device):
        return pltpu.make_async_remote_copy(
            src_ref=source,
            dst_ref=target,
            send_sem=send_sem,
            recv_sem=recv_sem,
            device_id=device,
            device_id_type=MESH,
        )

    def each(condition, action):
        pl.when(condition)(action)

    def piece_of(ref, piece):
        return ref.at[pl.ds(piece * piece_rows, piece_rows)]

    def own_x(way, piece):
        which, device, side = (
            (half, z_mate * 2 + y, 0),
            (1 - half, z_near * 2 + y, 0),
            (1 - half, z_pair * 2 + y, 0),
            (half, z * 2 + 1 - y, 1),
        )[way]
        return remote(
            piece_of(xsend.at[which], piece),
            piece_of(xbuf.at[side, z], piece),
            x_send.at[way, piece],
            x_recv.at[side, z, piece],
            (inst, device),
        )

    def relay_x(way, block, piece):
        device, side = ((z_mate * 2 + y, 0), (z * 2 + 1 - y, 1))[way]
        return remote(
            piece_of(xbuf.at[0, block], piece),
            piece_of(xbuf.at[side, block], piece),
            x_relay.at[way, block, piece],
            x_recv.at[side, block, piece],
            (inst, device),
        )

    def place(k):
        dz, dy = k // 2, k % 2
        return (z_mate if dz else z), (1 - y if dy else y)

    def slot_of(owner, k):
        pz, py = place(k)
        return owner * 4 + lax.rem(pz, 2) * 2 + py

    def tiles_of(j):
        first, last = CHUNKS[j % parts]
        return first, last - first, (j // parts) * tiles + first

    def rank_of(k, j):
        pz, py = place(k)
        return (pz if j >= parts else lax.rem(pz + 2, 4)) * 2 + py

    def fresh(k, j):
        first, count, _ = tiles_of(j)
        return wsend.at[rank_of(k, j), pl.ds(first, count)]

    def held(slot, j):
        _, count, first = tiles_of(j)
        return wbuf.at[slot, pl.ds(first, count)]

    def w_copy(k, j):
        pz, py = place(k)
        slot = slot_of(inst, 0)
        return remote(fresh(k, j), held(slot, j), w_send.at[k - 1, j], w_recv.at[slot, j], (inst, pz * 2 + py))

    def wx_copy(k, j):
        slot = slot_of(inst, k)
        source = held(slot, j) if k else fresh(0, j)
        return remote(source, held(slot, j), wx_send.at[k, j], w_recv.at[slot, j], (x_peer, me))

    def wc_copy(side, k, j):
        slot = slot_of((inst, x_peer)[side], k)
        source = held(slot, j) if k or side else fresh(0, j)
        return remote(source, held(slot, j), wc_send.at[side, k, j], w_recv.at[slot, j], (core_peer, me))

    def p_copy(m, j):
        first, count, _ = tiles_of(j)
        return remote(
            psend.at[m, pl.ds(first, count)],
            pbuf.at[m, pl.ds(first, count)],
            p_send.at[m, j],
            p_recv.at[m, j],
            (inst, z_pair * 2 + y),
        )

    def arrived(ref, sem):
        pltpu.make_async_copy(ref, ref, sem).wait()

    def wait_x(side, block, piece):
        arrived(piece_of(xbuf.at[side, block], piece), x_recv.at[side, block, piece])

    def wait_w(slot, j):
        arrived(held(slot, j), w_recv.at[slot, j])

    query = QHEADS * HEAD_DIM // TP
    pair = KVHEADS * HEAD_DIM // TP
    held_bias = bias_ref.shape[1]
    per_row = LANES // group
    groups = held_bias // group

    def needs(owner, rank):
        low, high = owner * held_bias, owner * held_bias + held_bias
        result = None
        for start, extent in (
            (rank * query, query),
            (TP * query + rank * pair, pair),
            (TP * (query + pair) + rank * pair, pair),
        ):
            overlap = jnp.logical_and(start < high, low < start + extent)
            result = overlap if result is None else jnp.logical_or(result, overlap)
        return result

    def bias_copy(step):
        there = lax.rem(flat + step, devices)
        return remote(
            bias_own,
            bbuf.at[flat],
            b_send.at[step],
            b_recv.at[flat],
            (there // shard_count, lax.rem(there, shard_count)),
        )

    def send_bias(finish):
        @pl.loop(1, devices)
        def _(step):
            there = lax.rem(flat + step, devices)

            @pl.when(needs(flat, lax.rem(there, shard_count)))
            def _():
                if finish:
                    bias_copy(step).wait_send()
                else:
                    bias_copy(step).start()

    def bias_row(number_first):
        lane = lax.broadcasted_iota(jnp.int32, (1, LANES), 1) // group
        row = jnp.zeros((1, LANES), jnp.float32)
        for q in range(per_row):
            number = number_first + q
            row = jnp.where(lane == q, bbuf[number // groups, pl.ds(lax.rem(number, groups), 1), :], row)
        return row

    def column_of(t):
        at = t * LANES
        if at < query:
            return me * query + at
        if at < query + pair:
            return TP * query + me * pair + (at - query)
        return TP * (query + pair) + me * pair + (at - query - pair)

    ids = lax.broadcasted_iota(jnp.int32, (rows, rows), 0), lax.broadcasted_iota(jnp.int32, (rows, rows), 1)
    gain_row = gain_ref[...].astype(jnp.bfloat16).astype(jnp.float32)
    gain = jnp.sum(jnp.where(ids[0] == ids[1], jnp.broadcast_to(gain_row, (rows, rows)), 0.0), axis=1, keepdims=True)
    group_id = lax.broadcasted_iota(jnp.int32, (8, held_bias), 0)
    lane_id = lax.broadcasted_iota(jnp.int32, (8, held_bias), 1)
    spread = jnp.where(lane_id // group == group_id, jnp.broadcast_to(bias_ref[...], (8, held_bias)), 0.0)
    from_id = lax.broadcasted_iota(jnp.int32, (held_bias, LANES), 0)
    to_id = lax.broadcasted_iota(jnp.int32, (held_bias, LANES), 1)
    pick = jnp.where(lax.rem(from_id, group) == lax.rem(to_id, group), 1.0, 0.0).astype(jnp.bfloat16)
    bias_own[...] = jnp.dot(spread.astype(jnp.bfloat16), pick, preferred_element_type=jnp.float32)

    token_load.wait()
    step_rows = 16
    for first in range(0, tokens, step_rows):
        values = tok_ref[first : first + step_rows, :].astype(jnp.float32)
        mean = jnp.sum(values * values, axis=-1, keepdims=True) * (1.0 / depth)
        scaled = (values * lax.rsqrt(mean + EPSILON)).astype(jnp.bfloat16)
        for which in range(2):
            for owner in range(inst_count):
                at = (owner * 2 + which) * half_block
                xsend[which, first : first + step_rows, owner * half_block : (owner + 1) * half_block] = scaled[
                    :, at : at + half_block
                ]
    pl.semaphore_wait(barrier, devices - 1)

    send_bias(False)
    for piece in range(pieces):
        own_x(1, piece).start()
        own_x(0, piece).start()
    xbuf[0, z] = xsend[half]

    weight_load.wait()
    for rank in range(TP):
        starts = (
            (rank * query, 0, query),
            (TP * query + rank * pair, query, pair),
            (TP * (query + pair) + rank * pair, query + pair, pair),
        )
        for source, target, extent in starts:
            for inside in range(0, extent, LANES):
                part = w_ref[:, source + inside : source + inside + LANES].astype(jnp.bfloat16).astype(jnp.float32)
                wsend[rank, (target + inside) // LANES] = (part * gain).astype(jnp.bfloat16)

    def product(m, j):
        first, count, at = tiles_of(j)
        lhs = xbuf[m].reshape(4 * tokens, 4 * half_block)
        result = []
        for t in range(0, count, 2):
            width = min(2, count - t)
            rhs = [wbuf[:, at + t + u].reshape(4 * half_block, LANES) for u in range(width)]
            rhs = jnp.concatenate(rhs, axis=1) if width > 1 else rhs[0]
            value = jnp.dot(lhs, rhs, preferred_element_type=jnp.float32)
            for u in range(width):
                result.append((first + t + u, value[:, u * LANES : (u + 1) * LANES]))
        return result

    def step_wp(j, *ks):
        for k in ks:
            w_copy(k, j).start()

    def step_ox(j):
        wx_copy(0, j).start()
        wc_copy(0, 0, j).start()

    def step_xy():
        for piece in range(pieces):
            own_x(3, piece).start()

    def step_rx(block, to_mate):
        for piece in range(pieces):
            wait_x(0, block, piece)
            if to_mate:
                relay_x(0, block, piece).start()

    def step_ry(block):
        for piece in range(pieces):
            relay_x(1, block, piece).start()

    def step_rw(j, *ks):
        for k in ks:
            wait_w(slot_of(inst, k), j)
            wx_copy(k, j).start()
            wc_copy(0, k, j).start()

    def step_rc(j, *ks):
        for k in ks:
            wait_w(slot_of(x_peer, k), j)
            wc_copy(1, k, j).start()

    def step_wc(j):
        for k in range(4):
            wait_w(slot_of(core_peer, k), j)
            wait_w(slot_of(far_core, k), j)

    def step_x1():
        for k in range(4):
            for piece in range(pieces):
                wait_x(1, k, piece)

    def step_pm(m, j):
        for t, value in product(m, j):
            psend[m, t] = value.astype(jnp.bfloat16)
        p_copy(m, j).start()

    def step_om(m, j):
        for t, value in product(m, j):
            acc[m, t] = value

    def step_fin(m, j):
        first, count, _ = tiles_of(j)
        arrived(pbuf.at[m, pl.ds(first, count)], p_recv.at[m, j])
        where = 1 - y if m else y
        for t in range(first, first + count):
            value = acc[m, t] + pbuf[m, t].astype(jnp.float32) + bias_row(column_of(t) // group)
            value = value.astype(jnp.bfloat16)
            for k in range(4):
                out_ref[k, where, :, t * LANES : (t + 1) * LANES] = value[k * tokens : (k + 1) * tokens]

    def step_bias_wait():
        @pl.loop(1, devices)
        def _(step):
            slot = lax.rem(flat + step, devices)

            @pl.when(needs(slot, me))
            def _():
                arrived(bbuf.at[slot], b_recv.at[slot])

        bbuf[flat] = bias_own[...]

    def run(steps):
        for name, *args in steps:
            names[name](*args)

    def run(steps):
        for name, *args in steps:
            names[name](*args)

    names = dict(
        wp=step_wp,
        ox=step_ox,
        xy=step_xy,
        rx=step_rx,
        ry=step_ry,
        rw=step_rw,
        rc=step_rc,
        wc=step_wc,
        x1=step_x1,
        pm=step_pm,
        om=step_om,
        fin=step_fin,
        biasw=step_bias_wait,
    )
    every = (0, 2, 1, 3)
    both_first = [
        ("wp", 0, 2, 3, 1),
        ("ox", 0),
        ("ox", 1),
        ("ox", 2),
        ("wp", 1, 1),
        ("wp", 2, 1),
        ("xy",),
    ]
    for_inner = [
        ("wp", 1, 2, 3),
        ("rw", 0, 1),
        ("rw", 0, 2, 3),
        ("rw", 1, 1),
        ("rw", 2, 1),
        ("rx", z_near, True),
        ("rx", z_end, True),
        ("rc", 0, *every),
        ("wp", 2, 2, 3),
        ("rx", z_mate, False),
        ("ry", z_near),
        ("ry", z_end),
        ("ry", z_mate),
        ("wc", 0),
        ("pm", 0, 0),
        ("ox", 3),
        ("rw", 1, 2, 3),
        ("wp", 3, 2, 3, 1),
        ("wp", 4, 2, 3, 1),
        ("wp", 5, 2, 3, 1),
        ("rc", 1, *every),
        ("wc", 1),
        ("pm", 0, 1),
        ("rw", 2, 2, 3),
        ("ox", 4),
        ("ox", 5),
        ("rc", 2, *every),
        ("wc", 2),
        ("pm", 0, 2),
    ]
    for_outer = [
        ("wp", 1, 2, 3),
        ("wp", 2, 2, 3),
        ("rw", 0, 1),
        ("rx", z_mate, False),
        ("ry", z_mate),
        ("rw", 0, 2, 3),
        ("rw", 1, 1),
        ("rw", 2, 1),
        ("rc", 0, *every),
        ("rw", 1, 2, 3),
        ("ox", 3),
        ("wp", 3, 2, 3, 1),
        ("wp", 4, 2, 3, 1),
        ("wp", 5, 2, 3, 1),
        ("rc", 1, *every),
        ("rx", z_near, False),
        ("ry", z_near),
        ("rx", z_end, False),
        ("ry", z_end),
        ("wc", 0),
        ("pm", 0, 0),
        ("wc", 1),
        ("pm", 0, 1),
        ("rw", 2, 2, 3),
        ("ox", 4),
        ("ox", 5),
        ("rc", 2, *every),
        ("wc", 2),
        ("pm", 0, 2),
    ]
    both_last = [
        ("rw", 3, 1, 2, 3),
        ("x1",),
        ("pm", 1, 0),
        ("pm", 1, 1),
        ("pm", 1, 2),
        ("rc", 3, *every),
        ("rw", 4, 1, 2, 3),
        ("rc", 4, *every),
        ("wc", 3),
        ("om", 0, 0 + parts),
        ("om", 1, 0 + parts),
        ("rw", 5, 1, 2, 3),
        ("rc", 5, *every),
        ("wc", 4),
        ("om", 0, 1 + parts),
        ("om", 1, 1 + parts),
        ("biasw",),
        ("fin", 0, 0),
        ("fin", 0, 1),
        ("wc", 5),
        ("om", 0, 2 + parts),
        ("om", 1, 2 + parts),
        ("fin", 0, 2),
        ("fin", 1, 0),
        ("fin", 1, 1),
        ("fin", 1, 2),
    ]
    mine = slot_of(inst, 0)
    run(both_first)
    wbuf[mine, :tiles] = wsend[rank_of(0, 0)]
    wbuf[mine, tiles:] = wsend[rank_of(0, parts)]
    each(inner, lambda: run(for_inner))
    each(jnp.logical_not(inner), lambda: run(for_outer))
    run(both_last)

    for piece in range(pieces):
        own_x(0, piece).wait_send()
        own_x(1, piece).wait_send()
        own_x(3, piece).wait_send()
        for block in (z_near, z_mate, z_end):
            relay_x(1, block, piece).wait_send()

        def mate_sends(piece=piece):
            relay_x(0, z_near, piece).wait_send()
            relay_x(0, z_end, piece).wait_send()

        each(inner, mate_sends)
    for j in range(2 * parts):
        for k in range(4):
            if k:
                w_copy(k, j).wait_send()
            wx_copy(k, j).wait_send()
            wc_copy(0, k, j).wait_send()
            wc_copy(1, k, j).wait_send()
    for m in range(2):
        for j in range(parts):
            p_copy(m, j).wait_send()
    send_bias(True)


def kernel_device(dims, tokens, norm_gain, master_qkv, qkv_bias):
    inst_count, shard_count, group = dims
    devices = inst_count * shard_count
    rows = master_qkv.shape[0]
    count, depth = tokens.shape
    tiles = master_qkv.shape[1] // TP // LANES
    pieces = TOKEN_PIECES
    parts = len(CHUNKS)
    dma = pltpu.SemaphoreType.DMA
    vmem = pl.BlockSpec(memory_space=pltpu.VMEM)
    anywhere = pl.BlockSpec(memory_space=pl.ANY)
    low, wide = jnp.bfloat16, jnp.float32
    result = pl.pallas_call(
        functools.partial(kernel, dims),
        out_shape=jax.ShapeDtypeStruct((4, 2, count, tiles * LANES), low),
        in_specs=[anywhere, vmem, anywhere, vmem],
        out_specs=vmem,
        scratch_shapes=[
            pltpu.VMEM((count, depth), low),
            pltpu.VMEM((rows, master_qkv.shape[1]), wide),
            pltpu.VMEM((2, count, depth // 2), low),
            pltpu.VMEM((2, 4, count, depth // 2), low),
            pltpu.VMEM((TP, tiles, rows, LANES), low),
            pltpu.VMEM((4 * inst_count, 2 * tiles, rows, LANES), low),
            pltpu.VMEM((2, tiles, 4 * count, LANES), low),
            pltpu.VMEM((2, tiles, 4 * count, LANES), low),
            pltpu.VMEM((2, tiles, 4 * count, LANES), wide),
            pltpu.VMEM((8, LANES), wide),
            pltpu.VMEM((devices, 8, LANES), wide),
            dma((2,)),
            dma((2, 4, pieces)),
            dma((4, pieces)),
            dma((2, 4, pieces)),
            dma((4 * inst_count, 2 * parts)),
            dma((3, 2 * parts)),
            dma((4, 2 * parts)),
            dma((2, 4, 2 * parts)),
            dma((2, parts)),
            dma((2, parts)),
            dma((devices,)),
            dma((devices,)),
        ],
        compiler_params=pltpu.CompilerParams(
            collective_id=0, has_side_effects=True, vmem_limit_bytes=60 * 1024 * 1024
        ),
    )(tokens, norm_gain.reshape(1, rows), master_qkv, qkv_bias.reshape(1, -1))
    return result.reshape(1, shard_count * count, tiles * LANES)


def per_device(tokens, norm_gain, master_qkv, qkv_bias):
    inst_count, shard_count = lax.axis_size("inst"), lax.axis_size("shard")
    group = 32
    fits = (
        shard_count == TP
        and inst_count == 4
        and master_qkv.shape[0] % 16 == 0
        and tokens.shape[0] % (16 * TOKEN_PIECES) == 0
        and QHEADS * HEAD_DIM // TP % LANES == 0
        and KVHEADS * HEAD_DIM // TP == LANES
        and 4 * master_qkv.shape[0] % LANES == 0
        and qkv_bias.shape[0] % group == 0
    )
    if fits:
        return kernel_device((inst_count, shard_count, group), tokens, norm_gain, master_qkv, qkv_bias)
    return general_device(tokens, norm_gain, master_qkv, qkv_bias)


def solution(mesh):
    in_specs = (
        P(("inst", "shard"), None),
        P(("inst", "shard")),
        P(("inst", "shard"), None),
        P(("inst", "shard")),
    )
    out_specs = P(("inst", "shard"), None, None)
    return jax.shard_map(
        per_device, mesh=mesh, in_specs=in_specs, out_specs=out_specs, check_vma=False
    )
```

```python
import functools

import jax
import jax.numpy as jnp
from jax import lax
from jax.experimental import pallas as pl
from jax.experimental.pallas import tpu as pltpu
from jax.sharding import PartitionSpec as P

QHEADS = 40
KVHEADS = 8
HEAD_DIM = 128
TP = 8


EPSILON = 1e-06
MESH = pl.DeviceIdType.MESH
LANES = 128
TOKEN_PIECES = 2
CHUNKS = (
    (("far", 0, 2), ("far", 2, 2), ("far", 4, 3), ("extra", 5, 2), ("own", 0, 2), ("own", 2, 3), ("own", 5, 2)),
    (("far", 0, 2), ("far", 2, 3), ("own", 0, 2), ("own", 2, 2), ("own", 4, 3)),
)
INNER = (
    ("xm", 1, 0),
    ("xf", 1, 0),
    ("xf", 0, 0),
    ("xy", 1, 0),
    ("wp", 0, 2),
    ("wp", 1, 1),
    ("ox", 0, 0),
    ("ox", 1, 0),
    ("ko", 0, 0),
    ("ox", 6, 0),
    ("ko", 1, 0),
    ("wp", 3, 1),
    ("bias", 0, 0),
    ("rc", 0, 0),
    ("ox", 3, 0),
    ("ko", 6, 0),
    ("rx", 2, 1),
    ("wp", 2, 1),
    ("rc", 1, 0),
    ("ox", 2, 0),
    ("ko", 3, 0),
    ("rc", 6, 0),
    ("ko", 2, 0),
    ("rx", 2, 0),
    ("ry", 2, 0),
    ("rw", 3, 1),
    ("wd", 1, 0),
    ("rc", 3, 0),
    ("ox", 4, 0),
    ("kw", 3, 1),
    ("rd", 1, 0),
    ("wd", 0, 0),
    ("rc", 2, 0),
    ("rw", 1, 1),
    ("ko", 4, 0),
    ("rd", 3, 0),
    ("rc", 3, 1),
    ("rw", 3, 2),
    ("kw", 1, 1),
    ("wp", 1, 2),
    ("rc", 4, 0),
    ("kw", 3, 2),
    ("ry", 3, 0),
    ("xm", 0, 0),
    ("wp", 6, 1),
    ("rw", 0, 2),
    ("rc", 1, 1),
    ("kw", 0, 2),
    ("rw", 1, 2),
    ("rx", 3, 0),
    ("rc", 3, 2),
    ("rw", 3, 3),
    ("kw", 1, 2),
    ("wp", 0, 1),
    ("rc", 0, 2),
    ("rw", 1, 3),
    ("kw", 3, 3),
    ("wp", 4, 1),
    ("rc", 1, 2),
    ("ox", 5, 0),
    ("kw", 1, 3),
    ("rx", 3, 1),
    ("ry", 2, 1),
    ("rc", 3, 3),
    ("ko", 5, 0),
    ("ry", 1, 1),
    ("pm", 0, 3),
    ("wp", 4, 2),
    ("rc", 1, 3),
    ("rw", 4, 1),
    ("kw", 4, 1),
    ("pm", 0, 1),
    ("rw", 2, 2),
    ("rc", 5, 0),
    ("rw", 2, 1),
    ("kw", 2, 2),
    ("wp", 3, 2),
    ("rc", 4, 1),
    ("rd", 5, 0),
    ("rw", 0, 1),
    ("kw", 2, 1),
    ("rc", 2, 2),
    ("rd", 2, 0),
    ("rw", 6, 1),
    ("kw", 0, 1),
    ("wp", 2, 2),
    ("rd", 0, 0),
    ("rc", 2, 1),
    ("kw", 6, 1),
    ("rw", 5, 3),
    ("wd", 3, 0),
    ("wp", 5, 1),
    ("rc", 0, 1),
    ("kw", 5, 3),
    ("wd", 2, 0),
    ("rw", 2, 3),
    ("ry", 3, 1),
    ("rc", 6, 1),
    ("wd", 4, 0),
    ("kw", 2, 3),
    ("rw", 0, 3),
    ("xy", 0, 0),
    ("rc", 5, 3),
    ("kw", 0, 3),
    ("rw", 5, 1),
    ("rc", 2, 3),
    ("kw", 5, 1),
    ("ry", 1, 0),
    ("pm", 0, 2),
    ("rc", 0, 3),
    ("pm", 0, 0),
    ("rc", 5, 1),
    ("rw", 4, 2),
    ("kw", 4, 2),
    ("rw", 5, 2),
    ("kw", 5, 2),
    ("pm", 1, 0),
    ("rc", 4, 2),
    ("pm", 1, 1),
    ("rd", 4, 0),
    ("pm", 1, 2),
    ("rw", 6, 2),
    ("kw", 6, 2),
    ("pm", 1, 3),
    ("rc", 5, 2),
    ("rw", 4, 3),
    ("rd", 6, 0),
    ("kw", 4, 3),
    ("om", 0, 5),
    ("rc", 6, 2),
    ("om", 1, 5),
    ("rw", 6, 3),
    ("rc", 4, 3),
    ("kw", 6, 3),
    ("fin", 0, 5),
    ("fin", 1, 5),
    ("om", 0, 4),
    ("om", 1, 4),
    ("fin", 0, 4),
    ("fin", 1, 4),
    ("rc", 6, 3),
    ("om", 0, 6),
    ("om", 1, 6),
    ("fin", 0, 6),
    ("fin", 1, 6),
)
OUTER = (
    ("xm", 0, 0),
    ("xy", 1, 0),
    ("wp", 3, 2),
    ("wp", 0, 1),
    ("ox", 2, 0),
    ("ox", 0, 0),
    ("ko", 2, 0),
    ("ox", 3, 0),
    ("ko", 0, 0),
    ("wd", 3, 0),
    ("bias", 0, 0),
    ("rc", 2, 0),
    ("ox", 4, 0),
    ("ko", 3, 0),
    ("ry", 1, 1),
    ("wd", 0, 0),
    ("wp", 1, 1),
    ("rc", 0, 0),
    ("ko", 4, 0),
    ("rw", 0, 2),
    ("wd", 1, 0),
    ("rc", 3, 0),
    ("xf", 0, 0),
    ("rw", 0, 1),
    ("kw", 0, 2),
    ("ry", 2, 1),
    ("wp", 0, 2),
    ("rc", 4, 0),
    ("ox", 1, 0),
    ("rc", 0, 2),
    ("ko", 1, 0),
    ("rw", 1, 1),
    ("ry", 2, 0),
    ("wp", 1, 2),
    ("rc", 0, 1),
    ("kw", 0, 1),
    ("kw", 1, 1),
    ("xf", 1, 0),
    ("rd", 1, 0),
    ("rc", 1, 0),
    ("xm", 1, 0),
    ("rd", 0, 0),
    ("rc", 1, 1),
    ("rw", 1, 2),
    ("kw", 1, 2),
    ("wp", 2, 2),
    ("xy", 0, 0),
    ("rw", 1, 3),
    ("kw", 1, 3),
    ("ry", 1, 0),
    ("rw", 0, 3),
    ("wd", 5, 0),
    ("rc", 1, 2),
    ("kw", 0, 3),
    ("wd", 2, 0),
    ("rc", 1, 3),
    ("ry", 3, 0),
    ("rc", 0, 3),
    ("ry", 3, 1),
    ("pm", 0, 0),
    ("pm", 0, 1),
    ("wp", 2, 1),
    ("rw", 4, 2),
    ("kw", 4, 2),
    ("wp", 4, 1),
    ("pm", 1, 0),
    ("wp", 3, 1),
    ("rw", 3, 2),
    ("pm", 1, 1),
    ("kw", 3, 2),
    ("rw", 2, 1),
    ("rc", 4, 2),
    ("rw", 2, 2),
    ("kw", 2, 1),
    ("rd", 3, 0),
    ("rc", 3, 2),
    ("kw", 2, 2),
    ("rw", 4, 1),
    ("wp", 4, 2),
    ("rd", 2, 0),
    ("rc", 2, 1),
    ("kw", 4, 1),
    ("rw", 3, 1),
    ("rc", 2, 2),
    ("rd", 4, 0),
    ("kw", 3, 1),
    ("wp", 5, 2),
    ("rw", 2, 3),
    ("rc", 4, 1),
    ("rw", 3, 3),
    ("kw", 2, 3),
    ("wd", 4, 0),
    ("rc", 3, 1),
    ("kw", 3, 3),
    ("rw", 4, 3),
    ("wp", 6, 2),
    ("rc", 2, 3),
    ("kw", 4, 3),
    ("om", 0, 2),
    ("wd", 6, 0),
    ("rc", 3, 3),
    ("om", 1, 2),
    ("om", 0, 3),
    ("om", 1, 3),
    ("rc", 4, 3),
    ("fin", 0, 3),
    ("fin", 0, 2),
    ("om", 0, 4),
    ("om", 1, 4),
    ("fin", 0, 4),
    ("fin", 1, 2),
    ("fin", 1, 4),
    ("fin", 1, 3),
)


def partner_2(value, axis, distance):
    mask = 2**distance
    pairs = [(source, source ^ mask) for source in range(lax.axis_size(axis))]
    return lax.ppermute(value, axis, pairs)


def rank_columns(matrix):
    query_cols = QHEADS * HEAD_DIM
    pair_cols = KVHEADS * HEAD_DIM
    leading = matrix.shape[:-1]
    query = matrix[..., :query_cols].reshape(leading + (TP, query_cols // TP))
    keys = matrix[..., query_cols : query_cols + pair_cols].reshape(leading + (TP, pair_cols // TP))
    values = matrix[..., query_cols + pair_cols :].reshape(leading + (TP, pair_cols // TP))
    return jnp.concatenate([query, keys, values], axis=-1)


def normalize(tokens, gain):
    floats = tokens.astype(jnp.float32)
    scale = lax.rsqrt(jnp.mean(floats * floats, axis=-1, keepdims=True) + EPSILON)
    return (floats * scale * gain.astype(jnp.float32)).astype(jnp.bfloat16)


def general_device(tokens, norm_gain, master_qkv, qkv_bias):
    shard_count = lax.axis_size("shard")
    local_rows = master_qkv.shape[0]
    rank_width = master_qkv.shape[1] // TP
    gain_full, bias_full = (
        lax.all_gather(norm_gain.astype(jnp.bfloat16), ("inst", "shard"), axis=0, tiled=True),
        lax.all_gather(qkv_bias.astype(jnp.bfloat16), ("inst", "shard"), axis=0, tiled=True),
    )
    normed = normalize(tokens, gain_full)
    shard_pos = lax.axis_index("shard")
    rank_index = shard_pos % TP
    bit_count = TP.bit_length() - 1
    bit_order = list(range(bit_count))
    group_rows = normed
    for bit_pos in bit_order:
        partner = partner_2(group_rows, "shard", bit_pos)
        lower = jnp.bitwise_and(jnp.right_shift(shard_pos, bit_pos), 1) == 0
        group_rows = jnp.where(
            lower,
            jnp.concatenate([group_rows, partner], 0),
            jnp.concatenate([partner, group_rows], 0),
        )
    copies = shard_count // TP
    inst_block = shard_count * local_rows
    rows_low = master_qkv.astype(jnp.bfloat16)
    ranked = jnp.transpose(rank_columns(rows_low), (1, 0, 2))
    spread = jnp.broadcast_to(ranked[None], (copies,) + ranked.shape)
    outgoing = spread.reshape(shard_count, rows_low.shape[0], rank_width)
    arrived = lax.all_to_all(outgoing, "shard", split_axis=0, concat_axis=0, tiled=True).reshape(
        inst_block, rank_width
    )
    product = jnp.dot(
        group_rows,
        lax.all_gather(arrived, "inst", axis=0, tiled=True),
        preferred_element_type=jnp.float32,
    )
    bias_ranks = rank_columns(bias_full)
    bias_mine = lax.dynamic_index_in_dim(bias_ranks, rank_index, 0, keepdims=False)
    result = (product + bias_mine.astype(jnp.float32)).astype(jnp.bfloat16)
    return result[None]


def chunk_of(kind, j):
    what, first, count = CHUNKS[kind][j]
    return what, first, count, sum(c[2] for c in CHUNKS[kind][:j])


def kernel(
    dims,
    tok_hbm,
    gain_ref,
    w_hbm,
    bias_ref,
    out_ref,
    tok_ref,
    w_ref,
    xsend,
    xbuf,
    wsend,
    wbuf,
    dbuf,
    psend,
    pbuf,
    acc,
    bias_own,
    bbuf,
    load_sem,
    x_recv,
    x1_recv,
    x_send,
    w_recv,
    wx_recv,
    wc_recv,
    d_recv,
    w_send,
    p_recv,
    p_send,
    b_recv,
    b_send,
):
    inst_count, shard_count, group = dims
    devices = inst_count * shard_count
    inst = lax.axis_index("inst")
    me = lax.axis_index("shard")
    z = me // 2
    y = lax.rem(me, 2)
    half = z // 2
    flat = inst * shard_count + me
    core_peer = inst + 1 - 2 * lax.rem(inst, 2)
    x_peer = lax.rem(inst + 2, inst_count)
    z_mate = z + 1 - 2 * lax.rem(z, 2)
    z_pair = lax.rem(z + 2, 4)
    z_near = 2 - half
    z_end = 3 - 3 * half
    inner = z_near + z == 3
    rows = w_ref.shape[0]
    tokens, depth = tok_ref.shape
    tiles = wsend.shape[1]
    half_block = 4 * rows
    pieces = TOKEN_PIECES
    piece_rows = tokens // pieces

    token_load = pltpu.make_async_copy(tok_hbm, tok_ref, load_sem.at[0])
    weight_load = pltpu.make_async_copy(w_hbm, w_ref, load_sem.at[1])
    token_load.start()
    weight_load.start()

    barrier = pltpu.get_barrier_semaphore()

    @pl.loop(1, devices)
    def _(step):
        there = lax.rem(flat + step, devices)
        pl.semaphore_signal(
            barrier,
            inc=1,
            device_id=(there // shard_count, lax.rem(there, shard_count)),
            device_id_type=MESH,
        )

    def remote(source, target, send_sem, recv_sem, device):
        return pltpu.make_async_remote_copy(
            src_ref=source,
            dst_ref=target,
            send_sem=send_sem,
            recv_sem=recv_sem,
            device_id=device,
            device_id_type=MESH,
        )

    def each(condition, action):
        pl.when(condition)(action)

    def piece_of(ref, piece):
        return ref.at[pl.ds(piece * piece_rows, piece_rows)]

    def own_x(which, device, side, piece):
        return remote(
            piece_of(xsend.at[which], piece),
            piece_of(xbuf.at[side, z], piece),
            x_send.at[0],
            x1_recv if side else x_recv.at[z, piece],
            (inst, device),
        )

    def relay_x(way, block, piece):
        device, side = ((z_mate * 2 + y, 0), (z * 2 + 1 - y, 1))[way]
        return remote(
            piece_of(xbuf.at[0, block], piece),
            piece_of(xbuf.at[side, block], piece),
            x_send.at[1 + way],
            x1_recv if side else x_recv.at[block, piece],
            (inst, device),
        )

    def slot_of(owner, k):
        return owner * 4 + lax.rem(z_mate if k // 2 else z, 2) * 2 + (1 - y if k % 2 else y)

    def fresh(kind, there, j, side):
        what, first, count, _ = chunk_of(kind, j)
        rank = {"far": lax.rem(there + 2, 4), "extra": z_near, "own": there}[what] * 2 + side
        return wsend.at[rank, pl.ds(first, count)]

    def held(kind, slot, j):
        _, _, count, at = chunk_of(kind, j)
        return wbuf.at[slot, pl.ds(at, count)]

    def arrived(ref, sem):
        pltpu.make_async_copy(ref, ref, sem).wait()

    query = QHEADS * HEAD_DIM // TP
    pair = KVHEADS * HEAD_DIM // TP
    held_bias = bias_ref.shape[1]
    per_row = LANES // group
    groups = held_bias // group

    def needs(owner, rank):
        low, high = owner * held_bias, owner * held_bias + held_bias
        result = None
        for start, extent in (
            (rank * query, query),
            (TP * query + rank * pair, pair),
            (TP * (query + pair) + rank * pair, pair),
        ):
            overlap = jnp.logical_and(start < high, low < start + extent)
            result = overlap if result is None else jnp.logical_or(result, overlap)
        return result

    def bias_copy(step):
        there = lax.rem(flat + step, devices)
        return remote(
            bias_own,
            bbuf.at[flat],
            b_send.at[step],
            b_recv.at[flat],
            (there // shard_count, lax.rem(there, shard_count)),
        )

    def send_bias(finish):
        @pl.loop(1, devices)
        def _(step):
            there = lax.rem(flat + step, devices)

            @pl.when(needs(flat, lax.rem(there, shard_count)))
            def _():
                if finish:
                    bias_copy(step).wait_send()
                else:
                    bias_copy(step).start()

    def bias_row(number_first):
        lane = lax.broadcasted_iota(jnp.int32, (1, LANES), 1) // group
        row = jnp.zeros((1, LANES), jnp.float32)
        for q in range(per_row):
            number = number_first + q
            row = jnp.where(lane == q, bbuf[number // groups, pl.ds(lax.rem(number, groups), 1), :], row)
        return row

    def column_of(t):
        at = t * LANES
        if at < query:
            return me * query + at
        if at < query + pair:
            return TP * query + me * pair + (at - query)
        return TP * (query + pair) + me * pair + (at - query - pair)

    ids = lax.broadcasted_iota(jnp.int32, (rows, rows), 0), lax.broadcasted_iota(jnp.int32, (rows, rows), 1)
    gain_row = gain_ref[...].astype(jnp.bfloat16).astype(jnp.float32)
    gain = jnp.sum(jnp.where(ids[0] == ids[1], jnp.broadcast_to(gain_row, (rows, rows)), 0.0), axis=1, keepdims=True)
    group_id = lax.broadcasted_iota(jnp.int32, (8, held_bias), 0)
    lane_id = lax.broadcasted_iota(jnp.int32, (8, held_bias), 1)
    spread = jnp.where(lane_id // group == group_id, jnp.broadcast_to(bias_ref[...], (8, held_bias)), 0.0)
    from_id = lax.broadcasted_iota(jnp.int32, (held_bias, LANES), 0)
    to_id = lax.broadcasted_iota(jnp.int32, (held_bias, LANES), 1)
    pick = jnp.where(lax.rem(from_id, group) == lax.rem(to_id, group), 1.0, 0.0).astype(jnp.bfloat16)
    bias_own[...] = jnp.dot(spread.astype(jnp.bfloat16), pick, preferred_element_type=jnp.float32)

    token_load.wait()
    step_rows = 16
    for first in range(0, tokens, step_rows):
        values = tok_ref[first : first + step_rows, :].astype(jnp.float32)
        mean = jnp.sum(values * values, axis=-1, keepdims=True) * (1.0 / depth)
        scaled = (values * lax.rsqrt(mean + EPSILON)).astype(jnp.bfloat16)
        for which in range(2):
            for owner in range(inst_count):
                at = (owner * 2 + which) * half_block
                xsend[which, first : first + step_rows, owner * half_block : (owner + 1) * half_block] = scaled[
                    :, at : at + half_block
                ]
    pl.semaphore_wait(barrier, devices - 1)

    def send_x(name, piece):
        which, device, side = {
            "xf": (1 - half, z_near * 2 + y, 0),
            "xm": (half, z_mate * 2 + y, 0),
            "xy": (half, z * 2 + 1 - y, 1),
        }[name]
        own_x(which, device, side, piece).start()

    def early(steps):
        for name, piece, _ in steps:
            if name not in ("xf", "xm", "xy"):
                break
            send_x(name, piece)

    each(inner, lambda: early(INNER))
    each(jnp.logical_not(inner), lambda: early(OUTER))
    xbuf[0, z] = xsend[half]

    weight_load.wait()
    for rank in range(TP):
        starts = (
            (rank * query, 0, query),
            (TP * query + rank * pair, query, pair),
            (TP * (query + pair) + rank * pair, query + pair, pair),
        )
        for source, target, extent in starts:
            for inside in range(0, extent, LANES):
                part = w_ref[:, source + inside : source + inside + LANES].astype(jnp.bfloat16).astype(jnp.float32)
                wsend[rank, (target + inside) // LANES] = (part * gain).astype(jnp.bfloat16)

    def product(kind, m, j):
        _, first, count, at = chunk_of(kind, j)
        lhs = xbuf[m].reshape(4 * tokens, 4 * half_block)
        result = []
        for t in range(0, count, 2):
            width = min(2, count - t)
            rhs = [wbuf[:, at + t + u].reshape(4 * half_block, LANES) for u in range(width)]
            rhs = jnp.concatenate(rhs, axis=1) if width > 1 else rhs[0]
            value = jnp.dot(lhs, rhs, preferred_element_type=jnp.float32)
            for u in range(width):
                result.append((t + u, value[:, u * LANES : (u + 1) * LANES]))
        return result

    def finish_bias():
        @pl.loop(1, devices)
        def _(step):
            slot = lax.rem(flat + step, devices)

            @pl.when(needs(slot, me))
            def _():
                arrived(bbuf.at[slot], b_recv.at[slot])

        bbuf[flat] = bias_own[...]
        send_bias(True)

    def run(kind, steps):
        other = 1 - kind
        done = set()

        def once(key, action):
            if key not in done:
                done.add(key)
                action()

        def need_x(block):
            for piece in range(pieces):
                once(
                    ("x", block, piece),
                    lambda piece=piece: arrived(
                        piece_of(xbuf.at[0, places[block]], piece), x_recv.at[places[block], piece]
                    ),
                )

        def need_w(k, j):
            once(("w", k, j), lambda: arrived(held(kind, slot_of(inst, k), j), w_recv.at[k - 1, j]))

        def need_chunk(j):
            _, first, count, at = chunk_of(kind, j)

            def action():
                arrived(wbuf.at[pl.ds(0, 8), pl.ds(at, count)], wc_recv.at[j])
                wbuf[slot_of(inst, 0), at : at + count] = fresh(kind, z, j, y)[...]

            once(("c", j), action)

        def need_tokens(m):
            for block in (1, 2, 3):
                need_x(block)
            if m:
                once("x1", lambda: arrived(xbuf.at[1], x1_recv))

        places = (z, z_mate, z_near, z_end)

        def step_rx(block, piece):
            once(
                ("x", block, piece),
                lambda: arrived(piece_of(xbuf.at[0, places[block]], piece), x_recv.at[places[block], piece]),
            )
            relay_x(0, places[block], piece).start()

        def step_ry(block, piece):
            once(
                ("x", block, piece),
                lambda: arrived(piece_of(xbuf.at[0, places[block]], piece), x_recv.at[places[block], piece]),
            )
            relay_x(1, places[block], piece).start()

        def step_wp(j, k):
            mine = slot_of(inst, 0)
            if k == 1:
                source, target, device = fresh(kind, z, j, 1 - y), held(kind, mine, j), z * 2 + 1 - y
            else:
                source, target, device = fresh(other, z_mate, j, y), held(other, mine, j), z_mate * 2 + y
            remote(source, target, w_send.at[k - 1], w_recv.at[k - 1, j], (inst, device)).start()

        def step_wd(j, _):
            _, _, count, at = chunk_of(other, j)
            target = dbuf.at[pl.ds(at, count)]
            remote(
                fresh(other, z_mate, j, 1 - y), target, w_send.at[2], d_recv.at[j], (inst, z_mate * 2 + y)
            ).start()

        def step_rd(j, _):
            _, _, count, at = chunk_of(kind, j)
            source = dbuf.at[pl.ds(at, count)]
            arrived(source, d_recv.at[j])
            target = held(kind, slot_of(inst, 2), j)
            remote(source, target, w_send.at[3], w_recv.at[2, j], (inst, z * 2 + 1 - y)).start()

        def send_block(j, k, source, across):
            device, send, recv = (
                ((x_peer, me), w_send.at[4], wx_recv.at[k, j]),
                ((core_peer, me), w_send.at[5], wc_recv.at[j]),
            )[across]
            remote(source, held(kind, slot_of(inst, k), j), send, recv, device).start()

        def step_ox(j, _):
            send_block(j, 0, fresh(kind, z, j, y), 0)

        def step_ko(j, _):
            send_block(j, 0, fresh(kind, z, j, y), 1)

        def step_rw(j, k):
            need_w(k, j)
            send_block(j, k, held(kind, slot_of(inst, k), j), 0)

        def step_kw(j, k):
            need_w(k, j)
            send_block(j, k, held(kind, slot_of(inst, k), j), 1)

        def step_rc(j, k):
            block = held(kind, slot_of(x_peer, k), j)
            arrived(block, wx_recv.at[k, j])
            remote(block, block, w_send.at[5], wc_recv.at[j], (core_peer, me)).start()

        def step_pm(m, j):
            need_tokens(m)
            need_chunk(j)
            what, first, count, at = chunk_of(kind, j)
            for t, value in product(kind, m, j):
                psend[m, at + t] = value.astype(jnp.bfloat16)
            target = other if what == "far" else kind
            index = [c[:3] for c in CHUNKS[target]].index(("own", first, count))
            remote(
                psend.at[m, pl.ds(at, count)],
                pbuf.at[m, pl.ds(first, count)],
                p_send.at[0],
                p_recv.at[m, index],
                (inst, (z_pair if what == "far" else z_near) * 2 + y),
            ).start()

        def step_om(m, j):
            need_tokens(m)
            need_chunk(j)
            first = chunk_of(kind, j)[1]
            for t, value in product(kind, m, j):
                acc[m, first + t] = value

        def step_fin(m, j):
            once("bias", finish_bias)
            _, first, count, _ = chunk_of(kind, j)
            arrived(pbuf.at[m, pl.ds(first, count)], p_recv.at[m, j])
            where = 1 - y if m else y
            for t in range(first, first + count):
                value = acc[m, t] + pbuf[m, t].astype(jnp.float32) + bias_row(column_of(t) // group)
                value = value.astype(jnp.bfloat16)
                for k in range(4):
                    out_ref[k, where, :, t * LANES : (t + 1) * LANES] = value[k * tokens : (k + 1) * tokens]

        def step_bias(*_):
            send_bias(False)

        table = dict(
            xy=lambda piece, _: send_x("xy", piece),
            xf=lambda piece, _: send_x("xf", piece),
            xm=lambda piece, _: send_x("xm", piece),
            rx=step_rx,
            ry=step_ry,
            wp=step_wp,
            wd=step_wd,
            rd=step_rd,
            ox=step_ox,
            ko=step_ko,
            rw=step_rw,
            kw=step_kw,
            rc=step_rc,
            pm=step_pm,
            om=step_om,
            fin=step_fin,
            bias=step_bias,
        )
        start = next(i for i, step in enumerate(steps) if step[0] not in ("xf", "xm", "xy"))
        for name, first, second in steps[start:]:
            table[name](first, second)

        counts = [sum(c[2] for c in CHUNKS[way]) for way in range(2)]
        sent = counts[kind] - tiles
        once("sent_x", lambda: arrived(xbuf.at[0, pl.ds(0, 3)], x_send.at[0]))
        once("sent_y", lambda: arrived(xbuf.at[0, pl.ds(0, 3)], x_send.at[2]))
        if kind == 0:
            arrived(xbuf.at[0, pl.ds(0, 2)], x_send.at[1])
        for way, target in enumerate((kind, other, other, kind)):
            arrived(wbuf.at[0, pl.ds(0, counts[target])], w_send.at[way])
        arrived(wbuf.at[pl.ds(0, 4), pl.ds(0, counts[kind])], w_send.at[4])
        arrived(wbuf.at[pl.ds(0, 8), pl.ds(0, counts[kind])], w_send.at[5])
        arrived(psend.at[:, pl.ds(0, sent)], p_send.at[0])

    each(inner, lambda: run(0, INNER))
    each(jnp.logical_not(inner), lambda: run(1, OUTER))


def kernel_device(dims, tokens, norm_gain, master_qkv, qkv_bias):
    inst_count, shard_count, group = dims
    devices = inst_count * shard_count
    rows = master_qkv.shape[0]
    count, depth = tokens.shape
    tiles = master_qkv.shape[1] // TP // LANES
    pieces = TOKEN_PIECES
    most = max(len(c) for c in CHUNKS)
    held = max(sum(c[2] for c in way) for way in CHUNKS)
    dma = pltpu.SemaphoreType.DMA
    vmem = pl.BlockSpec(memory_space=pltpu.VMEM)
    anywhere = pl.BlockSpec(memory_space=pl.ANY)
    low, wide = jnp.bfloat16, jnp.float32
    result = pl.pallas_call(
        functools.partial(kernel, dims),
        out_shape=jax.ShapeDtypeStruct((4, 2, count, tiles * LANES), low),
        in_specs=[anywhere, vmem, anywhere, vmem],
        out_specs=vmem,
        scratch_shapes=[
            pltpu.VMEM((count, depth), low),
            pltpu.VMEM((rows, master_qkv.shape[1]), wide),
            pltpu.VMEM((2, count, depth // 2), low),
            pltpu.VMEM((2, 4, count, depth // 2), low),
            pltpu.VMEM((TP, tiles, rows, LANES), low),
            pltpu.VMEM((4 * inst_count, held, rows, LANES), low),
            pltpu.VMEM((held, rows, LANES), low),
            pltpu.VMEM((2, held - tiles, 4 * count, LANES), low),
            pltpu.VMEM((2, tiles, 4 * count, LANES), low),
            pltpu.VMEM((2, tiles, 4 * count, LANES), wide),
            pltpu.VMEM((8, LANES), wide),
            pltpu.VMEM((devices, 8, LANES), wide),
            dma((2,)),
            dma((4, pieces)),
            dma,
            dma((3,)),
            dma((3, most)),
            dma((4, most)),
            dma((most,)),
            dma((most,)),
            dma((6,)),
            dma((2, most)),
            dma((1,)),
            dma((devices,)),
            dma((devices,)),
        ],
        compiler_params=pltpu.CompilerParams(
            collective_id=0, has_side_effects=True, vmem_limit_bytes=60 * 1024 * 1024
        ),
    )(tokens, norm_gain.reshape(1, rows), master_qkv, qkv_bias.reshape(1, -1))
    return result.reshape(1, shard_count * count, tiles * LANES)


def per_device(tokens, norm_gain, master_qkv, qkv_bias):
    inst_count, shard_count = lax.axis_size("inst"), lax.axis_size("shard")
    group = 32
    fits = (
        shard_count == TP
        and inst_count == 4
        and master_qkv.shape[0] % 16 == 0
        and tokens.shape[0] % (16 * TOKEN_PIECES) == 0
        and QHEADS * HEAD_DIM // TP % LANES == 0
        and KVHEADS * HEAD_DIM // TP == LANES
        and 4 * master_qkv.shape[0] % LANES == 0
        and qkv_bias.shape[0] % group == 0
    )
    if fits:
        return kernel_device((inst_count, shard_count, group), tokens, norm_gain, master_qkv, qkv_bias)
    return general_device(tokens, norm_gain, master_qkv, qkv_bias)


def solution(mesh):
    in_specs = (
        P(("inst", "shard"), None),
        P(("inst", "shard")),
        P(("inst", "shard"), None),
        P(("inst", "shard")),
    )
    out_specs = P(("inst", "shard"), None, None)
    return jax.shard_map(
        per_device, mesh=mesh, in_specs=in_specs, out_specs=out_specs, check_vma=False
    )
```

```python
import functools

import jax
import jax.numpy as jnp
from jax import lax
from jax.experimental import pallas as pl
from jax.experimental.pallas import tpu as pltpu
from jax.sharding import PartitionSpec as P

QHEADS = 40
KVHEADS = 8
HEAD_DIM = 128
TP = 8


EPSILON = 1e-06
MESH = pl.DeviceIdType.MESH
LANES = 128
TOKEN_PIECES = 2
CHUNKS = (
    (("far", 0, 1), ("far", 1, 2), ("far", 3, 2), ("far", 5, 2), ("extra", 4, 3), ("own", 0, 2), ("own", 2, 2), ("own", 4, 3)),
    (("far", 0, 2), ("far", 2, 2), ("own", 0, 2), ("own", 2, 2), ("own", 4, 3)),
)
ACROSS = ((5, 6, 7), ())
INNER = (
    ("xm", 1, 0),
    ("xy", 1, 0),
    ("xf", 1, 0),
    ("wp", 1, 2),
    ("wp", 4, 1),
    ("ox", 7, 0),
    ("ox", 1, 0),
    ("wp", 7, 1),
    ("ko", 4, 0),
    ("wd", 1, 0),
    ("wp", 1, 1),
    ("ox", 4, 0),
    ("wp", 0, 2),
    ("ox", 5, 0),
    ("bias", 0, 0),
    ("rx", 2, 1),
    ("wd", 0, 0),
    ("ox", 3, 0),
    ("ox", 6, 0),
    ("wp", 0, 1),
    ("wp", 3, 1),
    ("xf", 0, 0),
    ("xm", 0, 0),
    ("ko", 1, 0),
    ("rd", 1, 0),
    ("rx", 2, 0),
    ("rd", 4, 0),
    ("kw", 0, 1),
    ("rw", 4, 2),
    ("rc", 1, 0),
    ("ko", 3, 0),
    ("rx", 3, 1),
    ("ox", 2, 0),
    ("xy", 0, 0),
    ("ry", 1, 1),
    ("wd", 3, 0),
    ("rw", 4, 1),
    ("ry", 2, 1),
    ("rc", 2, 0),
    ("rw", 4, 3),
    ("kw", 1, 1),
    ("rx", 3, 0),
    ("rw", 7, 1),
    ("rc", 4, 2),
    ("rw", 1, 3),
    ("ko", 2, 0),
    ("rc", 3, 0),
    ("rc", 4, 0),
    ("wd", 2, 0),
    ("rw", 1, 2),
    ("ry", 1, 0),
    ("kw", 4, 2),
    ("kw", 4, 1),
    ("wp", 2, 1),
    ("rw", 0, 1),
    ("rc", 4, 3),
    ("kw", 4, 3),
    ("rc", 4, 1),
    ("kw", 1, 2),
    ("wp", 6, 1),
    ("rw", 3, 2),
    ("pm", 1, 4),
    ("ko", 0, 0),
    ("rw", 1, 1),
    ("wp", 3, 2),
    ("pm", 0, 4),
    ("rd", 3, 0),
    ("rw", 3, 1),
    ("wd", 4, 0),
    ("ko", 7, 0),
    ("rd", 2, 0),
    ("wp", 4, 2),
    ("wp", 5, 1),
    ("kw", 2, 2),
    ("kw", 1, 3),
    ("rw", 2, 1),
    ("rc", 1, 2),
    ("kw", 3, 2),
    ("rc", 3, 2),
    ("kw", 2, 1),
    ("rc", 1, 3),
    ("rw", 2, 2),
    ("rc", 1, 1),
    ("pm", 2, 4),
    ("rw", 3, 3),
    ("pm", 2, 1),
    ("rc", 7, 0),
    ("rd", 0, 0),
    ("rw", 2, 3),
    ("wp", 2, 2),
    ("rc", 3, 1),
    ("kw", 3, 1),
    ("ox", 0, 0),
    ("ry", 3, 1),
    ("kw", 0, 3),
    ("pm", 0, 1),
    ("ko", 5, 0),
    ("rw", 0, 2),
    ("rw", 0, 3),
    ("kw", 5, 1),
    ("pm", 1, 1),
    ("rc", 6, 0),
    ("kw", 3, 3),
    ("rw", 6, 1),
    ("rc", 3, 3),
    ("rc", 2, 1),
    ("kw", 0, 2),
    ("ry", 2, 0),
    ("rc", 0, 1),
    ("rc", 2, 2),
    ("kw", 2, 3),
    ("rc", 2, 3),
    ("pm", 1, 3),
    ("rc", 0, 0),
    ("ko", 6, 0),
    ("pm", 1, 2),
    ("pm", 2, 2),
    ("rw", 6, 3),
    ("rc", 0, 2),
    ("ry", 3, 0),
    ("rw", 5, 1),
    ("pm", 0, 3),
    ("kw", 6, 3),
    ("rw", 6, 2),
    ("kw", 6, 1),
    ("rc", 0, 3),
    ("pm", 0, 0),
    ("rc", 6, 3),
    ("pm", 2, 0),
    ("rw", 7, 3),
    ("pm", 0, 2),
    ("rc", 5, 0),
    ("pm", 3, 1),
    ("rc", 6, 1),
    ("kw", 7, 3),
    ("rc", 5, 1),
    ("rw", 7, 2),
    ("pm", 1, 0),
    ("pm", 3, 2),
    ("kw", 6, 2),
    ("pm", 2, 3),
    ("rc", 6, 2),
    ("rw", 5, 2),
    ("kw", 7, 2),
    ("pm", 3, 3),
    ("om", 1, 6),
    ("om", 0, 6),
    ("pm", 3, 0),
    ("kw", 7, 1),
    ("rw", 5, 3),
    ("pm", 3, 4),
    ("rc", 7, 1),
    ("rc", 7, 2),
    ("rc", 7, 3),
    ("om", 0, 7),
    ("fin", 0, 6),
    ("rc", 5, 2),
    ("kw", 5, 3),
    ("kw", 5, 2),
    ("fin", 2, 6),
    ("rc", 5, 3),
    ("fin", 1, 7),
    ("om", 1, 7),
    ("om", 1, 5),
    ("fin", 3, 6),
    ("om", 0, 5),
    ("fin", 2, 5),
    ("fin", 3, 5),
    ("fin", 1, 6),
    ("fin", 0, 5),
    ("fin", 1, 5),
    ("fin", 0, 7),
    ("fin", 3, 7),
    ("fin", 2, 7),
)
OUTER = (
    ("xy", 1, 0),
    ("xm", 1, 0),
    ("wp", 4, 2),
    ("wd", 4, 0),
    ("xy", 0, 0),
    ("wd", 1, 0),
    ("wp", 1, 1),
    ("bias", 0, 0),
    ("rw", 1, 2),
    ("wp", 3, 1),
    ("ko", 1, 0),
    ("ox", 1, 0),
    ("xf", 1, 0),
    ("ox", 0, 0),
    ("wp", 0, 1),
    ("rw", 1, 1),
    ("rd", 1, 0),
    ("xf", 0, 0),
    ("rc", 0, 0),
    ("ry", 1, 1),
    ("kw", 1, 3),
    ("xm", 0, 0),
    ("rw", 0, 1),
    ("rw", 1, 3),
    ("ox", 4, 0),
    ("wp", 1, 2),
    ("rc", 1, 2),
    ("kw", 1, 2),
    ("rd", 0, 0),
    ("ry", 1, 0),
    ("ko", 0, 0),
    ("rc", 0, 1),
    ("rc", 1, 0),
    ("rc", 1, 3),
    ("wp", 3, 2),
    ("ko", 4, 0),
    ("rc", 1, 1),
    ("rw", 0, 3),
    ("kw", 1, 1),
    ("ry", 2, 0),
    ("rw", 0, 2),
    ("kw", 0, 3),
    ("pm", 0, 1),
    ("ry", 2, 1),
    ("pm", 2, 1),
    ("wd", 3, 0),
    ("ox", 3, 0),
    ("rc", 0, 2),
    ("rw", 3, 1),
    ("ko", 3, 0),
    ("wp", 2, 2),
    ("ry", 3, 1),
    ("kw", 0, 1),
    ("wd", 2, 0),
    ("ry", 3, 0),
    ("rd", 3, 0),
    ("pm", 1, 1),
    ("we", 6, 0),
    ("kw", 0, 2),
    ("rc", 0, 3),
    ("pm", 0, 0),
    ("pm", 1, 0),
    ("kw", 3, 2),
    ("wd", 0, 0),
    ("wp", 0, 2),
    ("we", 7, 0),
    ("pm", 3, 0),
    ("rw", 3, 2),
    ("kw", 3, 3),
    ("pm", 3, 1),
    ("ko", 2, 0),
    ("ox", 2, 0),
    ("re", 6, 0),
    ("rw", 3, 3),
    ("rc", 3, 0),
    ("wp", 2, 1),
    ("wp", 6, 2),
    ("rw", 4, 2),
    ("wp", 4, 1),
    ("re", 7, 0),
    ("rc", 3, 3),
    ("rc", 3, 1),
    ("rd", 4, 0),
    ("kw", 3, 1),
    ("rw", 2, 1),
    ("kw", 2, 1),
    ("rc", 3, 2),
    ("om", 0, 3),
    ("rw", 4, 1),
    ("wp", 7, 2),
    ("om", 1, 3),
    ("rw", 2, 2),
    ("wp", 5, 2),
    ("rc", 2, 0),
    ("rc", 4, 0),
    ("we", 5, 0),
    ("kw", 4, 1),
    ("re", 5, 0),
    ("rw", 4, 3),
    ("kw", 4, 2),
    ("rd", 2, 0),
    ("rc", 4, 1),
    ("kw", 4, 3),
    ("kw", 2, 3),
    ("rw", 2, 3),
    ("kw", 2, 2),
    ("rc", 4, 2),
    ("rc", 4, 3),
    ("rc", 2, 2),
    ("pm", 2, 0),
    ("rc", 2, 1),
    ("fin", 0, 3),
    ("om", 0, 4),
    ("fin", 1, 3),
    ("om", 1, 4),
    ("rc", 2, 3),
    ("fin", 1, 4),
    ("om", 0, 2),
    ("om", 1, 2),
    ("fin", 1, 2),
    ("fin", 3, 4),
    ("fin", 2, 2),
    ("fin", 0, 4),
    ("fin", 3, 2),
    ("fin", 3, 3),
    ("fin", 2, 3),
    ("fin", 2, 4),
    ("fin", 0, 2),
)


def partner_2(value, axis, distance):
    mask = 2**distance
    pairs = [(source, source ^ mask) for source in range(lax.axis_size(axis))]
    return lax.ppermute(value, axis, pairs)


def rank_columns(matrix):
    query_cols = QHEADS * HEAD_DIM
    pair_cols = KVHEADS * HEAD_DIM
    leading = matrix.shape[:-1]
    query = matrix[..., :query_cols].reshape(leading + (TP, query_cols // TP))
    keys = matrix[..., query_cols : query_cols + pair_cols].reshape(leading + (TP, pair_cols // TP))
    values = matrix[..., query_cols + pair_cols :].reshape(leading + (TP, pair_cols // TP))
    return jnp.concatenate([query, keys, values], axis=-1)


def normalize(tokens, gain):
    floats = tokens.astype(jnp.float32)
    scale = lax.rsqrt(jnp.mean(floats * floats, axis=-1, keepdims=True) + EPSILON)
    return (floats * scale * gain.astype(jnp.float32)).astype(jnp.bfloat16)


def general_device(tokens, norm_gain, master_qkv, qkv_bias):
    shard_count = lax.axis_size("shard")
    local_rows = master_qkv.shape[0]
    rank_width = master_qkv.shape[1] // TP
    gain_full, bias_full = (
        lax.all_gather(norm_gain.astype(jnp.bfloat16), ("inst", "shard"), axis=0, tiled=True),
        lax.all_gather(qkv_bias.astype(jnp.bfloat16), ("inst", "shard"), axis=0, tiled=True),
    )
    normed = normalize(tokens, gain_full)
    shard_pos = lax.axis_index("shard")
    rank_index = shard_pos % TP
    bit_count = TP.bit_length() - 1
    bit_order = list(range(bit_count))
    group_rows = normed
    for bit_pos in bit_order:
        partner = partner_2(group_rows, "shard", bit_pos)
        lower = jnp.bitwise_and(jnp.right_shift(shard_pos, bit_pos), 1) == 0
        group_rows = jnp.where(
            lower,
            jnp.concatenate([group_rows, partner], 0),
            jnp.concatenate([partner, group_rows], 0),
        )
    copies = shard_count // TP
    inst_block = shard_count * local_rows
    rows_low = master_qkv.astype(jnp.bfloat16)
    ranked = jnp.transpose(rank_columns(rows_low), (1, 0, 2))
    spread = jnp.broadcast_to(ranked[None], (copies,) + ranked.shape)
    outgoing = spread.reshape(shard_count, rows_low.shape[0], rank_width)
    arrived = lax.all_to_all(outgoing, "shard", split_axis=0, concat_axis=0, tiled=True).reshape(
        inst_block, rank_width
    )
    product = jnp.dot(
        group_rows,
        lax.all_gather(arrived, "inst", axis=0, tiled=True),
        preferred_element_type=jnp.float32,
    )
    bias_ranks = rank_columns(bias_full)
    bias_mine = lax.dynamic_index_in_dim(bias_ranks, rank_index, 0, keepdims=False)
    result = (product + bias_mine.astype(jnp.float32)).astype(jnp.bfloat16)
    return result[None]


def incoming(kind):
    chunks = [c for c in CHUNKS[1 - kind] if c[0] == "far"]
    return [c[1:] for c in chunks + [c for c in CHUNKS[kind] if c[0] == "extra"]]


def chunk_of(kind, j):
    what, first, count = CHUNKS[kind][j]
    return what, first, count, sum(c[2] for c in CHUNKS[kind][:j])


def kernel(
    dims,
    tok_hbm,
    gain_ref,
    w_hbm,
    bias_ref,
    out_ref,
    tok_ref,
    w_ref,
    xsend,
    xbuf,
    wsend,
    wbuf,
    dbuf,
    ebuf,
    psend,
    pbuf,
    acc,
    bias_own,
    bbuf,
    load_sem,
    x_recv,
    x1_recv,
    x_send,
    w_recv,
    wx_recv,
    wc_recv,
    d_recv,
    e_recv,
    w_send,
    p_recv,
    p_send,
    b_recv,
    b_send,
):
    inst_count, shard_count, group = dims
    devices = inst_count * shard_count
    inst = lax.axis_index("inst")
    me = lax.axis_index("shard")
    z = me // 2
    y = lax.rem(me, 2)
    half = z // 2
    flat = inst * shard_count + me
    core_peer = inst + 1 - 2 * lax.rem(inst, 2)
    x_peer = lax.rem(inst + 2, inst_count)
    z_mate = z + 1 - 2 * lax.rem(z, 2)
    z_pair = lax.rem(z + 2, 4)
    z_near = 2 - half
    z_end = 3 - 3 * half
    inner = z_near + z == 3
    rows = w_ref.shape[0]
    tokens, depth = tok_ref.shape
    tiles = wsend.shape[1]
    half_block = 4 * rows
    pieces = TOKEN_PIECES
    piece_rows = tokens // pieces

    token_load = pltpu.make_async_copy(tok_hbm, tok_ref, load_sem.at[0])
    weight_load = pltpu.make_async_copy(w_hbm, w_ref, load_sem.at[1])
    token_load.start()
    weight_load.start()

    barrier = pltpu.get_barrier_semaphore()

    @pl.loop(1, devices)
    def _(step):
        there = lax.rem(flat + step, devices)
        pl.semaphore_signal(
            barrier,
            inc=1,
            device_id=(there // shard_count, lax.rem(there, shard_count)),
            device_id_type=MESH,
        )

    def remote(source, target, send_sem, recv_sem, device):
        return pltpu.make_async_remote_copy(
            src_ref=source,
            dst_ref=target,
            send_sem=send_sem,
            recv_sem=recv_sem,
            device_id=device,
            device_id_type=MESH,
        )

    def each(condition, action):
        pl.when(condition)(action)

    def piece_of(ref, piece):
        return ref.at[pl.ds(piece * piece_rows, piece_rows)]

    def own_x(which, device, side, piece):
        return remote(
            piece_of(xsend.at[which], piece),
            piece_of(xbuf.at[side, half, lax.rem(z, 2)], piece),
            x_send.at[0],
            x1_recv.at[half] if side else x_recv.at[z, piece],
            (inst, device),
        )

    def relay_x(way, block, piece):
        device, side = ((z_mate * 2 + y, 0), (z * 2 + 1 - y, 1))[way]
        return remote(
            piece_of(xbuf.at[0, block // 2, lax.rem(block, 2)], piece),
            piece_of(xbuf.at[side, block // 2, lax.rem(block, 2)], piece),
            x_send.at[1 + way],
            x1_recv.at[block // 2] if side else x_recv.at[block, piece],
            (inst, device),
        )

    def slot_of(owner, k):
        return owner * 4 + lax.rem(z_mate if k // 2 else z, 2) * 2 + (1 - y if k % 2 else y)

    def fresh(kind, there, j, side):
        what, first, count, _ = chunk_of(kind, j)
        rank = {"far": lax.rem(there + 2, 4), "extra": z_near, "own": there}[what] * 2 + side
        return wsend.at[rank, pl.ds(first, count)]

    def held(kind, slot, j):
        _, _, count, at = chunk_of(kind, j)
        return wbuf.at[slot, pl.ds(at, count)]

    def arrived(ref, sem):
        pltpu.make_async_copy(ref, ref, sem).wait()

    query = QHEADS * HEAD_DIM // TP
    pair = KVHEADS * HEAD_DIM // TP
    held_bias = bias_ref.shape[1]
    per_row = LANES // group
    groups = held_bias // group

    def needs(owner, rank):
        low, high = owner * held_bias, owner * held_bias + held_bias
        result = None
        for start, extent in (
            (rank * query, query),
            (TP * query + rank * pair, pair),
            (TP * (query + pair) + rank * pair, pair),
        ):
            overlap = jnp.logical_and(start < high, low < start + extent)
            result = overlap if result is None else jnp.logical_or(result, overlap)
        return result

    def bias_copy(step):
        there = lax.rem(flat + step, devices)
        return remote(
            bias_own,
            bbuf.at[flat],
            b_send.at[step],
            b_recv.at[flat],
            (there // shard_count, lax.rem(there, shard_count)),
        )

    def send_bias(finish):
        @pl.loop(1, devices)
        def _(step):
            there = lax.rem(flat + step, devices)

            @pl.when(needs(flat, lax.rem(there, shard_count)))
            def _():
                if finish:
                    bias_copy(step).wait_send()
                else:
                    bias_copy(step).start()

    def bias_row(number_first):
        lane = lax.broadcasted_iota(jnp.int32, (1, LANES), 1) // group
        row = jnp.zeros((1, LANES), jnp.float32)
        for q in range(per_row):
            number = number_first + q
            row = jnp.where(lane == q, bbuf[number // groups, pl.ds(lax.rem(number, groups), 1), :], row)
        return row

    def column_of(t):
        at = t * LANES
        if at < query:
            return me * query + at
        if at < query + pair:
            return TP * query + me * pair + (at - query)
        return TP * (query + pair) + me * pair + (at - query - pair)

    ids = lax.broadcasted_iota(jnp.int32, (rows, rows), 0), lax.broadcasted_iota(jnp.int32, (rows, rows), 1)
    gain_row = gain_ref[...].astype(jnp.bfloat16).astype(jnp.float32)
    gain = jnp.sum(jnp.where(ids[0] == ids[1], jnp.broadcast_to(gain_row, (rows, rows)), 0.0), axis=1, keepdims=True)
    group_id = lax.broadcasted_iota(jnp.int32, (8, held_bias), 0)
    lane_id = lax.broadcasted_iota(jnp.int32, (8, held_bias), 1)
    spread = jnp.where(lane_id // group == group_id, jnp.broadcast_to(bias_ref[...], (8, held_bias)), 0.0)
    from_id = lax.broadcasted_iota(jnp.int32, (held_bias, LANES), 0)
    to_id = lax.broadcasted_iota(jnp.int32, (held_bias, LANES), 1)
    pick = jnp.where(lax.rem(from_id, group) == lax.rem(to_id, group), 1.0, 0.0).astype(jnp.bfloat16)
    bias_own[...] = jnp.dot(spread.astype(jnp.bfloat16), pick, preferred_element_type=jnp.float32)

    token_load.wait()
    step_rows = 16
    for first in range(0, tokens, step_rows):
        values = tok_ref[first : first + step_rows, :].astype(jnp.float32)
        mean = jnp.sum(values * values, axis=-1, keepdims=True) * (1.0 / depth)
        scaled = (values * lax.rsqrt(mean + EPSILON)).astype(jnp.bfloat16)
        for which in range(2):
            for owner in range(inst_count):
                at = (owner * 2 + which) * half_block
                xsend[which, first : first + step_rows, owner * half_block : (owner + 1) * half_block] = scaled[
                    :, at : at + half_block
                ]
    pl.semaphore_wait(barrier, devices - 1)

    def send_x(name, piece):
        which, device, side = {
            "xf": (1 - half, z_near * 2 + y, 0),
            "xm": (half, z_mate * 2 + y, 0),
            "xy": (half, z * 2 + 1 - y, 1),
        }[name]
        own_x(which, device, side, piece).start()

    def early(steps):
        for name, piece, _ in steps:
            if name not in ("xf", "xm", "xy"):
                break
            send_x(name, piece)

    each(inner, lambda: early(INNER))
    each(jnp.logical_not(inner), lambda: early(OUTER))
    xbuf[0, half, lax.rem(z, 2)] = xsend[half]

    weight_load.wait()
    for rank in range(TP):
        starts = (
            (rank * query, 0, query),
            (TP * query + rank * pair, query, pair),
            (TP * (query + pair) + rank * pair, query + pair, pair),
        )
        for source, target, extent in starts:
            for inside in range(0, extent, LANES):
                part = w_ref[:, source + inside : source + inside + LANES].astype(jnp.bfloat16).astype(jnp.float32)
                wsend[rank, (target + inside) // LANES] = (part * gain).astype(jnp.bfloat16)

    def product(kind, lhs, j):
        _, first, count, at = chunk_of(kind, j)
        result = []
        for t in range(0, count, 2):
            width = min(2, count - t)
            rhs = [wbuf[:, at + t + u].reshape(4 * half_block, LANES) for u in range(width)]
            rhs = jnp.concatenate(rhs, axis=1) if width > 1 else rhs[0]
            value = jnp.dot(lhs, rhs, preferred_element_type=jnp.float32)
            for u in range(width):
                result.append((t + u, value[:, u * LANES : (u + 1) * LANES]))
        return result

    def finish_bias():
        @pl.loop(1, devices)
        def _(step):
            slot = lax.rem(flat + step, devices)

            @pl.when(needs(slot, me))
            def _():
                arrived(bbuf.at[slot], b_recv.at[slot])

        bbuf[flat] = bias_own[...]
        send_bias(True)

    def run(kind, steps):
        other = 1 - kind
        done = set()

        def once(key, action):
            if key not in done:
                done.add(key)
                action()

        def need_x(block):
            for piece in range(pieces):
                once(
                    ("x", block, piece),
                    lambda piece=piece: arrived(
                        mine(block, piece), x_recv.at[places[block], piece]
                    ),
                )

        def need_w(k, j):
            once(("w", k, j), lambda: arrived(held(kind, slot_of(inst, k), j), w_recv.at[k - 1, j]))

        def need_chunk(j):
            _, first, count, at = chunk_of(kind, j)

            def action():
                arrived(wbuf.at[pl.ds(0, 8), pl.ds(at, count)], wc_recv.at[j])
                wbuf[slot_of(inst, 0), at : at + count] = fresh(kind, z, j, y)[...]

            once(("c", j), action)

        def mine(block, piece):
            return piece_of(xbuf.at[0, places[block] // 2, lax.rem(places[block], 2)], piece)

        def need_tokens(unit):
            if unit < 2:
                for block in ((1,), (2, 3))[unit]:
                    need_x(block)
            else:
                part = half if unit == 2 else 1 - half
                once(("y", unit), lambda: arrived(xbuf.at[1, part], x1_recv.at[part]))

        places = (z, z_mate, z_near, z_end)

        def step_rx(block, piece):
            once(
                ("x", block, piece),
                lambda: arrived(mine(block, piece), x_recv.at[places[block], piece]),
            )
            relay_x(0, places[block], piece).start()

        def step_ry(block, piece):
            once(
                ("x", block, piece),
                lambda: arrived(mine(block, piece), x_recv.at[places[block], piece]),
            )
            relay_x(1, places[block], piece).start()

        def step_wp(j, k):
            mine = slot_of(inst, 0)
            if k == 1:
                source, target, device = fresh(kind, z, j, 1 - y), held(kind, mine, j), z * 2 + 1 - y
            else:
                source, target, device = fresh(other, z_mate, j, y), held(other, mine, j), z_mate * 2 + y
            remote(source, target, w_send.at[k - 1], w_recv.at[k - 1, j], (inst, device)).start()

        def step_wd(j, _):
            _, _, count, at = chunk_of(other, j)
            target = dbuf.at[pl.ds(at, count)]
            remote(
                fresh(other, z_mate, j, 1 - y), target, w_send.at[2], d_recv.at[j], (inst, z_mate * 2 + y)
            ).start()

        def step_we(j, _):
            _, _, count, at = chunk_of(other, j)
            remote(
                fresh(other, z_mate, j, 1 - y), ebuf.at[pl.ds(at, count)], w_send.at[6], e_recv.at[j], (inst, z * 2 + 1 - y)
            ).start()

        def step_re(j, _):
            _, _, count, at = chunk_of(other, j)
            source = ebuf.at[pl.ds(at, count)]
            arrived(source, e_recv.at[j])
            target = held(other, slot_of(inst, 1), j)
            remote(source, target, w_send.at[7], w_recv.at[2, j], (inst, z_mate * 2 + y)).start()

        def step_rd(j, _):
            _, _, count, at = chunk_of(kind, j)
            source = dbuf.at[pl.ds(at, count)]
            arrived(source, d_recv.at[j])
            target = held(kind, slot_of(inst, 2), j)
            remote(source, target, w_send.at[3], w_recv.at[2, j], (inst, z * 2 + 1 - y)).start()

        def send_block(j, k, source, across):
            device, send, recv = (
                ((x_peer, me), w_send.at[4], wx_recv.at[k, j]),
                ((core_peer, me), w_send.at[5], wc_recv.at[j]),
            )[across]
            remote(source, held(kind, slot_of(inst, k), j), send, recv, device).start()

        def step_ox(j, _):
            send_block(j, 0, fresh(kind, z, j, y), 0)

        def step_ko(j, _):
            send_block(j, 0, fresh(kind, z, j, y), 1)

        def step_rw(j, k):
            need_w(k, j)
            send_block(j, k, held(kind, slot_of(inst, k), j), 0)

        def step_kw(j, k):
            need_w(k, j)
            send_block(j, k, held(kind, slot_of(inst, k), j), 1)

        def step_rc(j, k):
            block = held(kind, slot_of(x_peer, k), j)
            arrived(block, wx_recv.at[k, j])
            remote(block, block, w_send.at[5], wc_recv.at[j], (core_peer, me)).start()

        def step_pm(unit, j):
            need_tokens(unit)
            need_chunk(j)
            what, first, count, at = chunk_of(kind, j)
            side, part = unit // 2, (1 - half if unit % 2 else half)
            lhs = xbuf[side, part].reshape(2 * tokens, 4 * half_block)
            for t, value in product(kind, lhs, j):
                psend[side, part, at + t] = value.astype(jnp.bfloat16)
            target = other if what == "far" else kind
            index = incoming(target).index((first, count))
            remote(
                psend.at[side, part, pl.ds(at, count)],
                pbuf.at[side, part, pl.ds(first, count)],
                p_send.at[0],
                p_recv.at[side, part, index],
                (inst, (z_pair if what == "far" else z_near) * 2 + y),
            ).start()

        def step_om(m, j):
            for unit in (0, 1) if m == 0 else (2, 3):
                need_tokens(unit)
            need_chunk(j)
            first = chunk_of(kind, j)[1]
            lhs = xbuf[m].reshape(4 * tokens, 4 * half_block)
            for t, value in product(kind, lhs, j):
                for part in range(2):
                    acc[m, part, first + t] = value[part * 2 * tokens : (part + 1) * 2 * tokens]

        def step_fin(unit, j):
            once("bias", finish_bias)
            _, first, count, _ = chunk_of(kind, j)
            side, part = unit // 2, (1 - half if unit % 2 else half)
            for index, (low, extent) in enumerate(incoming(kind)):
                if low < first + count and first < low + extent:
                    once(
                        ("p", unit, index),
                        lambda: arrived(
                            pbuf.at[side, part, pl.ds(low, extent)], p_recv.at[side, part, index]
                        ),
                    )
            where = 1 - y if side else y
            for t in range(first, first + count):
                value = acc[side, part, t] + pbuf[side, part, t].astype(jnp.float32) + bias_row(column_of(t) // group)
                value = value.astype(jnp.bfloat16)
                for k in range(2):
                    out_ref[part * 2 + k, where, :, t * LANES : (t + 1) * LANES] = value[k * tokens : (k + 1) * tokens]

        def step_bias(*_):
            send_bias(False)

        table = dict(
            xy=lambda piece, _: send_x("xy", piece),
            xf=lambda piece, _: send_x("xf", piece),
            xm=lambda piece, _: send_x("xm", piece),
            rx=step_rx,
            ry=step_ry,
            wp=step_wp,
            wd=step_wd,
            rd=step_rd,
            we=step_we,
            re=step_re,
            ox=step_ox,
            ko=step_ko,
            rw=step_rw,
            kw=step_kw,
            rc=step_rc,
            pm=step_pm,
            om=step_om,
            fin=step_fin,
            bias=step_bias,
        )
        start = next(i for i, step in enumerate(steps) if step[0] not in ("xf", "xm", "xy"))
        for name, first, second in steps[start:]:
            table[name](first, second)

        counts = [sum(c[2] for c in CHUNKS[way]) for way in range(2)]
        sent = counts[kind] - tiles
        three = xbuf.at[0, :, :, pl.ds(0, 3 * tokens // 4)]
        arrived(three, x_send.at[0])
        arrived(three, x_send.at[2])
        if kind == 0:
            arrived(xbuf.at[0, 0], x_send.at[1])
        across = [sum(c[2] for j, c in enumerate(CHUNKS[way]) if j in ACROSS[way]) for way in range(2)]
        for way, extent in (
            (0, counts[kind]),
            (1, counts[other]),
            (2, counts[other] - across[other]),
            (3, counts[kind] - across[kind]),
            (6, across[other]),
            (7, across[other]),
        ):
            if extent:
                arrived(wbuf.at[0, pl.ds(0, extent)], w_send.at[way])
        arrived(wbuf.at[pl.ds(0, 4), pl.ds(0, counts[kind])], w_send.at[4])
        arrived(wbuf.at[pl.ds(0, 8), pl.ds(0, counts[kind])], w_send.at[5])
        arrived(psend.at[:, :, pl.ds(0, sent)], p_send.at[0])

    each(inner, lambda: run(0, INNER))
    each(jnp.logical_not(inner), lambda: run(1, OUTER))


def kernel_device(dims, tokens, norm_gain, master_qkv, qkv_bias):
    inst_count, shard_count, group = dims
    devices = inst_count * shard_count
    rows = master_qkv.shape[0]
    count, depth = tokens.shape
    tiles = master_qkv.shape[1] // TP // LANES
    pieces = TOKEN_PIECES
    most = max(len(c) for c in CHUNKS)
    held = max(sum(c[2] for c in way) for way in CHUNKS)
    dma = pltpu.SemaphoreType.DMA
    vmem = pl.BlockSpec(memory_space=pltpu.VMEM)
    anywhere = pl.BlockSpec(memory_space=pl.ANY)
    low, wide = jnp.bfloat16, jnp.float32
    result = pl.pallas_call(
        functools.partial(kernel, dims),
        out_shape=pltpu.VMEM((4, 2, count, tiles * LANES), low),
        in_specs=[anywhere, vmem, anywhere, vmem],
        out_specs=vmem,
        scratch_shapes=[
            pltpu.VMEM((count, depth), low),
            pltpu.VMEM((rows, master_qkv.shape[1]), wide),
            pltpu.VMEM((2, count, depth // 2), low),
            pltpu.VMEM((2, 2, 2, count, depth // 2), low),
            pltpu.VMEM((TP, tiles, rows, LANES), low),
            pltpu.VMEM((4 * inst_count, held, rows, LANES), low),
            pltpu.VMEM((held, rows, LANES), low),
            pltpu.VMEM((held, rows, LANES), low),
            pltpu.VMEM((2, 2, held - tiles, 2 * count, LANES), low),
            pltpu.VMEM((2, 2, tiles, 2 * count, LANES), low),
            pltpu.VMEM((2, 2, tiles, 2 * count, LANES), wide),
            pltpu.VMEM((8, LANES), wide),
            pltpu.VMEM((devices, 8, LANES), wide),
            dma((2,)),
            dma((4, pieces)),
            dma((2,)),
            dma((3,)),
            dma((3, most)),
            dma((4, most)),
            dma((most,)),
            dma((most,)),
            dma((most,)),
            dma((8,)),
            dma((2, 2, most)),
            dma((1,)),
            dma((devices,)),
            dma((devices,)),
        ],
        compiler_params=pltpu.CompilerParams(
            collective_id=0, has_side_effects=True, vmem_limit_bytes=56 * 1024 * 1024
        ),
    )(tokens, norm_gain.reshape(1, rows), master_qkv, qkv_bias.reshape(1, -1))
    return result.reshape(1, shard_count * count, tiles * LANES)


def per_device(tokens, norm_gain, master_qkv, qkv_bias):
    inst_count, shard_count = lax.axis_size("inst"), lax.axis_size("shard")
    group = 32
    fits = (
        shard_count == TP
        and inst_count == 4
        and master_qkv.shape[0] % 16 == 0
        and tokens.shape[0] % (16 * TOKEN_PIECES) == 0
        and QHEADS * HEAD_DIM // TP % LANES == 0
        and KVHEADS * HEAD_DIM // TP == LANES
        and 4 * master_qkv.shape[0] % LANES == 0
        and qkv_bias.shape[0] % group == 0
    )
    if fits:
        return kernel_device((inst_count, shard_count, group), tokens, norm_gain, master_qkv, qkv_bias)
    return general_device(tokens, norm_gain, master_qkv, qkv_bias)


def solution(mesh):
    in_specs = (
        P(("inst", "shard"), None),
        P(("inst", "shard")),
        P(("inst", "shard"), None),
        P(("inst", "shard")),
    )
    out_specs = P(("inst", "shard"), None, None)
    return jax.shard_map(
        per_device, mesh=mesh, in_specs=in_specs, out_specs=out_specs, check_vma=False
    )
```

```python
import functools

import jax
import jax.numpy as jnp
from jax import lax
from jax.experimental import pallas as pl
from jax.experimental.pallas import tpu as pltpu
from jax.sharding import PartitionSpec as P

QHEADS = 40
KVHEADS = 8
HEAD_DIM = 128
TP = 8


EPSILON = 1e-06
MESH = pl.DeviceIdType.MESH
LANES = 128
TOKEN_PIECES = 2
CHUNKS = (
    (("far", 0, 1), ("far", 1, 2), ("far", 3, 2), ("far", 5, 2), ("extra", 4, 3), ("own", 0, 2), ("own", 2, 2), ("own", 4, 3)),
    (("far", 0, 2), ("far", 2, 2), ("own", 0, 2), ("own", 2, 2), ("own", 4, 3)),
)
ACROSS = ((5, 6, 7), ())
INNER = (
    ("xm", 1, 0),
    ("xf", 1, 0),
    ("xf", 0, 0),
    ("xy", 0, 0),
    ("wp", 0, 2),
    ("wp", 4, 1),
    ("ox", 5, 0),
    ("ox", 2, 0),
    ("ko", 5, 0),
    ("ox", 0, 0),
    ("ko", 2, 0),
    ("xm", 0, 0),
    ("rc", 5, 0),
    ("ox", 1, 0),
    ("ko", 0, 0),
    ("ox", 4, 0),
    ("ko", 1, 0),
    ("ry", 2, 1),
    ("rc", 2, 0),
    ("wp", 1, 1),
    ("rc", 0, 0),
    ("ko", 4, 0),
    ("rw", 4, 1),
    ("rc", 1, 0),
    ("rx", 2, 0),
    ("wd", 1, 0),
    ("kw", 4, 1),
    ("rw", 1, 2),
    ("rd", 4, 0),
    ("rc", 4, 0),
    ("ry", 2, 0),
    ("kw", 1, 2),
    ("rw", 4, 2),
    ("wp", 3, 2),
    ("rc", 4, 1),
    ("kw", 4, 2),
    ("wd", 0, 0),
    ("rc", 1, 2),
    ("rw", 4, 3),
    ("rx", 2, 1),
    ("rw", 1, 1),
    ("kw", 4, 3),
    ("ry", 3, 1),
    ("rc", 4, 2),
    ("ox", 3, 0),
    ("kw", 1, 1),
    ("rx", 3, 0),
    ("ry", 3, 0),
    ("rc", 4, 3),
    ("ox", 6, 0),
    ("ko", 3, 0),
    ("wp", 1, 2),
    ("wp", 6, 1),
    ("pm", 1, 4),
    ("rc", 1, 1),
    ("ox", 7, 0),
    ("pm", 0, 4),
    ("rc", 3, 0),
    ("ko", 6, 0),
    ("ko", 7, 0),
    ("rw", 2, 2),
    ("rx", 3, 1),
    ("rc", 6, 0),
    ("rd", 2, 0),
    ("pm", 3, 4),
    ("wd", 4, 0),
    ("wp", 3, 1),
    ("kw", 2, 2),
    ("rw", 6, 1),
    ("wp", 5, 1),
    ("rc", 7, 0),
    ("kw", 6, 1),
    ("wd", 3, 0),
    ("rc", 2, 2),
    ("rw", 3, 2),
    ("kw", 3, 2),
    ("rd", 1, 0),
    ("rw", 3, 1),
    ("wp", 0, 1),
    ("rc", 6, 1),
    ("kw", 3, 1),
    ("wp", 4, 2),
    ("rw", 5, 1),
    ("rd", 3, 0),
    ("rc", 3, 2),
    ("wp", 2, 2),
    ("wp", 2, 1),
    ("rw", 1, 3),
    ("rc", 3, 1),
    ("kw", 1, 3),
    ("rw", 0, 1),
    ("wp", 7, 1),
    ("wd", 2, 0),
    ("rc", 5, 1),
    ("rw", 2, 3),
    ("kw", 0, 1),
    ("ry", 1, 1),
    ("kw", 2, 3),
    ("rc", 1, 3),
    ("rw", 2, 1),
    ("pw", 1, 0),
    ("bias", 0, 0),
    ("rc", 0, 1),
    ("rw", 3, 3),
    ("kw", 2, 1),
    ("pm", 0, 1),
    ("pm", 1, 1),
    ("pm", 3, 1),
    ("rc", 2, 3),
    ("kw", 3, 3),
    ("rw", 7, 1),
    ("rc", 2, 1),
    ("kw", 5, 1),
    ("kw", 7, 1),
    ("rd", 0, 0),
    ("xy", 1, 0),
    ("rw", 0, 2),
    ("ry", 1, 0),
    ("pm", 0, 2),
    ("pm", 1, 2),
    ("rc", 3, 3),
    ("pm", 3, 2),
    ("kw", 0, 2),
    ("rw", 5, 2),
    ("pm", 0, 3),
    ("pm", 1, 3),
    ("rw", 0, 3),
    ("kw", 5, 2),
    ("pm", 3, 3),
    ("rc", 7, 1),
    ("rc", 0, 2),
    ("kw", 0, 3),
    ("rw", 7, 3),
    ("kw", 7, 3),
    ("rc", 5, 2),
    ("rw", 5, 3),
    ("rc", 0, 3),
    ("kw", 5, 3),
    ("pm", 0, 0),
    ("pm", 1, 0),
    ("pm", 3, 0),
    ("pm", 2, 0),
    ("rw", 7, 2),
    ("pm", 2, 1),
    ("rc", 7, 3),
    ("pm", 2, 2),
    ("kw", 7, 2),
    ("pm", 2, 3),
    ("pm", 2, 4),
    ("rw", 6, 3),
    ("rc", 5, 3),
    ("kw", 6, 3),
    ("bw", 0, 0),
    ("rw", 6, 2),
    ("om", 0, 5),
    ("om", 1, 5),
    ("rc", 7, 2),
    ("kw", 6, 2),
    ("fin", 0, 5),
    ("fin", 1, 5),
    ("fin", 2, 5),
    ("fin", 3, 5),
    ("om", 0, 7),
    ("rc", 6, 3),
    ("om", 1, 7),
    ("rc", 6, 2),
    ("fin", 0, 7),
    ("fin", 1, 7),
    ("fin", 2, 7),
    ("om", 0, 6),
    ("om", 1, 6),
    ("fin", 1, 6),
    ("fin", 0, 6),
    ("fin", 2, 6),
    ("fin", 3, 6),
    ("fin", 3, 7),
)
OUTER = (
    ("xm", 1, 0),
    ("xy", 0, 0),
    ("wd", 4, 0),
    ("wp", 0, 1),
    ("ox", 1, 0),
    ("ox", 2, 0),
    ("ko", 1, 0),
    ("ox", 0, 0),
    ("ko", 2, 0),
    ("wp", 1, 2),
    ("wp", 1, 1),
    ("rc", 2, 0),
    ("rc", 1, 0),
    ("ox", 3, 0),
    ("ko", 0, 0),
    ("xy", 1, 0),
    ("ko", 3, 0),
    ("wp", 4, 2),
    ("rw", 0, 1),
    ("rc", 0, 0),
    ("ox", 4, 0),
    ("kw", 0, 1),
    ("xf", 1, 0),
    ("rc", 3, 0),
    ("rw", 0, 2),
    ("ko", 4, 0),
    ("ry", 1, 0),
    ("xf", 0, 0),
    ("rc", 0, 1),
    ("rw", 1, 1),
    ("kw", 0, 2),
    ("rc", 4, 0),
    ("kw", 1, 1),
    ("ry", 2, 0),
    ("xm", 0, 0),
    ("ry", 1, 1),
    ("rc", 0, 2),
    ("rc", 1, 1),
    ("rw", 3, 2),
    ("kw", 3, 2),
    ("wp", 2, 2),
    ("rd", 0, 0),
    ("rc", 3, 2),
    ("wd", 2, 0),
    ("rd", 1, 0),
    ("wp", 3, 2),
    ("ry", 2, 1),
    ("rw", 0, 3),
    ("kw", 0, 3),
    ("wd", 3, 0),
    ("wd", 1, 0),
    ("ry", 3, 0),
    ("rw", 1, 3),
    ("kw", 1, 3),
    ("rc", 0, 3),
    ("rw", 1, 2),
    ("kw", 1, 2),
    ("pm", 0, 0),
    ("pm", 2, 0),
    ("rc", 1, 3),
    ("rc", 1, 2),
    ("ry", 3, 1),
    ("pm", 1, 0),
    ("pm", 0, 1),
    ("pm", 1, 1),
    ("pm", 2, 1),
    ("rd", 4, 0),
    ("rd", 3, 0),
    ("pm", 3, 0),
    ("pm", 3, 1),
    ("we", 7, 0),
    ("rw", 4, 2),
    ("kw", 4, 2),
    ("wp", 3, 1),
    ("wd", 0, 0),
    ("rw", 3, 3),
    ("rw", 4, 3),
    ("kw", 3, 3),
    ("wp", 0, 2),
    ("we", 5, 0),
    ("wp", 5, 2),
    ("rc", 4, 2),
    ("kw", 4, 3),
    ("re", 7, 0),
    ("wp", 4, 1),
    ("rc", 3, 3),
    ("rw", 3, 1),
    ("rw", 2, 2),
    ("kw", 3, 1),
    ("we", 6, 0),
    ("pw", 1, 1),
    ("bias", 0, 0),
    ("rc", 4, 3),
    ("kw", 2, 2),
    ("re", 5, 0),
    ("wp", 7, 2),
    ("rd", 2, 0),
    ("rc", 3, 1),
    ("rw", 4, 1),
    ("wp", 2, 1),
    ("om", 0, 3),
    ("rc", 2, 2),
    ("om", 1, 3),
    ("re", 6, 0),
    ("kw", 4, 1),
    ("wp", 6, 2),
    ("rw", 2, 3),
    ("kw", 2, 3),
    ("rc", 4, 1),
    ("rw", 2, 1),
    ("kw", 2, 1),
    ("om", 0, 4),
    ("om", 1, 4),
    ("bw", 0, 0),
    ("fin", 1, 3),
    ("fin", 2, 3),
    ("fin", 0, 3),
    ("rc", 2, 3),
    ("fin", 0, 4),
    ("fin", 1, 4),
    ("fin", 2, 4),
    ("rc", 2, 1),
    ("om", 0, 2),
    ("om", 1, 2),
    ("fin", 0, 2),
    ("fin", 1, 2),
    ("fin", 2, 2),
    ("fin", 3, 4),
    ("fin", 3, 2),
    ("fin", 3, 3),
)


def partner_2(value, axis, distance):
    mask = 2**distance
    pairs = [(source, source ^ mask) for source in range(lax.axis_size(axis))]
    return lax.ppermute(value, axis, pairs)


def rank_columns(matrix):
    query_cols = QHEADS * HEAD_DIM
    pair_cols = KVHEADS * HEAD_DIM
    leading = matrix.shape[:-1]
    query = matrix[..., :query_cols].reshape(leading + (TP, query_cols // TP))
    keys = matrix[..., query_cols : query_cols + pair_cols].reshape(leading + (TP, pair_cols // TP))
    values = matrix[..., query_cols + pair_cols :].reshape(leading + (TP, pair_cols // TP))
    return jnp.concatenate([query, keys, values], axis=-1)


def normalize(tokens, gain):
    floats = tokens.astype(jnp.float32)
    scale = lax.rsqrt(jnp.mean(floats * floats, axis=-1, keepdims=True) + EPSILON)
    return (floats * scale * gain.astype(jnp.float32)).astype(jnp.bfloat16)


def general_device(tokens, norm_gain, master_qkv, qkv_bias):
    shard_count = lax.axis_size("shard")
    local_rows = master_qkv.shape[0]
    rank_width = master_qkv.shape[1] // TP
    gain_full, bias_full = (
        lax.all_gather(norm_gain.astype(jnp.bfloat16), ("inst", "shard"), axis=0, tiled=True),
        lax.all_gather(qkv_bias.astype(jnp.bfloat16), ("inst", "shard"), axis=0, tiled=True),
    )
    normed = normalize(tokens, gain_full)
    shard_pos = lax.axis_index("shard")
    rank_index = shard_pos % TP
    bit_count = TP.bit_length() - 1
    bit_order = list(range(bit_count))
    group_rows = normed
    for bit_pos in bit_order:
        partner = partner_2(group_rows, "shard", bit_pos)
        lower = jnp.bitwise_and(jnp.right_shift(shard_pos, bit_pos), 1) == 0
        group_rows = jnp.where(
            lower,
            jnp.concatenate([group_rows, partner], 0),
            jnp.concatenate([partner, group_rows], 0),
        )
    copies = shard_count // TP
    inst_block = shard_count * local_rows
    rows_low = master_qkv.astype(jnp.bfloat16)
    ranked = jnp.transpose(rank_columns(rows_low), (1, 0, 2))
    spread = jnp.broadcast_to(ranked[None], (copies,) + ranked.shape)
    outgoing = spread.reshape(shard_count, rows_low.shape[0], rank_width)
    arrived = lax.all_to_all(outgoing, "shard", split_axis=0, concat_axis=0, tiled=True).reshape(
        inst_block, rank_width
    )
    product = jnp.dot(
        group_rows,
        lax.all_gather(arrived, "inst", axis=0, tiled=True),
        preferred_element_type=jnp.float32,
    )
    bias_ranks = rank_columns(bias_full)
    bias_mine = lax.dynamic_index_in_dim(bias_ranks, rank_index, 0, keepdims=False)
    result = (product + bias_mine.astype(jnp.float32)).astype(jnp.bfloat16)
    return result[None]


def incoming(kind):
    chunks = [c for c in CHUNKS[1 - kind] if c[0] == "far"]
    return [c[1:] for c in chunks + [c for c in CHUNKS[kind] if c[0] == "extra"]]


def chunk_of(kind, j):
    what, first, count = CHUNKS[kind][j]
    return what, first, count, sum(c[2] for c in CHUNKS[kind][:j])


def kernel(
    dims,
    tok_hbm,
    gain_hbm,
    w_hbm,
    bias_hbm,
    out_ref,
    gain_ref,
    bias_ref,
    tok_ref,
    w_ref,
    xsend,
    xbuf,
    wsend,
    wbuf,
    dbuf,
    ebuf,
    psend,
    pbuf,
    acc,
    bias_own,
    bbuf,
    load_sem,
    x_recv,
    x1_recv,
    x_send,
    w_recv,
    wx_recv,
    wc_recv,
    d_recv,
    e_recv,
    w_send,
    p_recv,
    p_send,
    b_recv,
    b_send,
):
    inst_count, shard_count, group = dims
    devices = inst_count * shard_count
    inst = lax.axis_index("inst")
    me = lax.axis_index("shard")
    z = me // 2
    y = lax.rem(me, 2)
    half = z // 2
    flat = inst * shard_count + me
    core_peer = inst + 1 - 2 * lax.rem(inst, 2)
    x_peer = lax.rem(inst + 2, inst_count)
    z_mate = z + 1 - 2 * lax.rem(z, 2)
    z_pair = lax.rem(z + 2, 4)
    z_near = 2 - half
    z_end = 3 - 3 * half
    inner = z_near + z == 3
    rows = w_ref.shape[0]
    tokens, depth = tok_ref.shape
    tiles = wsend.shape[1]
    half_block = 4 * rows
    pieces = TOKEN_PIECES
    piece_rows = tokens // pieces

    halves = 2
    step_rows = tokens // halves
    row_cut = rows // 2

    def token_load(q):
        part = pl.ds(q * step_rows, step_rows)
        return pltpu.make_async_copy(tok_hbm.at[part], tok_ref.at[part], load_sem.at[q])

    def weight_load(q):
        part = pl.ds(q * row_cut, row_cut)
        return pltpu.make_async_copy(w_hbm.at[part], w_ref.at[part], load_sem.at[2 + q])

    for q in range(halves):
        token_load(q).start()

    barrier = pltpu.get_barrier_semaphore()

    def greet(owner, there):
        pl.semaphore_signal(barrier, inc=1, device_id=(owner, there), device_id_type=MESH)

    greet(inst, z_pair * 2 + y)
    greet(inst, z_mate * 2 + y)
    greet(inst, z * 2 + 1 - y)
    greet(x_peer, me)
    greet(core_peer, me)
    pl.when(inner)(lambda: greet(inst, z_near * 2 + y))
    for q in range(2):
        weight_load(q).start()
    small_load = (
        pltpu.make_async_copy(gain_hbm, gain_ref, load_sem.at[4]),
        pltpu.make_async_copy(bias_hbm, bias_ref, load_sem.at[5]),
    )
    for copy in small_load:
        copy.start()

    def remote(source, target, send_sem, recv_sem, device):
        return pltpu.make_async_remote_copy(
            src_ref=source,
            dst_ref=target,
            send_sem=send_sem,
            recv_sem=recv_sem,
            device_id=device,
            device_id_type=MESH,
        )

    def each(condition, action):
        pl.when(condition)(action)

    def piece_of(ref, piece):
        return ref.at[pl.ds(piece * piece_rows, piece_rows)]

    def own_x(which, device, side, piece):
        return remote(
            piece_of(xsend.at[which], piece),
            piece_of(xbuf.at[side, half, lax.rem(z, 2)], piece),
            x_send.at[0],
            x1_recv.at[half] if side else x_recv.at[z, piece],
            (inst, device),
        )

    def relay_x(way, block, piece):
        device, side = ((z_mate * 2 + y, 0), (z * 2 + 1 - y, 1))[way]
        return remote(
            piece_of(xbuf.at[0, block // 2, lax.rem(block, 2)], piece),
            piece_of(xbuf.at[side, block // 2, lax.rem(block, 2)], piece),
            x_send.at[1 + way],
            x1_recv.at[block // 2] if side else x_recv.at[block, piece],
            (inst, device),
        )

    def slot_of(owner, k):
        return owner * 4 + lax.rem(z_mate if k // 2 else z, 2) * 2 + (1 - y if k % 2 else y)

    def fresh(kind, there, j, side):
        what, first, count, _ = chunk_of(kind, j)
        rank = {"far": lax.rem(there + 2, 4), "extra": z_near, "own": there}[what] * 2 + side
        return wsend.at[rank, pl.ds(first, count)]

    def held(kind, slot, j):
        _, _, count, at = chunk_of(kind, j)
        return wbuf.at[slot, pl.ds(at, count)]

    def arrived(ref, sem):
        pltpu.make_async_copy(ref, ref, sem).wait()

    query = QHEADS * HEAD_DIM // TP
    pair = KVHEADS * HEAD_DIM // TP
    held_bias = bias_ref.shape[1]
    per_row = LANES // group
    groups = held_bias // group

    def needs(owner, rank):
        low, high = owner * held_bias, owner * held_bias + held_bias
        result = None
        for start, extent in (
            (rank * query, query),
            (TP * query + rank * pair, pair),
            (TP * (query + pair) + rank * pair, pair),
        ):
            overlap = jnp.logical_and(start < high, low < start + extent)
            result = overlap if result is None else jnp.logical_or(result, overlap)
        return result

    def bias_copy(step):
        there = lax.rem(flat + step, devices)
        return remote(
            bias_own,
            bbuf.at[flat],
            b_send.at[step],
            b_recv.at[flat],
            (there // shard_count, lax.rem(there, shard_count)),
        )

    def send_bias(finish):
        @pl.loop(1, devices)
        def _(step):
            there = lax.rem(flat + step, devices)

            @pl.when(needs(flat, lax.rem(there, shard_count)))
            def _():
                if finish:
                    bias_copy(step).wait_send()
                else:
                    bias_copy(step).start()

    def bias_row(number_first):
        lane = lax.broadcasted_iota(jnp.int32, (1, LANES), 1) // group
        row = jnp.zeros((1, LANES), jnp.float32)
        for q in range(per_row):
            number = number_first + q
            row = jnp.where(lane == q, bbuf[number // groups, pl.ds(lax.rem(number, groups), 1), :], row)
        return row

    def column_of(t):
        at = t * LANES
        if at < query:
            return me * query + at
        if at < query + pair:
            return TP * query + me * pair + (at - query)
        return TP * (query + pair) + me * pair + (at - query - pair)

    narrow = 16
    for first in range(0, tokens, narrow):
        if first % step_rows == 0:
            token_load(first // step_rows).wait()
        values = tok_ref[first : first + narrow, :].astype(jnp.float32)
        mean = jnp.sum(values * values, axis=-1, keepdims=True) * (1.0 / depth)
        scaled = (values * lax.rsqrt(mean + EPSILON)).astype(jnp.bfloat16)
        for which in range(2):
            for owner in range(inst_count):
                at = (owner * 2 + which) * half_block
                xsend[which, first : first + narrow, owner * half_block : (owner + 1) * half_block] = scaled[
                    :, at : at + half_block
                ]
    pl.semaphore_wait(barrier, jnp.where(inner, 6, 5))

    def send_x(name, piece):
        which, device, side = {
            "xf": (1 - half, z_near * 2 + y, 0),
            "xm": (half, z_mate * 2 + y, 0),
            "xy": (half, z * 2 + 1 - y, 1),
        }[name]
        own_x(which, device, side, piece).start()

    def early(steps):
        for name, piece, _ in steps:
            if name not in ("xf", "xm", "xy"):
                break
            send_x(name, piece)

    each(inner, lambda: early(INNER))
    each(jnp.logical_not(inner), lambda: early(OUTER))
    xbuf[0, half, lax.rem(z, 2)] = xsend[half]

    small_load[0].wait()
    ids = lax.broadcasted_iota(jnp.int32, (rows, rows), 0), lax.broadcasted_iota(jnp.int32, (rows, rows), 1)
    gain_row = gain_ref[...].astype(jnp.bfloat16).astype(jnp.float32)
    gain = jnp.sum(jnp.where(ids[0] == ids[1], jnp.broadcast_to(gain_row, (rows, rows)), 0.0), axis=1, keepdims=True)
    for q in range(2):
        weight_load(q).wait()
    for rank in range(TP):
        starts = (
            (rank * query, 0, query),
            (TP * query + rank * pair, query, pair),
            (TP * (query + pair) + rank * pair, query + pair, pair),
        )
        for source, target, extent in starts:
            for inside in range(0, extent, LANES):
                part = w_ref[:, source + inside : source + inside + LANES].astype(jnp.bfloat16).astype(jnp.float32)
                wsend[rank, (target + inside) // LANES] = (part * gain).astype(jnp.bfloat16)

    def product(kind, lhs, j):
        _, first, count, at = chunk_of(kind, j)
        result = []
        for t in range(0, count, 2):
            width = min(2, count - t)
            rhs = [wbuf[:, at + t + u].reshape(4 * half_block, LANES) for u in range(width)]
            rhs = jnp.concatenate(rhs, axis=1) if width > 1 else rhs[0]
            value = jnp.dot(lhs, rhs, preferred_element_type=jnp.float32)
            for u in range(width):
                result.append((t + u, value[:, u * LANES : (u + 1) * LANES]))
        return result

    def finish_bias():
        @pl.loop(1, devices)
        def _(step):
            slot = lax.rem(flat + step, devices)

            @pl.when(needs(slot, me))
            def _():
                arrived(bbuf.at[slot], b_recv.at[slot])

        bbuf[flat] = bias_own[...]
        send_bias(True)

    def run(kind, steps):
        other = 1 - kind
        done = set()

        def once(key, action):
            if key not in done:
                done.add(key)
                action()

        def need_x(block):
            for piece in range(pieces):
                once(
                    ("x", block, piece),
                    lambda piece=piece: arrived(
                        mine(block, piece), x_recv.at[places[block], piece]
                    ),
                )

        def need_w(k, j):
            once(("w", k, j), lambda: arrived(held(kind, slot_of(inst, k), j), w_recv.at[k - 1, j]))

        def need_chunk(j):
            _, first, count, at = chunk_of(kind, j)

            def action():
                arrived(wbuf.at[pl.ds(0, 8), pl.ds(at, count)], wc_recv.at[j])
                wbuf[slot_of(inst, 0), at : at + count] = fresh(kind, z, j, y)[...]

            once(("c", j), action)

        def mine(block, piece):
            return piece_of(xbuf.at[0, places[block] // 2, lax.rem(places[block], 2)], piece)

        def need_tokens(unit):
            if unit < 2:
                for block in ((1,), (2, 3))[unit]:
                    need_x(block)
            else:
                part = half if unit == 2 else 1 - half
                once(("y", unit), lambda: arrived(xbuf.at[1, part], x1_recv.at[part]))

        places = (z, z_mate, z_near, z_end)

        def step_rx(block, piece):
            once(
                ("x", block, piece),
                lambda: arrived(mine(block, piece), x_recv.at[places[block], piece]),
            )
            relay_x(0, places[block], piece).start()

        def step_ry(block, piece):
            once(
                ("x", block, piece),
                lambda: arrived(mine(block, piece), x_recv.at[places[block], piece]),
            )
            relay_x(1, places[block], piece).start()

        def step_wp(j, k):
            mine = slot_of(inst, 0)
            if k == 1:
                source, target, device = fresh(kind, z, j, 1 - y), held(kind, mine, j), z * 2 + 1 - y
            else:
                source, target, device = fresh(other, z_mate, j, y), held(other, mine, j), z_mate * 2 + y
            remote(source, target, w_send.at[k - 1], w_recv.at[k - 1, j], (inst, device)).start()

        def step_wd(j, _):
            _, _, count, at = chunk_of(other, j)
            target = dbuf.at[pl.ds(at, count)]
            remote(
                fresh(other, z_mate, j, 1 - y), target, w_send.at[2], d_recv.at[j], (inst, z_mate * 2 + y)
            ).start()

        def step_we(j, _):
            _, _, count, at = chunk_of(other, j)
            remote(
                fresh(other, z_mate, j, 1 - y), ebuf.at[pl.ds(at, count)], w_send.at[6], e_recv.at[j], (inst, z * 2 + 1 - y)
            ).start()

        def step_re(j, _):
            _, _, count, at = chunk_of(other, j)
            source = ebuf.at[pl.ds(at, count)]
            arrived(source, e_recv.at[j])
            target = held(other, slot_of(inst, 1), j)
            remote(source, target, w_send.at[7], w_recv.at[2, j], (inst, z_mate * 2 + y)).start()

        def step_rd(j, _):
            _, _, count, at = chunk_of(kind, j)
            source = dbuf.at[pl.ds(at, count)]
            arrived(source, d_recv.at[j])
            target = held(kind, slot_of(inst, 2), j)
            remote(source, target, w_send.at[3], w_recv.at[2, j], (inst, z * 2 + 1 - y)).start()

        def send_block(j, k, source, across):
            device, send, recv = (
                ((x_peer, me), w_send.at[4], wx_recv.at[k, j]),
                ((core_peer, me), w_send.at[5], wc_recv.at[j]),
            )[across]
            remote(source, held(kind, slot_of(inst, k), j), send, recv, device).start()

        def step_ox(j, _):
            send_block(j, 0, fresh(kind, z, j, y), 0)

        def step_ko(j, _):
            send_block(j, 0, fresh(kind, z, j, y), 1)

        def step_rw(j, k):
            need_w(k, j)
            send_block(j, k, held(kind, slot_of(inst, k), j), 0)

        def step_kw(j, k):
            need_w(k, j)
            send_block(j, k, held(kind, slot_of(inst, k), j), 1)

        def step_rc(j, k):
            block = held(kind, slot_of(x_peer, k), j)
            arrived(block, wx_recv.at[k, j])
            remote(block, block, w_send.at[5], wc_recv.at[j], (core_peer, me)).start()

        def step_pm(unit, j):
            need_tokens(unit)
            need_chunk(j)
            what, first, count, at = chunk_of(kind, j)
            side, part = unit // 2, (1 - half if unit % 2 else half)
            lhs = xbuf[side, part].reshape(2 * tokens, 4 * half_block)
            for t, value in product(kind, lhs, j):
                psend[side, part, at + t] = value.astype(jnp.bfloat16)
            target = other if what == "far" else kind
            index = incoming(target).index((first, count))
            remote(
                psend.at[side, part, pl.ds(at, count)],
                pbuf.at[side, part, pl.ds(first, count)],
                p_send.at[0],
                p_recv.at[side, part, index],
                (inst, (z_pair if what == "far" else z_near) * 2 + y),
            ).start()

        def step_om(m, j):
            for unit in (0, 1) if m == 0 else (2, 3):
                need_tokens(unit)
            need_chunk(j)
            first = chunk_of(kind, j)[1]
            lhs = xbuf[m].reshape(4 * tokens, 4 * half_block)
            for t, value in product(kind, lhs, j):
                for part in range(2):
                    acc[m, part, first + t] = value[part * 2 * tokens : (part + 1) * 2 * tokens]

        def step_pw(unit, index):
            side, part = unit // 2, (1 - half if unit % 2 else half)
            low, extent = incoming(kind)[index]
            once(
                ("p", unit, index),
                lambda: arrived(pbuf.at[side, part, pl.ds(low, extent)], p_recv.at[side, part, index]),
            )

        def step_fin(unit, j):
            _, first, count, _ = chunk_of(kind, j)
            side, part = unit // 2, (1 - half if unit % 2 else half)
            for index, (low, extent) in enumerate(incoming(kind)):
                if low < first + count and first < low + extent:
                    step_pw(unit, index)
            where = 1 - y if side else y
            for t in range(first, first + count):
                value = acc[side, part, t] + pbuf[side, part, t].astype(jnp.float32) + bias_row(column_of(t) // group)
                value = value.astype(jnp.bfloat16)
                for k in range(2):
                    out_ref[part * 2 + k, where, :, t * LANES : (t + 1) * LANES] = value[k * tokens : (k + 1) * tokens]

        def step_bias(*_):
            small_load[1].wait()
            group_id = lax.broadcasted_iota(jnp.int32, (8, held_bias), 0)
            lane_id = lax.broadcasted_iota(jnp.int32, (8, held_bias), 1)
            spread = jnp.where(lane_id // group == group_id, jnp.broadcast_to(bias_ref[...], (8, held_bias)), 0.0)
            from_id = lax.broadcasted_iota(jnp.int32, (held_bias, LANES), 0)
            to_id = lax.broadcasted_iota(jnp.int32, (held_bias, LANES), 1)
            pick = jnp.where(lax.rem(from_id, group) == lax.rem(to_id, group), 1.0, 0.0).astype(jnp.bfloat16)
            bias_own[...] = jnp.dot(spread.astype(jnp.bfloat16), pick, preferred_element_type=jnp.float32)
            send_bias(False)

        table = dict(
            xy=lambda piece, _: send_x("xy", piece),
            xf=lambda piece, _: send_x("xf", piece),
            xm=lambda piece, _: send_x("xm", piece),
            rx=step_rx,
            ry=step_ry,
            wp=step_wp,
            wd=step_wd,
            rd=step_rd,
            we=step_we,
            re=step_re,
            ox=step_ox,
            ko=step_ko,
            rw=step_rw,
            kw=step_kw,
            rc=step_rc,
            pm=step_pm,
            om=step_om,
            fin=step_fin,
            bias=step_bias,
            bw=lambda *_: finish_bias(),
            pw=step_pw,
        )
        start = next(i for i, step in enumerate(steps) if step[0] not in ("xf", "xm", "xy"))
        for name, first, second in steps[start:]:
            table[name](first, second)

        counts = [sum(c[2] for c in CHUNKS[way]) for way in range(2)]
        sent = counts[kind] - tiles
        three = xbuf.at[0, :, :, pl.ds(0, 3 * tokens // 4)]
        arrived(three, x_send.at[0])
        arrived(three, x_send.at[2])
        if kind == 0:
            arrived(xbuf.at[0, 0], x_send.at[1])
        across = [sum(c[2] for j, c in enumerate(CHUNKS[way]) if j in ACROSS[way]) for way in range(2)]
        for way, extent in (
            (0, counts[kind]),
            (1, counts[other]),
            (2, counts[other] - across[other]),
            (3, counts[kind] - across[kind]),
            (6, across[other]),
            (7, across[other]),
        ):
            if extent:
                arrived(wbuf.at[0, pl.ds(0, extent)], w_send.at[way])
        arrived(wbuf.at[pl.ds(0, 4), pl.ds(0, counts[kind])], w_send.at[4])
        arrived(wbuf.at[pl.ds(0, 8), pl.ds(0, counts[kind])], w_send.at[5])
        arrived(psend.at[:, :, pl.ds(0, sent)], p_send.at[0])

    each(inner, lambda: run(0, INNER))
    each(jnp.logical_not(inner), lambda: run(1, OUTER))


def kernel_device(dims, tokens, norm_gain, master_qkv, qkv_bias):
    inst_count, shard_count, group = dims
    devices = inst_count * shard_count
    rows = master_qkv.shape[0]
    count, depth = tokens.shape
    tiles = master_qkv.shape[1] // TP // LANES
    pieces = TOKEN_PIECES
    most = max(len(c) for c in CHUNKS)
    held = max(sum(c[2] for c in way) for way in CHUNKS)
    dma = pltpu.SemaphoreType.DMA
    vmem = pl.BlockSpec(memory_space=pltpu.VMEM)
    anywhere = pl.BlockSpec(memory_space=pl.ANY)
    low, wide = jnp.bfloat16, jnp.float32
    result = pl.pallas_call(
        functools.partial(kernel, dims),
        out_shape=pltpu.VMEM((4, 2, count, tiles * LANES), low),
        in_specs=[anywhere] * 4,
        out_specs=vmem,
        scratch_shapes=[
            pltpu.VMEM((1, rows), wide),
            pltpu.VMEM((1, qkv_bias.shape[0]), wide),
            pltpu.VMEM((count, depth), low),
            pltpu.VMEM((rows, master_qkv.shape[1]), wide),
            pltpu.VMEM((2, count, depth // 2), low),
            pltpu.VMEM((2, 2, 2, count, depth // 2), low),
            pltpu.VMEM((TP, tiles, rows, LANES), low),
            pltpu.VMEM((4 * inst_count, held, rows, LANES), low),
            pltpu.VMEM((held, rows, LANES), low),
            pltpu.VMEM((held, rows, LANES), low),
            pltpu.VMEM((2, 2, held - tiles, 2 * count, LANES), low),
            pltpu.VMEM((2, 2, tiles, 2 * count, LANES), low),
            pltpu.VMEM((2, 2, tiles, 2 * count, LANES), wide),
            pltpu.VMEM((8, LANES), wide),
            pltpu.VMEM((devices, 8, LANES), wide),
            dma((8,)),
            dma((4, pieces)),
            dma((2,)),
            dma((3,)),
            dma((3, most)),
            dma((4, most)),
            dma((most,)),
            dma((most,)),
            dma((most,)),
            dma((8,)),
            dma((2, 2, most)),
            dma((1,)),
            dma((devices,)),
            dma((devices,)),
        ],
        compiler_params=pltpu.CompilerParams(
            collective_id=0, has_side_effects=True, vmem_limit_bytes=56 * 1024 * 1024
        ),
    )(tokens, norm_gain.reshape(1, rows), master_qkv, qkv_bias.reshape(1, -1))
    return result.reshape(1, shard_count * count, tiles * LANES)


def per_device(tokens, norm_gain, master_qkv, qkv_bias):
    inst_count, shard_count = lax.axis_size("inst"), lax.axis_size("shard")
    group = 32
    fits = (
        shard_count == TP
        and inst_count == 4
        and master_qkv.shape[0] % 16 == 0
        and tokens.shape[0] % (16 * TOKEN_PIECES) == 0
        and QHEADS * HEAD_DIM // TP % LANES == 0
        and KVHEADS * HEAD_DIM // TP == LANES
        and 4 * master_qkv.shape[0] % LANES == 0
        and qkv_bias.shape[0] % group == 0
    )
    if fits:
        return kernel_device((inst_count, shard_count, group), tokens, norm_gain, master_qkv, qkv_bias)
    return general_device(tokens, norm_gain, master_qkv, qkv_bias)


def solution(mesh):
    in_specs = (
        P(("inst", "shard"), None),
        P(("inst", "shard")),
        P(("inst", "shard"), None),
        P(("inst", "shard")),
    )
    out_specs = P(("inst", "shard"), None, None)
    return jax.shard_map(
        per_device, mesh=mesh, in_specs=in_specs, out_specs=out_specs, check_vma=False
    )
```

```python
import functools

import jax
import jax.numpy as jnp
from jax import lax
from jax.experimental import pallas as pl
from jax.experimental.pallas import tpu as pltpu
from jax.sharding import PartitionSpec as P

QHEADS = 40
KVHEADS = 8
HEAD_DIM = 128
TP = 8


EPSILON = 1e-06
MESH = pl.DeviceIdType.MESH
LANES = 128
TOKEN_PIECES = 2
CHUNKS = (
    (("far", 0, 1), ("far", 1, 2), ("far", 3, 2), ("far", 5, 2), ("extra", 4, 3), ("own", 0, 2), ("own", 2, 2), ("own", 4, 3)),
    (("far", 0, 2), ("far", 2, 2), ("own", 0, 2), ("own", 2, 2), ("own", 4, 3)),
)
ACROSS = ((5, 6, 7), ())
INNER = (
    ("xm", 0, 0),
    ("xf", 0, 0),
    ("xf", 1, 0),
    ("xy", 0, 0),
    ("wd", 2, 0),
    ("wp", 0, 1),
    ("ox", 2, 0),
    ("ox", 5, 0),
    ("ko", 2, 0),
    ("ox", 0, 0),
    ("xy", 1, 0),
    ("rc", 2, 0),
    ("ox", 6, 0),
    ("ko", 5, 0),
    ("wp", 0, 2),
    ("ko", 0, 0),
    ("wp", 7, 1),
    ("ko", 6, 0),
    ("wp", 1, 2),
    ("rc", 5, 0),
    ("rw", 0, 1),
    ("rc", 0, 0),
    ("ox", 4, 0),
    ("kw", 0, 1),
    ("wd", 1, 0),
    ("ko", 4, 0),
    ("rw", 4, 2),
    ("wp", 3, 1),
    ("rc", 6, 0),
    ("xm", 1, 0),
    ("rc", 0, 1),
    ("kw", 4, 2),
    ("rx", 2, 1),
    ("wp", 4, 1),
    ("rc", 4, 0),
    ("rw", 7, 1),
    ("kw", 7, 1),
    ("rd", 4, 0),
    ("rw", 3, 1),
    ("wd", 0, 0),
    ("rc", 4, 2),
    ("kw", 3, 1),
    ("rw", 4, 1),
    ("rc", 7, 1),
    ("kw", 4, 1),
    ("ry", 1, 1),
    ("rx", 2, 0),
    ("wp", 1, 1),
    ("rc", 3, 1),
    ("rw", 4, 3),
    ("ox", 7, 0),
    ("kw", 4, 3),
    ("wp", 2, 1),
    ("rc", 4, 1),
    ("rx", 3, 0),
    ("rw", 1, 2),
    ("ko", 7, 0),
    ("ry", 1, 0),
    ("rc", 4, 3),
    ("kw", 1, 2),
    ("rx", 3, 1),
    ("ry", 3, 1),
    ("pm", 0, 4),
    ("rw", 2, 1),
    ("pm", 1, 4),
    ("wp", 2, 2),
    ("rc", 7, 0),
    ("ox", 3, 0),
    ("kw", 2, 1),
    ("rc", 1, 2),
    ("ko", 3, 0),
    ("rw", 3, 2),
    ("pm", 2, 4),
    ("wd", 3, 0),
    ("rc", 2, 1),
    ("ox", 1, 0),
    ("kw", 3, 2),
    ("rd", 1, 0),
    ("wp", 4, 2),
    ("rc", 3, 0),
    ("rw", 1, 1),
    ("ko", 1, 0),
    ("rd", 3, 0),
    ("wp", 3, 2),
    ("rc", 3, 2),
    ("kw", 1, 1),
    ("rd", 2, 0),
    ("rw", 1, 3),
    ("wp", 5, 1),
    ("rc", 1, 0),
    ("kw", 1, 3),
    ("wd", 4, 0),
    ("rw", 3, 3),
    ("wp", 6, 1),
    ("rc", 1, 1),
    ("kw", 3, 3),
    ("rw", 2, 3),
    ("ry", 2, 0),
    ("rc", 1, 3),
    ("rw", 2, 2),
    ("kw", 2, 3),
    ("pw", 1, 1),
    ("bias", 0, 0),
    ("pm", 0, 1),
    ("pm", 1, 1),
    ("rc", 3, 3),
    ("kw", 2, 2),
    ("pm", 2, 1),
    ("rw", 6, 1),
    ("pm", 0, 3),
    ("pm", 1, 3),
    ("rc", 2, 3),
    ("rw", 5, 1),
    ("kw", 6, 1),
    ("pm", 2, 3),
    ("rd", 0, 0),
    ("ry", 3, 0),
    ("rc", 2, 2),
    ("kw", 5, 1),
    ("rw", 0, 2),
    ("ry", 2, 1),
    ("pm", 0, 2),
    ("pm", 1, 2),
    ("rc", 6, 1),
    ("kw", 0, 2),
    ("rw", 0, 3),
    ("pm", 2, 2),
    ("rw", 5, 2),
    ("kw", 0, 3),
    ("rc", 5, 1),
    ("kw", 5, 2),
    ("rw", 5, 3),
    ("rc", 0, 2),
    ("rc", 0, 3),
    ("kw", 5, 3),
    ("pm", 0, 0),
    ("rw", 7, 2),
    ("pm", 1, 0),
    ("pm", 2, 0),
    ("rc", 5, 2),
    ("kw", 7, 2),
    ("rc", 5, 3),
    ("pm", 3, 0),
    ("rw", 7, 3),
    ("pm", 3, 1),
    ("pm", 3, 2),
    ("kw", 7, 3),
    ("pm", 3, 3),
    ("pm", 3, 4),
    ("rw", 6, 2),
    ("rc", 7, 2),
    ("bw", 0, 0),
    ("om", 1, 5),
    ("kw", 6, 2),
    ("rw", 6, 3),
    ("fin", 0, 5),
    ("fin", 1, 5),
    ("fin", 2, 5),
    ("fin", 3, 5),
    ("rc", 7, 3),
    ("kw", 6, 3),
    ("rc", 6, 2),
    ("om", 1, 7),
    ("rc", 6, 3),
    ("fin", 0, 7),
    ("fin", 1, 7),
    ("fin", 3, 7),
    ("om", 1, 6),
    ("fin", 0, 6),
    ("fin", 1, 6),
    ("fin", 2, 6),
    ("fin", 2, 7),
    ("fin", 3, 6),
)
OUTER = (
    ("xm", 0, 0),
    ("xy", 1, 0),
    ("wp", 4, 2),
    ("wp", 0, 1),
    ("ox", 4, 0),
    ("ox", 1, 0),
    ("ko", 4, 0),
    ("ox", 2, 0),
    ("ko", 1, 0),
    ("wp", 1, 2),
    ("rc", 4, 0),
    ("ox", 3, 0),
    ("ko", 2, 0),
    ("ry", 1, 0),
    ("wp", 1, 1),
    ("wp", 2, 2),
    ("rc", 1, 0),
    ("ko", 3, 0),
    ("rw", 0, 1),
    ("wd", 4, 0),
    ("rc", 2, 0),
    ("kw", 0, 1),
    ("rw", 0, 2),
    ("xy", 0, 0),
    ("xm", 1, 0),
    ("rc", 3, 0),
    ("kw", 0, 2),
    ("rw", 1, 2),
    ("rc", 0, 1),
    ("kw", 1, 2),
    ("rd", 1, 0),
    ("rw", 1, 1),
    ("xf", 0, 0),
    ("rc", 0, 2),
    ("ox", 0, 0),
    ("kw", 1, 1),
    ("rc", 1, 2),
    ("ko", 0, 0),
    ("ry", 1, 1),
    ("xf", 1, 0),
    ("rc", 1, 1),
    ("rw", 1, 3),
    ("kw", 1, 3),
    ("rc", 0, 0),
    ("ry", 2, 1),
    ("rc", 1, 3),
    ("rd", 0, 0),
    ("pm", 0, 1),
    ("pm", 2, 1),
    ("wp", 3, 2),
    ("ry", 2, 0),
    ("wd", 1, 0),
    ("rw", 0, 3),
    ("kw", 0, 3),
    ("wd", 3, 0),
    ("ry", 3, 0),
    ("wd", 2, 0),
    ("rc", 0, 3),
    ("pm", 0, 0),
    ("pm", 2, 0),
    ("ry", 3, 1),
    ("pm", 1, 0),
    ("pm", 1, 1),
    ("rw", 2, 2),
    ("kw", 2, 2),
    ("rd", 3, 0),
    ("wp", 3, 1),
    ("rc", 2, 2),
    ("pm", 3, 0),
    ("wp", 2, 1),
    ("pm", 3, 1),
    ("rw", 4, 2),
    ("kw", 4, 2),
    ("we", 5, 0),
    ("rw", 3, 2),
    ("wd", 0, 0),
    ("rw", 3, 1),
    ("kw", 3, 2),
    ("wp", 0, 2),
    ("rc", 4, 2),
    ("rd", 4, 0),
    ("rw", 2, 1),
    ("kw", 3, 1),
    ("we", 7, 0),
    ("wp", 5, 2),
    ("rc", 3, 2),
    ("re", 5, 0),
    ("rw", 3, 3),
    ("kw", 2, 1),
    ("rd", 2, 0),
    ("wp", 7, 2),
    ("rc", 3, 1),
    ("kw", 3, 3),
    ("rw", 4, 3),
    ("pw", 1, 1),
    ("bias", 0, 0),
    ("rc", 2, 1),
    ("kw", 4, 3),
    ("we", 6, 0),
    ("rc", 3, 3),
    ("re", 7, 0),
    ("wp", 4, 1),
    ("wp", 6, 2),
    ("rw", 2, 3),
    ("kw", 2, 3),
    ("om", 1, 3),
    ("rc", 4, 3),
    ("re", 6, 0),
    ("rc", 2, 3),
    ("rw", 4, 1),
    ("kw", 4, 1),
    ("om", 1, 2),
    ("bw", 0, 0),
    ("fin", 1, 3),
    ("fin", 0, 3),
    ("fin", 3, 3),
    ("fin", 0, 2),
    ("fin", 1, 2),
    ("fin", 3, 2),
    ("rc", 4, 1),
    ("om", 1, 4),
    ("fin", 0, 4),
    ("fin", 1, 4),
    ("fin", 2, 2),
    ("fin", 2, 3),
    ("fin", 2, 4),
    ("fin", 3, 4),
)


def partner_2(value, axis, distance):
    mask = 2**distance
    pairs = [(source, source ^ mask) for source in range(lax.axis_size(axis))]
    return lax.ppermute(value, axis, pairs)


def rank_columns(matrix):
    query_cols = QHEADS * HEAD_DIM
    pair_cols = KVHEADS * HEAD_DIM
    leading = matrix.shape[:-1]
    query = matrix[..., :query_cols].reshape(leading + (TP, query_cols // TP))
    keys = matrix[..., query_cols : query_cols + pair_cols].reshape(leading + (TP, pair_cols // TP))
    values = matrix[..., query_cols + pair_cols :].reshape(leading + (TP, pair_cols // TP))
    return jnp.concatenate([query, keys, values], axis=-1)


def normalize(tokens, gain):
    floats = tokens.astype(jnp.float32)
    scale = lax.rsqrt(jnp.mean(floats * floats, axis=-1, keepdims=True) + EPSILON)
    return (floats * scale * gain.astype(jnp.float32)).astype(jnp.bfloat16)


def general_device(tokens, norm_gain, master_qkv, qkv_bias):
    shard_count = lax.axis_size("shard")
    local_rows = master_qkv.shape[0]
    rank_width = master_qkv.shape[1] // TP
    gain_full, bias_full = (
        lax.all_gather(norm_gain.astype(jnp.bfloat16), ("inst", "shard"), axis=0, tiled=True),
        lax.all_gather(qkv_bias.astype(jnp.bfloat16), ("inst", "shard"), axis=0, tiled=True),
    )
    normed = normalize(tokens, gain_full)
    shard_pos = lax.axis_index("shard")
    rank_index = shard_pos % TP
    bit_count = TP.bit_length() - 1
    bit_order = list(range(bit_count))
    group_rows = normed
    for bit_pos in bit_order:
        partner = partner_2(group_rows, "shard", bit_pos)
        lower = jnp.bitwise_and(jnp.right_shift(shard_pos, bit_pos), 1) == 0
        group_rows = jnp.where(
            lower,
            jnp.concatenate([group_rows, partner], 0),
            jnp.concatenate([partner, group_rows], 0),
        )
    copies = shard_count // TP
    inst_block = shard_count * local_rows
    rows_low = master_qkv.astype(jnp.bfloat16)
    ranked = jnp.transpose(rank_columns(rows_low), (1, 0, 2))
    spread = jnp.broadcast_to(ranked[None], (copies,) + ranked.shape)
    outgoing = spread.reshape(shard_count, rows_low.shape[0], rank_width)
    arrived = lax.all_to_all(outgoing, "shard", split_axis=0, concat_axis=0, tiled=True).reshape(
        inst_block, rank_width
    )
    product = jnp.dot(
        group_rows,
        lax.all_gather(arrived, "inst", axis=0, tiled=True),
        preferred_element_type=jnp.float32,
    )
    bias_ranks = rank_columns(bias_full)
    bias_mine = lax.dynamic_index_in_dim(bias_ranks, rank_index, 0, keepdims=False)
    result = (product + bias_mine.astype(jnp.float32)).astype(jnp.bfloat16)
    return result[None]


def incoming(kind):
    chunks = [c for c in CHUNKS[1 - kind] if c[0] == "far"]
    return [c[1:] for c in chunks + [c for c in CHUNKS[kind] if c[0] == "extra"]]


def chunk_of(kind, j):
    what, first, count = CHUNKS[kind][j]
    return what, first, count, sum(c[2] for c in CHUNKS[kind][:j])


def kernel(
    dims,
    tok_hbm,
    gain_hbm,
    w_hbm,
    bias_hbm,
    out_ref,
    gain_ref,
    bias_ref,
    tok_ref,
    w_ref,
    xsend,
    xbuf,
    wsend,
    wbuf,
    dbuf,
    ebuf,
    psend,
    pbuf,
    acc,
    bias_own,
    bbuf,
    load_sem,
    x_recv,
    x1_recv,
    x_send,
    w_recv,
    wx_recv,
    wc_recv,
    d_recv,
    e_recv,
    w_send,
    p_recv,
    p_send,
    b_recv,
    b_send,
):
    inst_count, shard_count, group = dims
    devices = inst_count * shard_count
    inst = lax.axis_index("inst")
    me = lax.axis_index("shard")
    z = me // 2
    y = lax.rem(me, 2)
    half = z // 2
    flat = inst * shard_count + me
    core_peer = inst + 1 - 2 * lax.rem(inst, 2)
    x_peer = lax.rem(inst + 2, inst_count)
    z_mate = z + 1 - 2 * lax.rem(z, 2)
    z_pair = lax.rem(z + 2, 4)
    z_near = 2 - half
    z_end = 3 - 3 * half
    inner = z_near + z == 3
    rows = w_ref.shape[0]
    tokens, depth = tok_ref.shape
    tiles = wsend.shape[1]
    half_block = 4 * rows
    pieces = TOKEN_PIECES
    piece_rows = tokens // pieces

    halves = 2
    step_rows = tokens // halves
    row_cut = rows // 2

    def token_load(q):
        part = pl.ds(q * step_rows, step_rows)
        return pltpu.make_async_copy(tok_hbm.at[part], tok_ref.at[part], load_sem.at[q])

    def weight_load(q):
        part = pl.ds(q * row_cut, row_cut)
        return pltpu.make_async_copy(w_hbm.at[part], w_ref.at[part], load_sem.at[2 + q])

    for q in range(halves):
        token_load(q).start()

    barrier = pltpu.get_barrier_semaphore()

    def greet(owner, there):
        pl.semaphore_signal(barrier, inc=1, device_id=(owner, there), device_id_type=MESH)

    greet(inst, z_pair * 2 + y)
    greet(inst, z_mate * 2 + y)
    greet(inst, z * 2 + 1 - y)
    greet(x_peer, me)
    greet(core_peer, me)
    pl.when(inner)(lambda: greet(inst, z_near * 2 + y))
    for q in range(2):
        weight_load(q).start()
    small_load = (
        pltpu.make_async_copy(gain_hbm, gain_ref, load_sem.at[4]),
        pltpu.make_async_copy(bias_hbm, bias_ref, load_sem.at[5]),
    )
    for copy in small_load:
        copy.start()

    def remote(source, target, send_sem, recv_sem, device):
        return pltpu.make_async_remote_copy(
            src_ref=source,
            dst_ref=target,
            send_sem=send_sem,
            recv_sem=recv_sem,
            device_id=device,
            device_id_type=MESH,
        )

    def each(condition, action):
        pl.when(condition)(action)

    def piece_of(ref, piece):
        return ref.at[pl.ds(piece * piece_rows, piece_rows)]

    def own_x(which, device, side, piece):
        return remote(
            piece_of(xsend.at[which], piece),
            piece_of(xbuf.at[side, half, lax.rem(z, 2)], piece),
            x_send.at[0],
            x1_recv.at[half] if side else x_recv.at[z, piece],
            (inst, device),
        )

    def relay_x(way, block, piece):
        device, side = ((z_mate * 2 + y, 0), (z * 2 + 1 - y, 1))[way]
        return remote(
            piece_of(xbuf.at[0, block // 2, lax.rem(block, 2)], piece),
            piece_of(xbuf.at[side, block // 2, lax.rem(block, 2)], piece),
            x_send.at[1 + way],
            x1_recv.at[block // 2] if side else x_recv.at[block, piece],
            (inst, device),
        )

    def slot_of(owner, k):
        return owner * 4 + lax.rem(z_mate if k // 2 else z, 2) * 2 + (1 - y if k % 2 else y)

    def fresh(kind, there, j, side):
        what, first, count, _ = chunk_of(kind, j)
        rank = {"far": lax.rem(there + 2, 4), "extra": z_near, "own": there}[what] * 2 + side
        return wsend.at[rank, pl.ds(first, count)]

    def held(kind, slot, j):
        _, _, count, at = chunk_of(kind, j)
        return wbuf.at[slot, pl.ds(at, count)]

    def arrived(ref, sem):
        pltpu.make_async_copy(ref, ref, sem).wait()

    query = QHEADS * HEAD_DIM // TP
    pair = KVHEADS * HEAD_DIM // TP
    held_bias = bias_ref.shape[1]
    per_row = LANES // group
    groups = held_bias // group

    def needs(owner, rank):
        low, high = owner * held_bias, owner * held_bias + held_bias
        result = None
        for start, extent in (
            (rank * query, query),
            (TP * query + rank * pair, pair),
            (TP * (query + pair) + rank * pair, pair),
        ):
            overlap = jnp.logical_and(start < high, low < start + extent)
            result = overlap if result is None else jnp.logical_or(result, overlap)
        return result

    def bias_slot(owner, rank):
        first = rank * query // held_bias
        pairs = [(TP * query + (rank + TP * n) * pair) // held_bias for n in range(2)]
        late = jnp.where(owner - pairs[1] >= 0, 6 + owner - pairs[1], 4 + owner - pairs[0])
        return jnp.where(jnp.logical_and(owner - first >= 0, owner - first < 4), owner - first, late)

    def bias_copy(step):
        there = lax.rem(flat + step, devices)
        owner, rank = there // shard_count, lax.rem(there, shard_count)
        return remote(
            bias_own,
            bbuf.at[flat],
            b_send.at[owner * 3 + lax.rem(rank, 3)],
            b_recv.at[bias_slot(flat, rank)],
            (owner, rank),
        )

    def send_bias(finish):
        @pl.loop(1, devices)
        def _(step):
            there = lax.rem(flat + step, devices)

            @pl.when(needs(flat, lax.rem(there, shard_count)))
            def _():
                if finish:
                    bias_copy(step).wait_send()
                else:
                    bias_copy(step).start()

    def bias_row(number_first):
        lane = lax.broadcasted_iota(jnp.int32, (1, LANES), 1) // group
        row = jnp.zeros((1, LANES), jnp.float32)
        for q in range(per_row):
            number = number_first + q
            row = jnp.where(lane == q, bbuf[number // groups, pl.ds(lax.rem(number, groups), 1), :], row)
        return row

    def column_of(t):
        at = t * LANES
        if at < query:
            return me * query + at
        if at < query + pair:
            return TP * query + me * pair + (at - query)
        return TP * (query + pair) + me * pair + (at - query - pair)

    narrow = 16
    for first in range(0, tokens, narrow):
        if first % step_rows == 0:
            token_load(first // step_rows).wait()
        values = tok_ref[first : first + narrow, :].astype(jnp.float32)
        mean = jnp.sum(values * values, axis=-1, keepdims=True) * (1.0 / depth)
        scaled = (values * lax.rsqrt(mean + EPSILON)).astype(jnp.bfloat16)
        for which in range(2):
            for owner in range(inst_count):
                at = (owner * 2 + which) * half_block
                xsend[which, first : first + narrow, owner * half_block : (owner + 1) * half_block] = scaled[
                    :, at : at + half_block
                ]
    pl.semaphore_wait(barrier, jnp.where(inner, 6, 5))

    def send_x(name, piece):
        which, device, side = {
            "xf": (1 - half, z_near * 2 + y, 0),
            "xm": (half, z_mate * 2 + y, 0),
            "xy": (half, z * 2 + 1 - y, 1),
        }[name]
        own_x(which, device, side, piece).start()

    def early(steps):
        for name, piece, _ in steps:
            if name not in ("xf", "xm", "xy"):
                break
            send_x(name, piece)

    each(inner, lambda: early(INNER))
    each(jnp.logical_not(inner), lambda: early(OUTER))
    xbuf[0, half, lax.rem(z, 2)] = xsend[half]

    small_load[0].wait()
    ids = lax.broadcasted_iota(jnp.int32, (rows, rows), 0), lax.broadcasted_iota(jnp.int32, (rows, rows), 1)
    gain_row = gain_ref[...].astype(jnp.bfloat16).astype(jnp.float32)
    gain = jnp.sum(jnp.where(ids[0] == ids[1], jnp.broadcast_to(gain_row, (rows, rows)), 0.0), axis=1, keepdims=True)
    for q in range(2):
        weight_load(q).wait()
    for rank in range(TP):
        starts = (
            (rank * query, 0, query),
            (TP * query + rank * pair, query, pair),
            (TP * (query + pair) + rank * pair, query + pair, pair),
        )
        for source, target, extent in starts:
            for inside in range(0, extent, LANES):
                part = w_ref[:, source + inside : source + inside + LANES].astype(jnp.bfloat16).astype(jnp.float32)
                wsend[rank, (target + inside) // LANES] = (part * gain).astype(jnp.bfloat16)

    def product(kind, lhs, j):
        _, first, count, at = chunk_of(kind, j)
        result = []
        for t in range(0, count, 2):
            width = min(2, count - t)
            rhs = [wbuf[:, at + t + u].reshape(4 * half_block, LANES) for u in range(width)]
            rhs = jnp.concatenate(rhs, axis=1) if width > 1 else rhs[0]
            value = jnp.dot(lhs, rhs, preferred_element_type=jnp.float32)
            for u in range(width):
                result.append((t + u, value[:, u * LANES : (u + 1) * LANES]))
        return result

    def finish_bias():
        @pl.loop(1, devices)
        def _(step):
            slot = lax.rem(flat + step, devices)

            @pl.when(needs(slot, me))
            def _():
                arrived(bbuf.at[slot], b_recv.at[bias_slot(slot, me)])

        bbuf[flat] = bias_own[...]
        send_bias(True)

    def run(kind, steps):
        other = 1 - kind
        done = set()

        def once(key, action):
            if key not in done:
                done.add(key)
                action()

        def need_x(block):
            for piece in range(pieces):
                once(
                    ("x", block, piece),
                    lambda piece=piece: arrived(
                        mine(block, piece), x_recv.at[places[block], piece]
                    ),
                )

        def need_w(k, j):
            once(("w", k, j), lambda: arrived(held(kind, slot_of(inst, k), j), w_recv.at[k - 1, j]))

        def need_chunk(j):
            _, first, count, at = chunk_of(kind, j)

            def action():
                arrived(wbuf.at[pl.ds(0, 8), pl.ds(at, count)], wc_recv.at[j])
                wbuf[slot_of(inst, 0), at : at + count] = fresh(kind, z, j, y)[...]

            once(("c", j), action)

        def mine(block, piece):
            return piece_of(xbuf.at[0, places[block] // 2, lax.rem(places[block], 2)], piece)

        def need_tokens(unit):
            if unit < 2:
                for block in ((1,), (2, 3))[unit]:
                    need_x(block)
            else:
                part = half if unit == 2 else 1 - half
                once(("y", unit), lambda: arrived(xbuf.at[1, part], x1_recv.at[part]))

        places = (z, z_mate, z_near, z_end)

        def step_rx(block, piece):
            once(
                ("x", block, piece),
                lambda: arrived(mine(block, piece), x_recv.at[places[block], piece]),
            )
            relay_x(0, places[block], piece).start()

        def step_ry(block, piece):
            once(
                ("x", block, piece),
                lambda: arrived(mine(block, piece), x_recv.at[places[block], piece]),
            )
            relay_x(1, places[block], piece).start()

        def step_wp(j, k):
            mine = slot_of(inst, 0)
            if k == 1:
                source, target, device = fresh(kind, z, j, 1 - y), held(kind, mine, j), z * 2 + 1 - y
            else:
                source, target, device = fresh(other, z_mate, j, y), held(other, mine, j), z_mate * 2 + y
            remote(source, target, w_send.at[k - 1], w_recv.at[k - 1, j], (inst, device)).start()

        def step_wd(j, _):
            _, _, count, at = chunk_of(other, j)
            target = dbuf.at[pl.ds(at, count)]
            remote(
                fresh(other, z_mate, j, 1 - y), target, w_send.at[2], d_recv.at[j], (inst, z_mate * 2 + y)
            ).start()

        def step_we(j, _):
            _, _, count, at = chunk_of(other, j)
            remote(
                fresh(other, z_mate, j, 1 - y), ebuf.at[pl.ds(at, count)], w_send.at[6], e_recv.at[j], (inst, z * 2 + 1 - y)
            ).start()

        def step_re(j, _):
            _, _, count, at = chunk_of(other, j)
            source = ebuf.at[pl.ds(at, count)]
            arrived(source, e_recv.at[j])
            target = held(other, slot_of(inst, 1), j)
            remote(source, target, w_send.at[7], w_recv.at[2, j], (inst, z_mate * 2 + y)).start()

        def step_rd(j, _):
            _, _, count, at = chunk_of(kind, j)
            source = dbuf.at[pl.ds(at, count)]
            arrived(source, d_recv.at[j])
            target = held(kind, slot_of(inst, 2), j)
            remote(source, target, w_send.at[3], w_recv.at[2, j], (inst, z * 2 + 1 - y)).start()

        def send_block(j, k, source, across):
            device, send, recv = (
                ((x_peer, me), w_send.at[4], wx_recv.at[k, j]),
                ((core_peer, me), w_send.at[5], wc_recv.at[j]),
            )[across]
            remote(source, held(kind, slot_of(inst, k), j), send, recv, device).start()

        def step_ox(j, _):
            send_block(j, 0, fresh(kind, z, j, y), 0)

        def step_ko(j, _):
            send_block(j, 0, fresh(kind, z, j, y), 1)

        def step_rw(j, k):
            need_w(k, j)
            send_block(j, k, held(kind, slot_of(inst, k), j), 0)

        def step_kw(j, k):
            need_w(k, j)
            send_block(j, k, held(kind, slot_of(inst, k), j), 1)

        def step_rc(j, k):
            block = held(kind, slot_of(x_peer, k), j)
            arrived(block, wx_recv.at[k, j])
            remote(block, block, w_send.at[5], wc_recv.at[j], (core_peer, me)).start()

        def step_pm(unit, j):
            need_tokens(unit)
            need_chunk(j)
            what, first, count, at = chunk_of(kind, j)
            side, part = unit // 2, (1 - half if unit % 2 else half)
            lhs = xbuf[side, part].reshape(2 * tokens, 4 * half_block)
            for t, value in product(kind, lhs, j):
                psend[side, part, at + t] = value.astype(jnp.bfloat16)
            target = other if what == "far" else kind
            index = incoming(target).index((first, count))
            remote(
                psend.at[side, part, pl.ds(at, count)],
                pbuf.at[side, part, pl.ds(first, count)],
                p_send.at[0],
                p_recv.at[side, part, index],
                (inst, (z_pair if what == "far" else z_near) * 2 + y),
            ).start()

        def step_om(_, j):
            for unit in range(4):
                need_tokens(unit)
            need_chunk(j)
            first = chunk_of(kind, j)[1]
            lhs = xbuf[...].reshape(8 * tokens, 4 * half_block)
            for t, value in product(kind, lhs, j):
                for unit in range(4):
                    acc[unit // 2, unit % 2, first + t] = value[unit * 2 * tokens : (unit + 1) * 2 * tokens]

        def step_pw(unit, index):
            side, part = unit // 2, (1 - half if unit % 2 else half)
            low, extent = incoming(kind)[index]
            once(
                ("p", unit, index),
                lambda: arrived(pbuf.at[side, part, pl.ds(low, extent)], p_recv.at[side, part, index]),
            )

        def step_fin(unit, j):
            _, first, count, _ = chunk_of(kind, j)
            side, part = unit // 2, (1 - half if unit % 2 else half)
            for index, (low, extent) in enumerate(incoming(kind)):
                if low < first + count and first < low + extent:
                    step_pw(unit, index)
            where = 1 - y if side else y
            for t in range(first, first + count):
                value = acc[side, part, t] + pbuf[side, part, t].astype(jnp.float32) + bias_row(column_of(t) // group)
                value = value.astype(jnp.bfloat16)
                for k in range(2):
                    out_ref[part * 2 + k, where, :, t * LANES : (t + 1) * LANES] = value[k * tokens : (k + 1) * tokens]

        def step_bias(*_):
            small_load[1].wait()
            group_id = lax.broadcasted_iota(jnp.int32, (8, held_bias), 0)
            lane_id = lax.broadcasted_iota(jnp.int32, (8, held_bias), 1)
            spread = jnp.where(lane_id // group == group_id, jnp.broadcast_to(bias_ref[...], (8, held_bias)), 0.0)
            from_id = lax.broadcasted_iota(jnp.int32, (held_bias, LANES), 0)
            to_id = lax.broadcasted_iota(jnp.int32, (held_bias, LANES), 1)
            pick = jnp.where(lax.rem(from_id, group) == lax.rem(to_id, group), 1.0, 0.0).astype(jnp.bfloat16)
            bias_own[...] = jnp.dot(spread.astype(jnp.bfloat16), pick, preferred_element_type=jnp.float32)
            send_bias(False)

        table = dict(
            xy=lambda piece, _: send_x("xy", piece),
            xf=lambda piece, _: send_x("xf", piece),
            xm=lambda piece, _: send_x("xm", piece),
            rx=step_rx,
            ry=step_ry,
            wp=step_wp,
            wd=step_wd,
            rd=step_rd,
            we=step_we,
            re=step_re,
            ox=step_ox,
            ko=step_ko,
            rw=step_rw,
            kw=step_kw,
            rc=step_rc,
            pm=step_pm,
            om=step_om,
            fin=step_fin,
            bias=step_bias,
            bw=lambda *_: finish_bias(),
            pw=step_pw,
        )
        start = next(i for i, step in enumerate(steps) if step[0] not in ("xf", "xm", "xy"))
        for name, first, second in steps[start:]:
            table[name](first, second)

        counts = [sum(c[2] for c in CHUNKS[way]) for way in range(2)]
        sent = counts[kind] - tiles
        three = xbuf.at[0, :, :, pl.ds(0, 3 * tokens // 4)]
        arrived(three, x_send.at[0])
        arrived(three, x_send.at[2])
        if kind == 0:
            arrived(xbuf.at[0, 0], x_send.at[1])
        across = [sum(c[2] for j, c in enumerate(CHUNKS[way]) if j in ACROSS[way]) for way in range(2)]
        for way, extent in (
            (0, counts[kind]),
            (1, counts[other]),
            (2, counts[other] - across[other]),
            (3, counts[kind] - across[kind]),
            (6, across[other]),
            (7, across[other]),
        ):
            if extent:
                arrived(wbuf.at[0, pl.ds(0, extent)], w_send.at[way])
        arrived(wbuf.at[pl.ds(0, 4), pl.ds(0, counts[kind])], w_send.at[4])
        arrived(wbuf.at[pl.ds(0, 8), pl.ds(0, counts[kind])], w_send.at[5])
        arrived(psend.at[:, :, pl.ds(0, sent)], p_send.at[0])

    each(inner, lambda: run(0, INNER))
    each(jnp.logical_not(inner), lambda: run(1, OUTER))


def kernel_device(dims, tokens, norm_gain, master_qkv, qkv_bias):
    inst_count, shard_count, group = dims
    devices = inst_count * shard_count
    rows = master_qkv.shape[0]
    count, depth = tokens.shape
    tiles = master_qkv.shape[1] // TP // LANES
    pieces = TOKEN_PIECES
    most = max(len(c) for c in CHUNKS)
    held = max(sum(c[2] for c in way) for way in CHUNKS)
    dma = pltpu.SemaphoreType.DMA
    vmem = pl.BlockSpec(memory_space=pltpu.VMEM)
    anywhere = pl.BlockSpec(memory_space=pl.ANY)
    low, wide = jnp.bfloat16, jnp.float32
    result = pl.pallas_call(
        functools.partial(kernel, dims),
        out_shape=pltpu.VMEM((4, 2, count, tiles * LANES), low),
        in_specs=[anywhere] * 4,
        out_specs=vmem,
        scratch_shapes=[
            pltpu.VMEM((1, rows), wide),
            pltpu.VMEM((1, qkv_bias.shape[0]), wide),
            pltpu.VMEM((count, depth), low),
            pltpu.VMEM((rows, master_qkv.shape[1]), wide),
            pltpu.VMEM((2, count, depth // 2), low),
            pltpu.VMEM((2, 2, 2, count, depth // 2), low),
            pltpu.VMEM((TP, tiles, rows, LANES), low),
            pltpu.VMEM((4 * inst_count, held, rows, LANES), low),
            pltpu.VMEM((held, rows, LANES), low),
            pltpu.VMEM((held, rows, LANES), low),
            pltpu.VMEM((2, 2, held - tiles, 2 * count, LANES), low),
            pltpu.VMEM((2, 2, tiles, 2 * count, LANES), low),
            pltpu.VMEM((2, 2, tiles, 2 * count, LANES), wide),
            pltpu.VMEM((8, LANES), wide),
            pltpu.VMEM((devices, 8, LANES), wide),
            dma((6,)),
            dma((4, pieces)),
            dma((2,)),
            dma((3,)),
            dma((3, most)),
            dma((4, most)),
            dma((most,)),
            dma((most,)),
            dma((most,)),
            dma((8,)),
            dma((2, 2, max(len(incoming(way)) for way in range(2)))),
            dma((1,)),
            dma((8,)),
            dma((3 * inst_count,)),
        ],
        compiler_params=pltpu.CompilerParams(
            collective_id=0, has_side_effects=True, vmem_limit_bytes=56 * 1024 * 1024
        ),
    )(tokens, norm_gain.reshape(1, rows), master_qkv, qkv_bias.reshape(1, -1))
    return result.reshape(1, shard_count * count, tiles * LANES)


def per_device(tokens, norm_gain, master_qkv, qkv_bias):
    inst_count, shard_count = lax.axis_size("inst"), lax.axis_size("shard")
    group = 32
    fits = (
        shard_count == TP
        and inst_count == 4
        and master_qkv.shape[0] % 16 == 0
        and tokens.shape[0] % (16 * TOKEN_PIECES) == 0
        and QHEADS * HEAD_DIM // TP % LANES == 0
        and KVHEADS * HEAD_DIM // TP == LANES
        and 4 * master_qkv.shape[0] % LANES == 0
        and qkv_bias.shape[0] % group == 0
    )
    if fits:
        return kernel_device((inst_count, shard_count, group), tokens, norm_gain, master_qkv, qkv_bias)
    return general_device(tokens, norm_gain, master_qkv, qkv_bias)


def solution(mesh):
    in_specs = (
        P(("inst", "shard"), None),
        P(("inst", "shard")),
        P(("inst", "shard"), None),
        P(("inst", "shard")),
    )
    out_specs = P(("inst", "shard"), None, None)
    return jax.shard_map(
        per_device, mesh=mesh, in_specs=in_specs, out_specs=out_specs, check_vma=False
    )
```

```python
import functools

import jax
import jax.numpy as jnp
from jax import lax
from jax.experimental import pallas as pl
from jax.experimental.pallas import tpu as pltpu
from jax.sharding import PartitionSpec as P

QHEADS = 40
KVHEADS = 8
HEAD_DIM = 128
TP = 8


EPSILON = 1e-06
MESH = pl.DeviceIdType.MESH
LANES = 128
TOKEN_PIECES = 2
CHUNKS = (
    (("far", 0, 1), ("far", 1, 2), ("far", 3, 2), ("far", 5, 2), ("extra", 4, 3), ("own", 0, 2), ("own", 2, 2), ("own", 4, 3)),
    (("far", 0, 2), ("far", 2, 2), ("own", 0, 2), ("own", 2, 2), ("own", 4, 3)),
)
ACROSS = ((5, 6, 7), ())
INNER = (
    ("xm", 0, 0),
    ("xf", 1, 0),
    ("xf", 0, 0),
    ("xy", 1, 0),
    ("wp", 0, 2),
    ("wp", 3, 1),
    ("ox", 7, 0),
    ("ox", 0, 0),
    ("ko", 7, 0),
    ("ox", 3, 0),
    ("ko", 0, 0),
    ("wd", 0, 0),
    ("ox", 1, 0),
    ("ko", 3, 0),
    ("rc", 7, 0),
    ("ry", 2, 1),
    ("xm", 1, 0),
    ("ry", 1, 0),
    ("rc", 0, 0),
    ("ox", 4, 0),
    ("ko", 1, 0),
    ("rc", 3, 0),
    ("ko", 4, 0),
    ("rw", 4, 2),
    ("rx", 2, 0),
    ("rc", 1, 0),
    ("rw", 3, 1),
    ("kw", 4, 2),
    ("rd", 4, 0),
    ("wp", 3, 2),
    ("rc", 4, 0),
    ("wp", 4, 1),
    ("kw", 3, 1),
    ("rw", 2, 2),
    ("wd", 1, 0),
    ("rc", 4, 2),
    ("ox", 5, 0),
    ("kw", 2, 2),
    ("rx", 2, 1),
    ("rc", 3, 1),
    ("ko", 5, 0),
    ("rw", 4, 3),
    ("ry", 1, 1),
    ("wp", 1, 2),
    ("wp", 5, 1),
    ("rc", 2, 2),
    ("kw", 4, 3),
    ("rw", 4, 1),
    ("rc", 5, 0),
    ("rw", 1, 2),
    ("kw", 4, 1),
    ("xy", 0, 0),
    ("rx", 3, 0),
    ("rc", 4, 3),
    ("wp", 6, 1),
    ("kw", 1, 2),
    ("rw", 5, 1),
    ("rc", 4, 1),
    ("ox", 2, 0),
    ("kw", 5, 1),
    ("rx", 3, 1),
    ("wp", 4, 2),
    ("wp", 2, 1),
    ("pm", 0, 4),
    ("rc", 1, 2),
    ("ox", 6, 0),
    ("ko", 2, 0),
    ("pm", 1, 4),
    ("pm", 2, 4),
    ("rc", 5, 1),
    ("ko", 6, 0),
    ("rd", 3, 0),
    ("rw", 6, 1),
    ("wd", 3, 0),
    ("rd", 0, 0),
    ("rc", 2, 0),
    ("kw", 6, 1),
    ("kw", 2, 1),
    ("rw", 2, 1),
    ("rd", 2, 0),
    ("rc", 6, 0),
    ("wp", 2, 2),
    ("wp", 0, 1),
    ("rw", 3, 3),
    ("rc", 6, 1),
    ("rw", 0, 2),
    ("kw", 3, 3),
    ("wd", 2, 0),
    ("rd", 1, 0),
    ("wp", 1, 1),
    ("rc", 2, 1),
    ("kw", 0, 2),
    ("rw", 2, 3),
    ("wd", 4, 0),
    ("rw", 0, 1),
    ("wp", 7, 1),
    ("rc", 3, 3),
    ("rc", 0, 2),
    ("kw", 2, 3),
    ("rw", 0, 3),
    ("kw", 0, 1),
    ("ry", 2, 0),
    ("rw", 1, 3),
    ("kw", 0, 3),
    ("pw", 1, 0),
    ("bias", 0, 0),
    ("rc", 2, 3),
    ("kw", 1, 3),
    ("rw", 1, 1),
    ("rc", 0, 1),
    ("ry", 3, 0),
    ("pm", 0, 2),
    ("pm", 1, 2),
    ("rc", 0, 3),
    ("kw", 1, 1),
    ("pm", 2, 2),
    ("rw", 7, 1),
    ("pm", 0, 0),
    ("pm", 1, 0),
    ("rc", 1, 3),
    ("pm", 2, 0),
    ("kw", 7, 1),
    ("ry", 3, 1),
    ("rc", 1, 1),
    ("rw", 3, 2),
    ("kw", 3, 2),
    ("pm", 0, 1),
    ("pm", 1, 1),
    ("pm", 2, 1),
    ("rc", 7, 1),
    ("rw", 7, 2),
    ("kw", 7, 2),
    ("rc", 3, 2),
    ("rw", 7, 3),
    ("kw", 7, 3),
    ("pm", 0, 3),
    ("pm", 1, 3),
    ("pm", 2, 3),
    ("rc", 7, 2),
    ("rw", 6, 3),
    ("kw", 6, 3),
    ("pm", 3, 0),
    ("pm", 3, 1),
    ("pm", 3, 2),
    ("rw", 6, 2),
    ("pm", 3, 3),
    ("rc", 7, 3),
    ("kw", 6, 2),
    ("pm", 3, 4),
    ("rw", 5, 2),
    ("bw", 0, 0),
    ("om", 1, 7),
    ("rc", 6, 3),
    ("kw", 5, 2),
    ("fin", 0, 7),
    ("rw", 5, 3),
    ("rc", 6, 2),
    ("kw", 5, 3),
    ("fin", 3, 7),
    ("fin", 1, 7),
    ("om", 1, 6),
    ("rc", 5, 2),
    ("fin", 0, 6),
    ("fin", 1, 6),
    ("fin", 2, 6),
    ("fin", 3, 6),
    ("rc", 5, 3),
    ("om", 1, 5),
    ("fin", 0, 5),
    ("fin", 1, 5),
    ("fin", 2, 5),
    ("fin", 3, 5),
    ("fin", 2, 7),
)
OUTER = (
    ("xm", 0, 0),
    ("xy", 0, 0),
    ("wp", 4, 2),
    ("wp", 3, 1),
    ("ox", 3, 0),
    ("ox", 1, 0),
    ("ko", 3, 0),
    ("ox", 0, 0),
    ("ko", 1, 0),
    ("wd", 4, 0),
    ("wp", 0, 1),
    ("rc", 3, 0),
    ("ox", 4, 0),
    ("ko", 0, 0),
    ("xy", 1, 0),
    ("rc", 1, 0),
    ("ko", 4, 0),
    ("wp", 1, 2),
    ("rw", 0, 2),
    ("rc", 0, 0),
    ("rw", 3, 1),
    ("kw", 0, 2),
    ("rd", 0, 0),
    ("wp", 2, 2),
    ("rc", 4, 0),
    ("ox", 2, 0),
    ("kw", 3, 1),
    ("xm", 1, 0),
    ("rc", 0, 2),
    ("rw", 0, 1),
    ("ko", 2, 0),
    ("ry", 1, 1),
    ("xf", 0, 0),
    ("ry", 1, 0),
    ("rc", 3, 1),
    ("kw", 0, 1),
    ("rw", 0, 3),
    ("rc", 2, 0),
    ("kw", 0, 3),
    ("xf", 1, 0),
    ("wp", 1, 1),
    ("rw", 3, 2),
    ("rc", 0, 1),
    ("kw", 3, 2),
    ("rc", 0, 3),
    ("rd", 1, 0),
    ("pm", 0, 0),
    ("rc", 3, 2),
    ("pm", 2, 0),
    ("ry", 2, 1),
    ("rw", 1, 1),
    ("kw", 1, 1),
    ("ry", 2, 0),
    ("wd", 3, 0),
    ("rw", 1, 3),
    ("rw", 1, 2),
    ("kw", 1, 3),
    ("wd", 0, 0),
    ("rc", 1, 1),
    ("kw", 1, 2),
    ("wd", 2, 0),
    ("rc", 1, 3),
    ("ry", 3, 0),
    ("wp", 0, 2),
    ("rc", 1, 2),
    ("wd", 1, 0),
    ("pm", 0, 1),
    ("pm", 2, 1),
    ("ry", 3, 1),
    ("pm", 1, 0),
    ("pm", 1, 1),
    ("rw", 4, 2),
    ("kw", 4, 2),
    ("rd", 3, 0),
    ("wp", 2, 1),
    ("rw", 2, 2),
    ("kw", 2, 2),
    ("rc", 4, 2),
    ("pm", 3, 0),
    ("we", 7, 0),
    ("pm", 3, 1),
    ("rw", 3, 3),
    ("kw", 3, 3),
    ("wp", 3, 2),
    ("rc", 2, 2),
    ("rd", 4, 0),
    ("rw", 2, 1),
    ("kw", 2, 1),
    ("wp", 7, 2),
    ("we", 6, 0),
    ("rc", 3, 3),
    ("re", 7, 0),
    ("om", 1, 3),
    ("rc", 2, 1),
    ("rd", 2, 0),
    ("pw", 1, 2),
    ("bias", 0, 0),
    ("rw", 4, 3),
    ("kw", 4, 3),
    ("wp", 4, 1),
    ("re", 6, 0),
    ("wp", 6, 2),
    ("we", 5, 0),
    ("rw", 2, 3),
    ("kw", 2, 3),
    ("wp", 5, 2),
    ("rc", 4, 3),
    ("rw", 4, 1),
    ("kw", 4, 1),
    ("rc", 2, 3),
    ("re", 5, 0),
    ("om", 1, 2),
    ("bw", 0, 0),
    ("fin", 1, 3),
    ("fin", 3, 3),
    ("fin", 0, 3),
    ("fin", 0, 2),
    ("fin", 1, 2),
    ("fin", 3, 2),
    ("rc", 4, 1),
    ("fin", 2, 2),
    ("om", 1, 4),
    ("fin", 1, 4),
    ("fin", 2, 3),
    ("fin", 2, 4),
    ("fin", 0, 4),
    ("fin", 3, 4),
)


def partner_2(value, axis, distance):
    mask = 2**distance
    pairs = [(source, source ^ mask) for source in range(lax.axis_size(axis))]
    return lax.ppermute(value, axis, pairs)


def rank_columns(matrix):
    query_cols = QHEADS * HEAD_DIM
    pair_cols = KVHEADS * HEAD_DIM
    leading = matrix.shape[:-1]
    query = matrix[..., :query_cols].reshape(leading + (TP, query_cols // TP))
    keys = matrix[..., query_cols : query_cols + pair_cols].reshape(leading + (TP, pair_cols // TP))
    values = matrix[..., query_cols + pair_cols :].reshape(leading + (TP, pair_cols // TP))
    return jnp.concatenate([query, keys, values], axis=-1)


def normalize(tokens, gain):
    floats = tokens.astype(jnp.float32)
    scale = lax.rsqrt(jnp.mean(floats * floats, axis=-1, keepdims=True) + EPSILON)
    return (floats * scale * gain.astype(jnp.float32)).astype(jnp.bfloat16)


def general_device(tokens, norm_gain, master_qkv, qkv_bias):
    shard_count = lax.axis_size("shard")
    local_rows = master_qkv.shape[0]
    rank_width = master_qkv.shape[1] // TP
    gain_full, bias_full = (
        lax.all_gather(norm_gain.astype(jnp.bfloat16), ("inst", "shard"), axis=0, tiled=True),
        lax.all_gather(qkv_bias.astype(jnp.bfloat16), ("inst", "shard"), axis=0, tiled=True),
    )
    normed = normalize(tokens, gain_full)
    shard_pos = lax.axis_index("shard")
    rank_index = shard_pos % TP
    bit_count = TP.bit_length() - 1
    bit_order = list(range(bit_count))
    group_rows = normed
    for bit_pos in bit_order:
        partner = partner_2(group_rows, "shard", bit_pos)
        lower = jnp.bitwise_and(jnp.right_shift(shard_pos, bit_pos), 1) == 0
        group_rows = jnp.where(
            lower,
            jnp.concatenate([group_rows, partner], 0),
            jnp.concatenate([partner, group_rows], 0),
        )
    copies = shard_count // TP
    inst_block = shard_count * local_rows
    rows_low = master_qkv.astype(jnp.bfloat16)
    ranked = jnp.transpose(rank_columns(rows_low), (1, 0, 2))
    spread = jnp.broadcast_to(ranked[None], (copies,) + ranked.shape)
    outgoing = spread.reshape(shard_count, rows_low.shape[0], rank_width)
    arrived = lax.all_to_all(outgoing, "shard", split_axis=0, concat_axis=0, tiled=True).reshape(
        inst_block, rank_width
    )
    product = jnp.dot(
        group_rows,
        lax.all_gather(arrived, "inst", axis=0, tiled=True),
        preferred_element_type=jnp.float32,
    )
    bias_ranks = rank_columns(bias_full)
    bias_mine = lax.dynamic_index_in_dim(bias_ranks, rank_index, 0, keepdims=False)
    result = (product + bias_mine.astype(jnp.float32)).astype(jnp.bfloat16)
    return result[None]


def incoming(kind):
    chunks = [c for c in CHUNKS[1 - kind] if c[0] == "far"]
    return [c[1:] for c in chunks + [c for c in CHUNKS[kind] if c[0] == "extra"]]


def chunk_of(kind, j):
    what, first, count = CHUNKS[kind][j]
    return what, first, count, sum(c[2] for c in CHUNKS[kind][:j])


def kernel(
    dims,
    tok_hbm,
    gain_hbm,
    w_hbm,
    bias_hbm,
    out_ref,
    gain_ref,
    bias_ref,
    tok_ref,
    w_ref,
    xsend,
    xbuf,
    wsend,
    wbuf,
    dbuf,
    ebuf,
    psend,
    pbuf,
    acc,
    bias_own,
    bbuf,
    load_sem,
    x_recv,
    x1_recv,
    x_send,
    w_recv,
    wx_recv,
    wc_recv,
    d_recv,
    e_recv,
    w_send,
    p_recv,
    p_send,
    b_recv,
    b_send,
):
    inst_count, shard_count, group = dims
    devices = inst_count * shard_count
    inst = lax.axis_index("inst")
    me = lax.axis_index("shard")
    z = me // 2
    y = lax.rem(me, 2)
    half = z // 2
    flat = inst * shard_count + me
    core_peer = inst + 1 - 2 * lax.rem(inst, 2)
    x_peer = lax.rem(inst + 2, inst_count)
    z_mate = z + 1 - 2 * lax.rem(z, 2)
    z_pair = lax.rem(z + 2, 4)
    z_near = 2 - half
    z_end = 3 - 3 * half
    inner = z_near + z == 3
    rows = w_ref.shape[0]
    tokens, depth = tok_ref.shape
    tiles = wsend.shape[1]
    half_block = 4 * rows
    pieces = TOKEN_PIECES
    piece_rows = tokens // pieces

    halves = 2
    step_rows = tokens // halves
    row_cut = rows // 2

    def token_load(q):
        part = pl.ds(q * step_rows, step_rows)
        return pltpu.make_async_copy(tok_hbm.at[part], tok_ref.at[part], load_sem.at[q])

    def weight_load(q):
        part = pl.ds(q * row_cut, row_cut)
        return pltpu.make_async_copy(w_hbm.at[part], w_ref.at[part], load_sem.at[2 + q])

    for q in range(halves):
        token_load(q).start()

    barrier = pltpu.get_barrier_semaphore()

    def greet(owner, there):
        pl.semaphore_signal(barrier, inc=1, device_id=(owner, there), device_id_type=MESH)

    greet(inst, z_pair * 2 + y)
    greet(inst, z_mate * 2 + y)
    greet(inst, z * 2 + 1 - y)
    greet(x_peer, me)
    greet(core_peer, me)
    pl.when(inner)(lambda: greet(inst, z_near * 2 + y))
    for q in range(2):
        weight_load(q).start()
    small_load = (
        pltpu.make_async_copy(gain_hbm, gain_ref, load_sem.at[4]),
        pltpu.make_async_copy(bias_hbm, bias_ref, load_sem.at[5]),
    )
    for copy in small_load:
        copy.start()

    def remote(source, target, send_sem, recv_sem, device):
        return pltpu.make_async_remote_copy(
            src_ref=source,
            dst_ref=target,
            send_sem=send_sem,
            recv_sem=recv_sem,
            device_id=device,
            device_id_type=MESH,
        )

    def each(condition, action):
        pl.when(condition)(action)

    def piece_of(ref, piece):
        return ref.at[pl.ds(piece * piece_rows, piece_rows)]

    def own_x(which, device, side, piece):
        return remote(
            piece_of(xsend.at[which], piece),
            piece_of(xbuf.at[side, half, lax.rem(z, 2)], piece),
            x_send.at[0],
            x1_recv.at[half] if side else x_recv.at[z, piece],
            (inst, device),
        )

    def relay_x(way, block, piece):
        device, side = ((z_mate * 2 + y, 0), (z * 2 + 1 - y, 1))[way]
        return remote(
            piece_of(xbuf.at[0, block // 2, lax.rem(block, 2)], piece),
            piece_of(xbuf.at[side, block // 2, lax.rem(block, 2)], piece),
            x_send.at[1 + way],
            x1_recv.at[block // 2] if side else x_recv.at[block, piece],
            (inst, device),
        )

    def slot_of(owner, k):
        return owner * 4 + lax.rem(z_mate if k // 2 else z, 2) * 2 + (1 - y if k % 2 else y)

    def fresh(kind, there, j, side):
        what, first, count, _ = chunk_of(kind, j)
        rank = {"far": lax.rem(there + 2, 4), "extra": z_near, "own": there}[what] * 2 + side
        return wsend.at[rank, pl.ds(first, count)]

    def held(kind, slot, j):
        _, _, count, at = chunk_of(kind, j)
        return wbuf.at[slot, pl.ds(at, count)]

    def arrived(ref, sem):
        pltpu.make_async_copy(ref, ref, sem).wait()

    query = QHEADS * HEAD_DIM // TP
    pair = KVHEADS * HEAD_DIM // TP
    held_bias = bias_ref.shape[1]
    per_row = LANES // group
    groups = held_bias // group

    def needs(owner, rank):
        low, high = owner * held_bias, owner * held_bias + held_bias
        result = None
        for start, extent in (
            (rank * query, query),
            (TP * query + rank * pair, pair),
            (TP * (query + pair) + rank * pair, pair),
        ):
            overlap = jnp.logical_and(start < high, low < start + extent)
            result = overlap if result is None else jnp.logical_or(result, overlap)
        return result

    def bias_slot(owner, rank):
        first = rank * query // held_bias
        pairs = [(TP * query + (rank + TP * n) * pair) // held_bias for n in range(2)]
        late = jnp.where(owner - pairs[1] >= 0, 6 + owner - pairs[1], 4 + owner - pairs[0])
        return jnp.where(jnp.logical_and(owner - first >= 0, owner - first < 4), owner - first, late)

    def bias_copy(step):
        there = lax.rem(flat + step, devices)
        owner, rank = there // shard_count, lax.rem(there, shard_count)
        return remote(
            bias_own,
            bbuf.at[flat],
            b_send.at[owner * 3 + lax.rem(rank, 3)],
            b_recv.at[bias_slot(flat, rank)],
            (owner, rank),
        )

    def send_bias(finish):
        @pl.loop(1, devices)
        def _(step):
            there = lax.rem(flat + step, devices)

            @pl.when(needs(flat, lax.rem(there, shard_count)))
            def _():
                if finish:
                    bias_copy(step).wait_send()
                else:
                    bias_copy(step).start()

    def bias_row(number_first):
        lane = lax.broadcasted_iota(jnp.int32, (1, LANES), 1) // group
        row = jnp.zeros((1, LANES), jnp.float32)
        for q in range(per_row):
            number = number_first + q
            row = jnp.where(lane == q, bbuf[number // groups, pl.ds(lax.rem(number, groups), 1), :], row)
        return row

    def column_of(t):
        at = t * LANES
        if at < query:
            return me * query + at
        if at < query + pair:
            return TP * query + me * pair + (at - query)
        return TP * (query + pair) + me * pair + (at - query - pair)

    narrow = 16
    for first in range(0, tokens, narrow):
        if first % step_rows == 0:
            token_load(first // step_rows).wait()
        values = tok_ref[first : first + narrow, :].astype(jnp.float32)
        mean = jnp.sum(values * values, axis=-1, keepdims=True) * (1.0 / depth)
        scaled = (values * lax.rsqrt(mean + EPSILON)).astype(jnp.bfloat16)
        for which in range(2):
            for owner in range(inst_count):
                at = (owner * 2 + which) * half_block
                xsend[which, first : first + narrow, owner * half_block : (owner + 1) * half_block] = scaled[
                    :, at : at + half_block
                ]
    pl.semaphore_wait(barrier, jnp.where(inner, 6, 5))

    def send_x(name, piece):
        which, device, side = {
            "xf": (1 - half, z_near * 2 + y, 0),
            "xm": (half, z_mate * 2 + y, 0),
            "xy": (half, z * 2 + 1 - y, 1),
        }[name]
        own_x(which, device, side, piece).start()

    def early(steps):
        for name, piece, _ in steps:
            if name not in ("xf", "xm", "xy"):
                break
            send_x(name, piece)

    each(inner, lambda: early(INNER))
    each(jnp.logical_not(inner), lambda: early(OUTER))
    xbuf[0, half, lax.rem(z, 2)] = xsend[half]

    small_load[0].wait()
    ids = lax.broadcasted_iota(jnp.int32, (rows, rows), 0), lax.broadcasted_iota(jnp.int32, (rows, rows), 1)
    gain_row = gain_ref[...].astype(jnp.bfloat16).astype(jnp.float32)
    gain = jnp.sum(jnp.where(ids[0] == ids[1], jnp.broadcast_to(gain_row, (rows, rows)), 0.0), axis=1, keepdims=True)
    for q in range(2):
        weight_load(q).wait()
    for rank in range(TP):
        starts = (
            (rank * query, 0, query),
            (TP * query + rank * pair, query, pair),
            (TP * (query + pair) + rank * pair, query + pair, pair),
        )
        for source, target, extent in starts:
            for inside in range(0, extent, LANES):
                part = w_ref[:, source + inside : source + inside + LANES].astype(jnp.bfloat16).astype(jnp.float32)
                wsend[rank, (target + inside) // LANES] = (part * gain).astype(jnp.bfloat16)

    def product(kind, lhs, j):
        _, first, count, at = chunk_of(kind, j)
        result = []
        for t in range(0, count, 2):
            width = min(2, count - t)
            rhs = [wbuf[:, at + t + u].reshape(4 * half_block, LANES) for u in range(width)]
            rhs = jnp.concatenate(rhs, axis=1) if width > 1 else rhs[0]
            value = jnp.dot(lhs, rhs, preferred_element_type=jnp.float32)
            for u in range(width):
                result.append((t + u, value[:, u * LANES : (u + 1) * LANES]))
        return result

    def finish_bias():
        @pl.loop(1, devices)
        def _(step):
            slot = lax.rem(flat + step, devices)

            @pl.when(needs(slot, me))
            def _():
                arrived(bbuf.at[slot], b_recv.at[bias_slot(slot, me)])

        bbuf[flat] = bias_own[...]
        send_bias(True)

    def run(kind, steps):
        other = 1 - kind
        done = set()

        def once(key, action):
            if key not in done:
                done.add(key)
                action()

        def need_x(block):
            for piece in range(pieces):
                once(
                    ("x", block, piece),
                    lambda piece=piece: arrived(
                        mine(block, piece), x_recv.at[places[block], piece]
                    ),
                )

        def need_w(k, j):
            once(("w", k, j), lambda: arrived(held(kind, slot_of(inst, k), j), w_recv.at[k - 1, j]))

        def need_chunk(j):
            _, first, count, at = chunk_of(kind, j)

            def action():
                arrived(wbuf.at[pl.ds(0, 8), pl.ds(at, count)], wc_recv.at[j])
                wbuf[slot_of(inst, 0), at : at + count] = fresh(kind, z, j, y)[...]

            once(("c", j), action)

        def mine(block, piece):
            return piece_of(xbuf.at[0, places[block] // 2, lax.rem(places[block], 2)], piece)

        def need_tokens(unit):
            if unit < 2:
                for block in ((1,), (2, 3))[unit]:
                    need_x(block)
            else:
                part = half if unit == 2 else 1 - half
                once(("y", unit), lambda: arrived(xbuf.at[1, part], x1_recv.at[part]))

        places = (z, z_mate, z_near, z_end)

        def step_rx(block, piece):
            once(
                ("x", block, piece),
                lambda: arrived(mine(block, piece), x_recv.at[places[block], piece]),
            )
            relay_x(0, places[block], piece).start()

        def step_ry(block, piece):
            once(
                ("x", block, piece),
                lambda: arrived(mine(block, piece), x_recv.at[places[block], piece]),
            )
            relay_x(1, places[block], piece).start()

        def step_wp(j, k):
            mine = slot_of(inst, 0)
            if k == 1:
                source, target, device = fresh(kind, z, j, 1 - y), held(kind, mine, j), z * 2 + 1 - y
            else:
                source, target, device = fresh(other, z_mate, j, y), held(other, mine, j), z_mate * 2 + y
            remote(source, target, w_send.at[k - 1], w_recv.at[k - 1, j], (inst, device)).start()

        def step_wd(j, _):
            _, _, count, at = chunk_of(other, j)
            target = dbuf.at[pl.ds(at, count)]
            remote(
                fresh(other, z_mate, j, 1 - y), target, w_send.at[2], d_recv.at[j], (inst, z_mate * 2 + y)
            ).start()

        def step_we(j, _):
            _, _, count, at = chunk_of(other, j)
            remote(
                fresh(other, z_mate, j, 1 - y), ebuf.at[pl.ds(at, count)], w_send.at[6], e_recv.at[j], (inst, z * 2 + 1 - y)
            ).start()

        def step_re(j, _):
            _, _, count, at = chunk_of(other, j)
            source = ebuf.at[pl.ds(at, count)]
            arrived(source, e_recv.at[j])
            target = held(other, slot_of(inst, 1), j)
            remote(source, target, w_send.at[7], w_recv.at[2, j], (inst, z_mate * 2 + y)).start()

        def step_rd(j, _):
            _, _, count, at = chunk_of(kind, j)
            source = dbuf.at[pl.ds(at, count)]
            arrived(source, d_recv.at[j])
            target = held(kind, slot_of(inst, 2), j)
            remote(source, target, w_send.at[3], w_recv.at[2, j], (inst, z * 2 + 1 - y)).start()

        def send_block(j, k, source, across):
            device, send, recv = (
                ((x_peer, me), w_send.at[4], wx_recv.at[k, j]),
                ((core_peer, me), w_send.at[5], wc_recv.at[j]),
            )[across]
            remote(source, held(kind, slot_of(inst, k), j), send, recv, device).start()

        def step_ox(j, _):
            send_block(j, 0, fresh(kind, z, j, y), 0)

        def step_ko(j, _):
            send_block(j, 0, fresh(kind, z, j, y), 1)

        def step_rw(j, k):
            need_w(k, j)
            send_block(j, k, held(kind, slot_of(inst, k), j), 0)

        def step_kw(j, k):
            need_w(k, j)
            send_block(j, k, held(kind, slot_of(inst, k), j), 1)

        def step_rc(j, k):
            block = held(kind, slot_of(x_peer, k), j)
            arrived(block, wx_recv.at[k, j])
            remote(block, block, w_send.at[5], wc_recv.at[j], (core_peer, me)).start()

        def step_pm(unit, j):
            need_tokens(unit)
            need_chunk(j)
            what, first, count, at = chunk_of(kind, j)
            side, part = unit // 2, (1 - half if unit % 2 else half)
            lhs = xbuf[side, part].reshape(2 * tokens, 4 * half_block)
            for t, value in product(kind, lhs, j):
                psend[side, part, at + t] = value.astype(jnp.bfloat16)
            target = other if what == "far" else kind
            index = incoming(target).index((first, count))
            remote(
                psend.at[side, part, pl.ds(at, count)],
                pbuf.at[side, part, pl.ds(first, count)],
                p_send.at[0],
                p_recv.at[side, part, index],
                (inst, (z_pair if what == "far" else z_near) * 2 + y),
            ).start()

        def step_om(_, j):
            for unit in range(4):
                need_tokens(unit)
            need_chunk(j)
            first = chunk_of(kind, j)[1]
            lhs = xbuf[...].reshape(8 * tokens, 4 * half_block)
            for t, value in product(kind, lhs, j):
                for unit in range(4):
                    acc[unit // 2, unit % 2, first + t] = value[unit * 2 * tokens : (unit + 1) * 2 * tokens]

        def step_pw(unit, index):
            side, part = unit // 2, (1 - half if unit % 2 else half)
            low, extent = incoming(kind)[index]
            once(
                ("p", unit, index),
                lambda: arrived(pbuf.at[side, part, pl.ds(low, extent)], p_recv.at[side, part, index]),
            )

        def step_fin(unit, j):
            _, first, count, _ = chunk_of(kind, j)
            side, part = unit // 2, (1 - half if unit % 2 else half)
            for index, (low, extent) in enumerate(incoming(kind)):
                if low < first + count and first < low + extent:
                    step_pw(unit, index)
            where = 1 - y if side else y
            for t in range(first, first + count):
                value = acc[side, part, t] + pbuf[side, part, t].astype(jnp.float32) + bias_row(column_of(t) // group)
                value = value.astype(jnp.bfloat16)
                for k in range(2):
                    out_ref[part * 2 + k, where, :, t * LANES : (t + 1) * LANES] = value[k * tokens : (k + 1) * tokens]

        def step_bias(*_):
            small_load[1].wait()
            group_id = lax.broadcasted_iota(jnp.int32, (8, held_bias), 0)
            lane_id = lax.broadcasted_iota(jnp.int32, (8, held_bias), 1)
            spread = jnp.where(lane_id // group == group_id, jnp.broadcast_to(bias_ref[...], (8, held_bias)), 0.0)
            from_id = lax.broadcasted_iota(jnp.int32, (held_bias, LANES), 0)
            to_id = lax.broadcasted_iota(jnp.int32, (held_bias, LANES), 1)
            pick = jnp.where(lax.rem(from_id, group) == lax.rem(to_id, group), 1.0, 0.0).astype(jnp.bfloat16)
            bias_own[...] = jnp.dot(spread.astype(jnp.bfloat16), pick, preferred_element_type=jnp.float32)
            send_bias(False)

        table = dict(
            xy=lambda piece, _: send_x("xy", piece),
            xf=lambda piece, _: send_x("xf", piece),
            xm=lambda piece, _: send_x("xm", piece),
            rx=step_rx,
            ry=step_ry,
            wp=step_wp,
            wd=step_wd,
            rd=step_rd,
            we=step_we,
            re=step_re,
            ox=step_ox,
            ko=step_ko,
            rw=step_rw,
            kw=step_kw,
            rc=step_rc,
            pm=step_pm,
            om=step_om,
            fin=step_fin,
            bias=step_bias,
            bw=lambda *_: finish_bias(),
            pw=step_pw,
        )
        start = next(i for i, step in enumerate(steps) if step[0] not in ("xf", "xm", "xy"))
        for name, first, second in steps[start:]:
            table[name](first, second)

        counts = [sum(c[2] for c in CHUNKS[way]) for way in range(2)]
        sent = counts[kind] - tiles
        three = xbuf.at[0, :, :, pl.ds(0, 3 * tokens // 4)]
        arrived(three, x_send.at[0])
        arrived(three, x_send.at[2])
        if kind == 0:
            arrived(xbuf.at[0, 0], x_send.at[1])
        across = [sum(c[2] for j, c in enumerate(CHUNKS[way]) if j in ACROSS[way]) for way in range(2)]
        for way, extent in (
            (0, counts[kind]),
            (1, counts[other]),
            (2, counts[other] - across[other]),
            (3, counts[kind] - across[kind]),
            (6, across[other]),
            (7, across[other]),
        ):
            if extent:
                arrived(wbuf.at[0, pl.ds(0, extent)], w_send.at[way])
        arrived(wbuf.at[pl.ds(0, 4), pl.ds(0, counts[kind])], w_send.at[4])
        arrived(wbuf.at[pl.ds(0, 8), pl.ds(0, counts[kind])], w_send.at[5])
        arrived(psend.at[:, :, pl.ds(0, sent)], p_send.at[0])

    each(inner, lambda: run(0, INNER))
    each(jnp.logical_not(inner), lambda: run(1, OUTER))


def kernel_device(dims, tokens, norm_gain, master_qkv, qkv_bias):
    inst_count, shard_count, group = dims
    devices = inst_count * shard_count
    rows = master_qkv.shape[0]
    count, depth = tokens.shape
    tiles = master_qkv.shape[1] // TP // LANES
    pieces = TOKEN_PIECES
    most = max(len(c) for c in CHUNKS)
    held = max(sum(c[2] for c in way) for way in CHUNKS)
    dma = pltpu.SemaphoreType.DMA
    vmem = pl.BlockSpec(memory_space=pltpu.VMEM)
    anywhere = pl.BlockSpec(memory_space=pl.ANY)
    low, wide = jnp.bfloat16, jnp.float32
    result = pl.pallas_call(
        functools.partial(kernel, dims),
        out_shape=pltpu.VMEM((4, 2, count, tiles * LANES), low),
        in_specs=[anywhere] * 4,
        out_specs=vmem,
        scratch_shapes=[
            pltpu.VMEM((1, rows), wide),
            pltpu.VMEM((1, qkv_bias.shape[0]), wide),
            pltpu.VMEM((count, depth), low),
            pltpu.VMEM((rows, master_qkv.shape[1]), wide),
            pltpu.VMEM((2, count, depth // 2), low),
            pltpu.VMEM((2, 2, 2, count, depth // 2), low),
            pltpu.VMEM((TP, tiles, rows, LANES), low),
            pltpu.VMEM((4 * inst_count, held, rows, LANES), low),
            pltpu.VMEM((held, rows, LANES), low),
            pltpu.VMEM((held, rows, LANES), low),
            pltpu.VMEM((2, 2, held - tiles, 2 * count, LANES), low),
            pltpu.VMEM((2, 2, tiles, 2 * count, LANES), low),
            pltpu.VMEM((2, 2, tiles, 2 * count, LANES), wide),
            pltpu.VMEM((8, LANES), wide),
            pltpu.VMEM((devices, 8, LANES), wide),
            dma((6,)),
            dma((4, pieces)),
            dma((2,)),
            dma((3,)),
            dma((3, most)),
            dma((4, most)),
            dma((most,)),
            dma((most,)),
            dma((most,)),
            dma((8,)),
            dma((2, 2, max(len(incoming(way)) for way in range(2)))),
            dma((1,)),
            dma((8,)),
            dma((3 * inst_count,)),
        ],
        compiler_params=pltpu.CompilerParams(
            collective_id=0, has_side_effects=True, vmem_limit_bytes=56 * 1024 * 1024
        ),
    )(tokens, norm_gain.reshape(1, rows), master_qkv, qkv_bias.reshape(1, -1))
    return result.reshape(1, shard_count * count, tiles * LANES)


def per_device(tokens, norm_gain, master_qkv, qkv_bias):
    inst_count, shard_count = lax.axis_size("inst"), lax.axis_size("shard")
    group = 32
    fits = (
        shard_count == TP
        and inst_count == 4
        and master_qkv.shape[0] % 16 == 0
        and tokens.shape[0] % (16 * TOKEN_PIECES) == 0
        and QHEADS * HEAD_DIM // TP % LANES == 0
        and KVHEADS * HEAD_DIM // TP == LANES
        and 4 * master_qkv.shape[0] % LANES == 0
        and qkv_bias.shape[0] % group == 0
    )
    if fits:
        return kernel_device((inst_count, shard_count, group), tokens, norm_gain, master_qkv, qkv_bias)
    return general_device(tokens, norm_gain, master_qkv, qkv_bias)


def solution(mesh):
    in_specs = (
        P(("inst", "shard"), None),
        P(("inst", "shard")),
        P(("inst", "shard"), None),
        P(("inst", "shard")),
    )
    out_specs = P(("inst", "shard"), None, None)
    return jax.shard_map(
        per_device, mesh=mesh, in_specs=in_specs, out_specs=out_specs, check_vma=False
    )
```
